32 devices in a mesh: cp: 8 (over z, y), fsdp: 4 (over x, core).
Axes of the slice: x: 2, y: 2, z: 4, core: 2. Of those that a mesh axis runs over, the one named last changes fastest.
Arguments:
- query_states: bfloat16 [4, 1024, 1024], P('fsdp', 'cp'), may hold values from -32 to 32
- key_states: bfloat16 [4, 1024, 1024], P('fsdp', 'cp'), may hold values from -32 to 32
- value_states: bfloat16 [4, 1024, 1024], P('fsdp', 'cp'), may hold values from -6 to 6
- span_order: int32 [16], replicated, may hold values from 0 to 15, as said below
- block_mask: int32 [16, 16], replicated, may hold values from 0 to 1, as said below
- output_weight: bfloat16 [1024, 2048], P(('cp', 'fsdp')), may hold values from -0.1875 to 0.1875
- upstream: bfloat16 [4, 1024, 2048], P('fsdp', 'cp'), may hold values from -6 to 6
Outputs:
- projected: bfloat16 [4, 1024, 2048], P('fsdp', 'cp')
- query_gradient: bfloat16 [4, 1024, 1024], P('fsdp', 'cp')
- key_gradient: bfloat16 [4, 1024, 1024], P('fsdp', 'cp')
- value_gradient: bfloat16 [4, 1024, 1024], P('fsdp', 'cp')
- weight_gradient: float32 [1024, 2048], P(('cp', 'fsdp'))
The draws below stay inside these ranges and needn't reach their ends.
Inputs may be any that keep to these rules, and one draw needn't show every extreme that they name: `span_order`: entries 2 d and 2 d + 1 hold positions p and 15 - p; every position appears once. `block_mask`: the diagonal is 1.
All inputs are finite; a program needn't handle non-finite values.
Results may differ from the reference program's by a relative error of at most 0.024.
Values may be sent and summed in bfloat16 or wider, within the bound.
A program may use at most 128 MiB of HBM per device.

```python
import jax
import jax.numpy as jnp
from jax import lax

D = 2048
HEADS = 8
HEAD = 128
TOK_DEV = 128
HD = 1024
CH = 64
NCH = 16
LEN = 1024
SEQS = 4
N_CP = 8


def base_draw(key, salt):
    subkey = jax.random.fold_in(key, salt)
    values = jnp.clip(5.0 * jax.random.normal(subkey, (SEQS, LEN, HEADS * HEAD), jnp.float32), -32.0, 32.0)
    return values


def draw_query_states(key, part):
    values = base_draw(key, 11)
    return values.astype(jnp.bfloat16)


def draw_key_states(key, part):
    values = base_draw(key, 23)
    return values.astype(jnp.bfloat16)


def draw_span_order(key, part):
    pair_count = NCH // 2
    shuffled = jax.random.permutation(key, pair_count)
    paired = jnp.stack([shuffled, NCH - 1 - shuffled], axis=1).reshape(NCH)
    return paired.astype(jnp.int32)


def draw_block_mask(key, part):
    random_bits = jax.random.randint(key, (NCH, NCH), 0, 2)
    diagonal = jnp.arange(NCH)[:, None] == jnp.arange(NCH)[None, :]
    return jnp.where(diagonal, 1, random_bits).astype(jnp.int32)


def block_scale(rng, extent, pieces, least, top_value):
    def one(dim, blocks):
        draws = jax.random.uniform(jax.random.fold_in(jax.random.fold_in(rng, 6), dim), (blocks,), jnp.float32, least / len(pieces), top_value / len(pieces))
        return jnp.repeat(jnp.exp(draws), extent[dim] // blocks).reshape((-1,) + (1,) * (len(extent) - dim - 1))

    factor_of = one(*pieces[0])
    for cut in pieces[1:]:
        factor_of = factor_of * one(*cut)
    return factor_of


def normal_values(rng, dims, width, most, shards=(), kind=jnp.bfloat16):
    values = width * jax.random.normal(rng, dims, jnp.float32)
    if shards:
        values = values * block_scale(rng, dims, shards, -0.22, 0.18)
    return jnp.clip(values, -most, most).astype(kind)


def setup_inputs(seed: int = 0) -> dict:
    splits = jax.random.split(jax.random.key(seed), 8)
    query_states = draw_query_states(jax.random.fold_in(splits[7], 71), 0)
    key_states = draw_key_states(jax.random.fold_in(splits[7], 71), 0)
    value_states = normal_values(splits[2], (SEQS, LEN, HD), 1.0, 6.0, ((0, 4), (1, 8)))
    span_order = draw_span_order(jax.random.fold_in(splits[7], 71), 0)
    block_mask = draw_block_mask(jax.random.fold_in(splits[7], 71), 0)
    output_weight = normal_values(splits[5], (HD, D), HD ** -0.5, 0.1875, ((0, 32),))
    upstream = normal_values(splits[6], (SEQS, LEN, D), 1.0, 6.0, ((0, 4), (1, 8)))
    return {"query_states": query_states, "key_states": key_states, "value_states": value_states, "span_order": span_order, "block_mask": block_mask, "output_weight": output_weight, "upstream": upstream}


def reference(query_states, key_states, value_states, span_order, block_mask, output_weight, upstream):
    span_rows = CH
    positions = (span_order[:, None] * span_rows + jnp.arange(span_rows, dtype=jnp.int32)[None, :]).reshape(-1)
    onehot = (span_order[:, None] == jnp.arange(NCH, dtype=jnp.int32)[None, :]).astype(jnp.float32)
    span_ok = jnp.dot(jnp.dot(onehot, block_mask.astype(jnp.float32)), onehot.T) > 0.5
    row_span = jnp.arange(LEN, dtype=jnp.int32) // span_rows
    score_scale = 1.0 / HEAD

    def one_sequence(arrays):
        queries, key_all, value_all, grad_all = arrays
        key_f32 = key_all.astype(jnp.float32).reshape(LEN, HEADS, HEAD)
        value_f32 = value_all.astype(jnp.float32).reshape(LEN, HEADS, HEAD)

        def block_step(carry, step_index):
            key_sum, value_sum, weight_sum = carry
            begin_row = step_index * TOK_DEV
            query_block = lax.dynamic_slice_in_dim(queries, begin_row, TOK_DEV)
            grad_rows = lax.dynamic_slice_in_dim(grad_all, begin_row, TOK_DEV)
            query_pos = lax.dynamic_slice_in_dim(positions, begin_row, TOK_DEV)
            query_span = lax.dynamic_slice_in_dim(row_span, begin_row, TOK_DEV)
            allowed = span_ok[query_span][:, row_span] & (positions[None, :] <= query_pos[:, None])
            query_f32 = query_block.astype(jnp.float32).reshape(TOK_DEV, HEADS, HEAD)
            scores = jnp.einsum('qhd,khd->hqk', query_f32, key_f32) * score_scale
            masked = jnp.where(allowed[None], scores, -jnp.inf)
            row_max = masked.max(-1)
            exp_terms = jnp.where(allowed[None], jnp.exp(scores - row_max[..., None]), 0.0)
            log_total = row_max + jnp.log(exp_terms.sum(-1))
            probability = jnp.where(allowed[None], jnp.exp(scores - log_total[..., None]), 0.0)
            probability_low = lax.optimization_barrier(probability.astype(jnp.bfloat16))
            attended = jnp.einsum('hqk,khd->qhd', probability_low.astype(jnp.float32), value_f32)
            attended = lax.optimization_barrier(attended.reshape(TOK_DEV, HD).astype(jnp.bfloat16))
            projected = jnp.dot(attended, output_weight, preferred_element_type=jnp.float32).astype(jnp.bfloat16)
            grad_attended = jnp.dot(grad_rows, output_weight.T, preferred_element_type=jnp.float32).astype(jnp.bfloat16)
            grad_attended = lax.optimization_barrier(grad_attended)
            grad_f32 = grad_attended.astype(jnp.float32).reshape(TOK_DEV, HEADS, HEAD)
            row_delta = (grad_f32 * attended.astype(jnp.float32).reshape(TOK_DEV, HEADS, HEAD)).sum(-1)
            dprob = jnp.einsum('qhd,khd->hqk', grad_f32, value_f32)
            dscores = (probability * (dprob - row_delta.T[..., None]) * score_scale).astype(jnp.bfloat16)
            dscores_f32 = lax.optimization_barrier(dscores).astype(jnp.float32)
            query_grad = jnp.einsum('hqk,khd->qhd', dscores_f32, key_f32).reshape(TOK_DEV, HD).astype(jnp.bfloat16)
            key_piece = jnp.einsum('hqk,qhd->khd', dscores_f32, query_f32).astype(jnp.bfloat16)
            value_piece = jnp.einsum('hqk,qhd->khd', probability_low.astype(jnp.float32), grad_f32).astype(jnp.bfloat16)
            weight_piece = jnp.dot(attended.T, grad_rows, preferred_element_type=jnp.float32).astype(jnp.bfloat16)
            key_piece, value_piece, weight_piece = lax.optimization_barrier((key_piece, value_piece, weight_piece))
            updated = (key_sum + key_piece.astype(jnp.float32), value_sum + value_piece.astype(jnp.float32),
                       weight_sum + weight_piece.astype(jnp.float32))
            return updated, (projected, query_grad)

        start_sums = (jnp.zeros((LEN, HEADS, HEAD), jnp.float32), jnp.zeros((LEN, HEADS, HEAD), jnp.float32),
                      jnp.zeros((HD, D), jnp.float32))
        sums_out, rows_out = lax.scan(block_step, start_sums, jnp.arange(N_CP, dtype=jnp.int32))
        key_sum, value_sum, weight_sum = sums_out
        projected, query_grad = rows_out
        return (projected.reshape(LEN, D), query_grad.reshape(LEN, HD),
                key_sum.reshape(LEN, HD).astype(jnp.bfloat16), value_sum.reshape(LEN, HD).astype(jnp.bfloat16),
                weight_sum)

    projected, query_gradient, key_gradient, value_gradient, weight_sums = lax.map(
        one_sequence, (query_states, key_states, value_states, upstream))
    return projected, query_gradient, key_gradient, value_gradient, weight_sums.sum(0)
```

```python
import math

import jax
import jax.numpy as jnp
from jax import lax
from jax.experimental import pallas as pl
from jax.experimental.pallas import tpu as pltpu
from jax.sharding import PartitionSpec as P

HEADS = 8
HEAD = 128


lowest = -1e30


def split_heads(row_block):
    return row_block.reshape(row_block.shape[0], HEADS, HEAD)


def pair_scores(query_rows, key_rows):
    return jnp.einsum(
        "qhd,khd->hqk",
        split_heads(query_rows),
        split_heads(key_rows),
        preferred_element_type=jnp.float32,
    ) * (1.0 / HEAD)


def storage_mask(span_order, block_mask):
    span_count = span_order.shape[0]
    onehot = (span_order[:, None] == jnp.arange(span_count, dtype=jnp.int32)[None, :]).astype(
        jnp.float32
    )
    permuted = jnp.dot(jnp.dot(onehot, block_mask.astype(jnp.float32)), onehot.T)
    return permuted > 0.5


def allowed_block(span_ok, positions, query_begin, query_total, key_begin, key_total, span_rows):
    span_sub = lax.dynamic_slice(
        span_ok,
        (query_begin // span_rows, key_begin // span_rows),
        (query_total // span_rows, key_total // span_rows),
    )
    spread = jnp.broadcast_to(
        span_sub[:, None, :, None],
        (query_total // span_rows, span_rows, key_total // span_rows, span_rows),
    )
    spread = spread.reshape(query_total, key_total)
    query_pos = lax.dynamic_slice_in_dim(positions, query_begin, query_total)
    key_pos = lax.dynamic_slice_in_dim(positions, key_begin, key_total)
    return spread & (key_pos[None, :] <= query_pos[:, None])


def local_terms(query_rows, grad_rows, log_rows, delta_rows, key_rows, value_rows, allowed):
    scores = pair_scores(query_rows, key_rows)
    probability = jnp.where(allowed[None], jnp.exp(scores - log_rows[..., None]), 0.0)
    dprob = jnp.einsum(
        "qhd,khd->hqk",
        split_heads(grad_rows),
        split_heads(value_rows),
        preferred_element_type=jnp.float32,
    )
    dscores = (probability * (dprob - delta_rows[..., None]) * (1.0 / HEAD)).astype(jnp.bfloat16)
    return (probability, dscores)


def local(query_states, key_states, value_states, span_order, block_mask, output_weight, upstream):
    query_rows = query_states[0]
    key_local = key_states[0]
    value_local = value_states[0]
    upstream_rows = upstream[0]
    tokens = query_rows.shape[0]
    span_rows = tokens // 2
    positions = (
        span_order[:, None] * span_rows + jnp.arange(span_rows, dtype=jnp.int32)[None, :]
    ).reshape(-1)
    span_ok = storage_mask(span_order, block_mask)
    own_start = lax.axis_index("cp") * tokens
    key_all, value_all = (
        lax.all_gather(key_local, "cp", axis=0, tiled=True),
        lax.all_gather(value_local, "cp", axis=0, tiled=True),
    )
    weight = lax.all_gather(output_weight, ("cp", "fsdp"), axis=0, tiled=True)
    length = key_all.shape[0]
    key_block = math.gcd(length, 512)
    block_count = length // key_block
    block_steps = jnp.arange(block_count, dtype=jnp.int32)

    def stats_step(running, step_index):
        key_begin = step_index * key_block
        key_rows = lax.dynamic_slice_in_dim(key_all, key_begin, key_block)
        allowed = allowed_block(
            span_ok, positions, own_start, tokens, key_begin, key_block, span_rows
        )
        maxima, totals = running
        scores = pair_scores(query_rows, key_rows)
        masked = jnp.where(allowed[None], scores, lowest)
        new_max = jnp.maximum(maxima, masked.max(-1))
        exp_terms = jnp.where(allowed[None], jnp.exp(scores - new_max[..., None]), 0.0)
        return ((new_max, totals * jnp.exp(maxima - new_max) + exp_terms.sum(-1)), None)

    stat_start = (
        jnp.full((HEADS, tokens), lowest, jnp.float32),
        jnp.zeros((HEADS, tokens), jnp.float32),
    )
    (maxima, totals), _ = lax.scan(stats_step, stat_start, block_steps)
    log_total = maxima + jnp.log(totals)

    def output_step(attn_sum, step_index):
        key_begin = step_index * key_block
        key_rows = lax.dynamic_slice_in_dim(key_all, key_begin, key_block)
        value_rows = lax.dynamic_slice_in_dim(value_all, key_begin, key_block)
        allowed = allowed_block(
            span_ok, positions, own_start, tokens, key_begin, key_block, span_rows
        )
        scores = pair_scores(query_rows, key_rows)
        probability = jnp.where(allowed[None], jnp.exp(scores - log_total[..., None]), 0.0)
        return (
            attn_sum
            + jnp.einsum(
                "hqk,khd->qhd",
                probability.astype(jnp.bfloat16),
                split_heads(value_rows),
                preferred_element_type=jnp.float32,
            ),
            None,
        )

    zero_heads = jnp.zeros((tokens, HEADS, HEAD), jnp.float32)
    attn_sum, _ = lax.scan(output_step, zero_heads, block_steps)
    attended = lax.optimization_barrier(attn_sum.reshape(tokens, -1).astype(jnp.bfloat16))
    projected = jnp.dot(attended, weight, preferred_element_type=jnp.float32).astype(jnp.bfloat16)
    grad_attended = lax.dot_general(
        upstream_rows, weight, (((1,), (1,)), ((), ())), preferred_element_type=jnp.float32
    ).astype(jnp.bfloat16)
    grad_attended = lax.optimization_barrier(grad_attended)
    weight_term = lax.dot_general(
        attended, upstream_rows, (((0,), (0,)), ((), ())), preferred_element_type=jnp.float32
    )
    row_delta = (
        (grad_attended.astype(jnp.float32) * attended.astype(jnp.float32))
        .reshape(tokens, HEADS, HEAD)
        .sum(-1)
    )
    delta_heads = row_delta.T

    def query_step(grad_sum, step_index):
        key_begin = step_index * key_block
        key_rows = lax.dynamic_slice_in_dim(key_all, key_begin, key_block)
        value_rows = lax.dynamic_slice_in_dim(value_all, key_begin, key_block)
        allowed = allowed_block(
            span_ok, positions, own_start, tokens, key_begin, key_block, span_rows
        )
        probability, dscores = local_terms(
            query_rows, grad_attended, log_total, delta_heads, key_rows, value_rows, allowed
        )
        return (
            grad_sum
            + jnp.einsum(
                "hqk,khd->qhd", dscores, split_heads(key_rows), preferred_element_type=jnp.float32
            ),
            None,
        )

    query_sum, _ = lax.scan(query_step, zero_heads, block_steps)
    query_gradient = query_sum.reshape(tokens, -1).astype(jnp.bfloat16)
    log_all, delta_all = (
        lax.all_gather(log_total.T, "cp", axis=0, tiled=True),
        lax.all_gather(row_delta, "cp", axis=0, tiled=True),
    )
    sums_now = (zero_heads, zero_heads)
    query_piece = lax.all_gather(query_rows, "cp", axis=0, tiled=True)
    grad_piece = lax.all_gather(grad_attended, "cp", axis=0, tiled=True)
    row_count = query_piece.shape[0]
    sources = row_count // tokens
    group_size = math.gcd(sources, max(1, 512 // tokens))
    group_rows = group_size * tokens

    def group_step(running, step_index):
        offset = step_index * group_rows
        query_group = lax.dynamic_slice_in_dim(query_piece, offset, group_rows)
        grad_group = lax.dynamic_slice_in_dim(grad_piece, offset, group_rows)
        log_group = lax.dynamic_slice_in_dim(log_all, offset, group_rows).T
        delta_group = lax.dynamic_slice_in_dim(delta_all, offset, group_rows).T
        allowed = allowed_block(
            span_ok, positions, offset, group_rows, own_start, tokens, span_rows
        )
        key_sum, value_sum = running
        probability, dscores = local_terms(
            query_group, grad_group, log_group, delta_group, key_local, value_local, allowed
        )
        probability_low = probability.astype(jnp.bfloat16).reshape(
            HEADS, group_size, tokens, tokens
        )
        dscores_group = dscores.reshape(HEADS, group_size, tokens, tokens)
        qsplit = query_group.reshape(group_size, tokens, HEADS, HEAD)
        gsplit = grad_group.reshape(group_size, tokens, HEADS, HEAD)
        key_part = jnp.einsum(
            "hgqk,gqhd->gkhd", dscores_group, qsplit, preferred_element_type=jnp.float32
        ).astype(jnp.bfloat16)
        value_part = jnp.einsum(
            "hgqk,gqhd->gkhd", probability_low, gsplit, preferred_element_type=jnp.float32
        ).astype(jnp.bfloat16)
        key_part, value_part = lax.optimization_barrier((key_part, value_part))
        return (
            (
                key_sum + key_part.astype(jnp.float32).sum(0),
                value_sum + value_part.astype(jnp.float32).sum(0),
            ),
            None,
        )

    sums_now, _ = lax.scan(group_step, sums_now, jnp.arange(sources // group_size, dtype=jnp.int32))
    key_sum, value_sum = sums_now
    key_gradient = key_sum.reshape(tokens, -1).astype(jnp.bfloat16)
    value_gradient = value_sum.reshape(tokens, -1).astype(jnp.bfloat16)
    cycle_count = lax.axis_size("cp")
    batch_count = lax.axis_size("fsdp")
    slab_rows = weight_term.shape[0] // (cycle_count * batch_count)
    reordered = weight_term.reshape(cycle_count, batch_count, slab_rows, -1).transpose(1, 0, 2, 3)
    reordered = reordered.reshape(weight_term.shape[0], -1)
    partial_batch = lax.psum_scatter(
        reordered.astype(jnp.bfloat16), "fsdp", scatter_dimension=0, tiled=True
    )
    weight_gradient = lax.psum_scatter(partial_batch, "cp", scatter_dimension=0, tiled=True).astype(
        jnp.float32
    )
    return (
        projected[None],
        query_gradient[None],
        key_gradient[None],
        value_gradient[None],
        weight_gradient,
    )


MESH = pl.DeviceIdType.MESH


def remote(src, dst, send_sem, recv_sem, device):
    return pltpu.make_async_remote_copy(
        src_ref=src,
        dst_ref=dst,
        send_sem=send_sem,
        recv_sem=recv_sem,
        device_id=device,
        device_id_type=MESH,
    )


def rows_of(begin, count):
    return pl.ds(pl.multiple_of(begin, count), count)


def greet(devices):
    barrier = pltpu.get_barrier_semaphore()
    for device in devices:
        pl.semaphore_signal(barrier, inc=1, device_id=device, device_id_type=MESH)
    pl.semaphore_wait(barrier, len(devices))


def swap_bits(v):
    return 2 * lax.rem(v, 2) + v // 2


class PlaneGather:
    def __init__(self, buf, base, y, col, count, ss, rs, sends):
        self.buf, self.base, self.y, self.col = buf, base, y, col
        self.count, self.ss, self.rs, self.sends = count, ss, rs, sends
        self.mate = col + 1 - 2 * lax.rem(col, 2)
        self.across = lax.rem(col + 2, 4)
        self.mate_across = lax.rem(self.mate + 2, 4)

    def block(self, y, col, part=None):
        begin = self.base(y, col) * self.count
        if part is None:
            return self.buf.at[rows_of(begin, self.count)]
        half = self.count // 2
        return self.buf.at[rows_of(begin + part * half, half)]

    def send(self, slot, source, target, device):
        copy = remote(source, target, self.ss.at[slot], self.rs.at[slot], device)
        copy.start()
        self.sends.append(copy)

    def wait(self, slot, block):
        remote(
            block, block, self.ss.at[slot], self.rs.at[slot], {"fsdp": self.mate}
        ).wait_recv()

    def start(self, own):
        half = self.count // 2
        other = {"cp": lax.axis_index("cp") + 1 - 2 * self.y}
        for part in range(2):
            piece = own.at[pl.ds(part * half, half)]
            self.send(part, piece, self.block(self.y, self.col, part), other)
        whole = self.block(self.y, self.col)
        self.send(2, own, whole, {"fsdp": self.across})
        self.send(3, own, whole, {"fsdp": self.mate})

    def relay_y(self, part):
        block = self.block(1 - self.y, self.col, part)
        self.wait(part, block)
        self.send(4 + part, block, block, {"fsdp": self.across})
        self.send(6 + part, block, block, {"fsdp": self.mate})

    def relay_x(self):
        block = self.block(self.y, self.across)
        self.wait(2, block)
        self.send(8, block, block, {"fsdp": self.mate})

    def relay_diagonal(self, part):
        block = self.block(1 - self.y, self.across, part)
        self.wait(4 + part, block)
        self.send(9 + part, block, block, {"fsdp": self.mate})

    def wait_mate(self):
        self.wait(3, self.block(self.y, self.mate))

    def wait_mate_y(self):
        for part in range(2):
            self.wait(6 + part, self.block(1 - self.y, self.mate, part))

    def wait_mate_x(self):
        self.wait(8, self.block(self.y, self.mate_across))

    def wait_mate_diagonal(self):
        for part in range(2):
            self.wait(9 + part, self.block(1 - self.y, self.mate_across, part))


def layer_kernel(
    n, q, k, v, up, w, order, mask, proj, dq, dk, dv, wg,
    qh, kh, vh, ups, wall, bias, prob, dsb, att, attended, attp, ga_out, ga,
    dqh, dkh, dvh, dw, dwr, kt, vt,
    heads_s, heads_r, out_s, out_r, up_s, up_r, wide_s, wide_r,
    slab_s, slab_r, chain_s, chain_r, ga_s, ga_r, attp_s, attp_r, dw_s, dw_r,
):
    me = lax.axis_index("cp")
    col = lax.axis_index("fsdp")
    cols = lax.axis_size("fsdp")
    planes = n // 2
    zed, why = me // 2, lax.rem(me, 2)
    tokens = up.shape[0]
    slab = w.shape[0]
    length = tokens * n
    span_rows = tokens // 2
    bf16, f32 = jnp.bfloat16, jnp.float32
    nt = (((1,), (1,)), ((), ()))
    home = swap_bits(col)
    work_head = 2 * home + why
    root = home == zed
    pieces = chain_r.shape[0]

    def head_cols(d):
        return rows_of(d * HEAD, HEAD)

    def rows(d):
        return rows_of(d * tokens, tokens)

    barrier = pltpu.get_barrier_semaphore()
    for i in range(n):
        for j in range(cols):
            if i or j:
                pl.semaphore_signal(
                    barrier, inc=1,
                    device_id={"cp": lax.rem(me + i, n), "fsdp": lax.rem(col + j, cols)},
                    device_id_type=MESH,
                )
    pl.semaphore_wait(barrier, n * cols - 1)

    sends = []
    offsets = [n // 2]
    for i in range(1, n // 2):
        offsets += [n // 2 - i, n // 2 + i]

    def heads_send(t, source, target):
        for i in offsets:
            d = lax.rem(me + i, n)
            copy = remote(
                source.at[:, head_cols(d)], target.at[rows(me)],
                heads_s.at[t, i], heads_r.at[t, i], {"cp": d},
            )
            copy.start()
            sends.append(copy)

    def heads_wait(t, target):
        for i in offsets:
            source = lax.rem(me + n - i, n)
            block = target.at[rows(source)]
            remote(block, block, heads_s.at[t, i], heads_r.at[t, i], {"cp": source}).wait_recv()

    def out_send(t, i, source, target):
        d = lax.rem(me + i, n)
        return remote(
            source.at[rows(d)], target.at[:, head_cols(me)],
            out_s.at[t, i], out_r.at[t, i], {"cp": d},
        )

    def out_wait(t, target):
        for i in offsets:
            source = lax.rem(me + n - i, n)
            block = target.at[:, head_cols(source)]
            remote(block, block, out_s.at[t, i], out_r.at[t, i], {"cp": source}).wait_recv()

    up_gather = PlaneGather(
        ups, lambda y, c: c * 2 + y, why, col, tokens, up_s, up_r, sends
    )
    wide_gather = PlaneGather(
        wall, lambda y, c: 2 * swap_bits(c) + y, why, col, HEAD, wide_s, wide_r, sends
    )

    mine_slab = wall.at[rows_of(me * HEAD + col * slab, slab)]
    slab_copy = remote(
        w, mine_slab, slab_s.at[0], slab_r.at[col], {"fsdp": swap_bits(zed)}
    )

    @pl.when(jnp.logical_not(root))
    def _():
        slab_copy.start()

    heads_send(0, k, kh)
    up_gather.start(up)

    @pl.when(root)
    def _():
        wall[rows_of(me * HEAD + col * slab, slab)] = w[...]
        for j in range(1, cols):
            other = lax.rem(col + j, cols)
            block = wall.at[rows_of(me * HEAD + other * slab, slab)]
            remote(block, block, slab_s.at[0], slab_r.at[other], {"fsdp": other}).wait_recv()

    piece_rows = HEAD // pieces
    rising = jnp.logical_and(zed >= home, zed < planes - 1)
    falling = jnp.logical_and(zed <= home, zed > 0)

    def chain_copy(p, way):
        block = wall.at[rows_of(work_head * HEAD + p * piece_rows, piece_rows)]
        target = me + 2 if way == 0 else me - 2
        return remote(block, block, chain_s.at[way, p], chain_r.at[p], {"cp": target})

    def chain_forward(p):
        @pl.when(rising)
        def _():
            chain_copy(p, 0).start()

        @pl.when(falling)
        def _():
            chain_copy(p, 1).start()

    @pl.when(root)
    def _():
        for p in range(pieces):
            chain_forward(p)

    heads_send(1, q, qh)
    heads_send(2, v, vh)
    for source, target in ((k, kh), (q, qh), (v, vh)):
        target[rows(me)] = source[:, head_cols(me)]
    ups[rows(col * 2 + why)] = up[...]

    spans = order.shape[0]
    order_row = jnp.broadcast_to(order[...].reshape(1, spans), (spans, spans))
    place = lax.broadcasted_iota(jnp.int32, (spans, spans), 0)
    at_place = (order_row == place).astype(f32).astype(bf16)
    row = lax.broadcasted_iota(jnp.int32, (length, spans), 0)
    begin = lax.broadcasted_iota(jnp.int32, (length, spans), 1) * span_rows
    member = jnp.logical_and(row >= begin, row < begin + span_rows).astype(f32).astype(bf16)
    row_t = lax.broadcasted_iota(jnp.int32, (spans, length), 1)
    begin_t = lax.broadcasted_iota(jnp.int32, (spans, length), 0) * span_rows
    member_t = jnp.logical_and(row_t >= begin_t, row_t < begin_t + span_rows)
    member_t = member_t.astype(f32).astype(bf16)
    placed = lax.dot_general(member, at_place, nt, preferred_element_type=f32)
    placed_t = jnp.dot(at_place, member_t, preferred_element_type=f32)
    shift = lax.broadcasted_iota(jnp.int32, (length, spans), 1) * span_rows
    shift_t = lax.broadcasted_iota(jnp.int32, (spans, length), 0) * span_rows
    within = (row - begin).astype(f32) * member.astype(f32)
    within_t = (row_t - begin_t).astype(f32) * member_t.astype(f32)
    key_pos = (placed * shift.astype(f32) + within).sum(1, keepdims=True)
    query_pos = (placed_t * shift_t.astype(f32) + within_t).sum(0, keepdims=True)
    key_side = lax.dot_general(
        placed.astype(bf16), mask[...].astype(f32).astype(bf16), nt, preferred_element_type=f32
    ).astype(bf16)
    placed_low = placed_t.astype(bf16)
    for o in range(n):
        part = slice(o * tokens, (o + 1) * tokens)
        seen = jnp.dot(key_side, placed_low[:, part], preferred_element_type=f32)
        allowed = jnp.logical_and(seen > 0.5, key_pos <= query_pos[:, part])
        bias[:, part] = jnp.where(allowed, 0.0, lowest)

    def chain_relay(p):
        @pl.when(jnp.logical_not(root))
        def _():
            block = wall.at[rows_of(work_head * HEAD + p * piece_rows, piece_rows)]
            remote(block, block, chain_s.at[0, p], chain_r.at[p], {"cp": me}).wait_recv()
            chain_forward(p)

    heads_wait(0, kh)
    kt[...] = kh[...].astype(f32).T.astype(bf16)
    for p in range(pieces // 2):
        chain_relay(p)
    up_gather.relay_y(0)
    for p in range(pieces // 2, pieces):
        chain_relay(p)
    up_gather.relay_x()
    heads_wait(1, qh)

    def soft(o, carry):
        part = rows(o)
        scores = lax.dot_general(kh[...], qh[part], nt, preferred_element_type=f32) * (1.0 / HEAD)
        scores = scores + bias[:, part]
        terms = jnp.exp(scores - scores.max(0, keepdims=True))
        probability = terms * (1.0 / terms.sum(0, keepdims=True))
        prob[:, part] = probability.astype(bf16)
        return carry

    lax.fori_loop(0, n // 2, soft, 0)
    up_gather.relay_y(1)
    wide_gather.start(wall.at[rows_of(work_head * HEAD, HEAD)])
    lax.fori_loop(n // 2, n, soft, 0)

    def ga_copy(j, s):
        return remote(
            ga_out.at[rows_of(s * 2 * tokens, 2 * tokens)],
            ga.at[rows_of(zed * 2 * tokens, 2 * tokens)],
            ga_s.at[j], ga_r.at[zed], {"cp": work_head, "fsdp": s},
        )

    def ga_group(j, s):
        part = rows_of(s * 2 * tokens, 2 * tokens)
        result = lax.dot_general(
            ups[part], wall[rows_of(work_head * HEAD, HEAD)], nt, preferred_element_type=f32
        ).astype(bf16)
        ga_out[part] = result
        if j == 0:
            @pl.when(root)
            def _():
                ga[rows_of(zed * 2 * tokens, 2 * tokens)] = result

            @pl.when(jnp.logical_not(root))
            def _():
                ga_copy(j, s).start()
        else:
            copy = ga_copy(j, s)
            copy.start()
            sends.append(copy)

    ga_group(0, col)
    up_gather.wait_mate()
    up_gather.wait_mate_y()
    ga_group(1, up_gather.mate)
    heads_wait(2, vh)
    vt[...] = vh[...].astype(f32).T.astype(bf16)

    def attend(o, carry):
        part = rows_of(o * 2 * tokens, 2 * tokens)
        att_t = jnp.dot(vt[...], prob[:, part], preferred_element_type=f32)
        att[part] = att_t.T.astype(bf16)
        return carry

    lax.fori_loop(0, n // 2, attend, 0)
    for i in offsets:
        copy = out_send(0, i, att, attended)
        copy.start()
        sends.append(copy)
    attended[:, head_cols(me)] = att[rows(me)]
    up_gather.relay_diagonal(0)
    up_gather.relay_diagonal(1)
    ga_group(2, up_gather.across)
    up_gather.wait_mate_x()
    up_gather.wait_mate_diagonal()
    ga_group(3, up_gather.mate_across)
    wide_gather.relay_y(0)
    wide_gather.relay_x()
    wide_gather.relay_y(1)

    out_wait(0, attended)
    own_rows = (col * 2 + why) * tokens
    for i in range(2):
        for j in range(cols):
            if i == 0 and j == 0:
                attp[rows_of(own_rows, tokens)] = attended[:, head_cols(work_head)]
                continue
            other_y = lax.rem(why + i, 2)
            other_col = lax.rem(col + j, cols)
            head = 2 * swap_bits(other_col) + other_y
            copy = remote(
                attended.at[:, head_cols(head)], attp.at[rows_of(own_rows, tokens)],
                attp_s.at[i * cols + j], attp_r.at[i * cols + j],
                {"cp": zed * 2 + other_y, "fsdp": other_col},
            )
            copy.start()
            sends.append(copy)

    for j in range(planes):
        source = lax.rem(zed + j, planes)
        block = ga.at[rows_of(source * 2 * tokens, 2 * tokens)]
        arrived = remote(block, block, ga_s.at[0], ga_r.at[source], {"cp": me})
        if j == 0:
            @pl.when(jnp.logical_not(root))
            def _():
                arrived.wait_recv()
        else:
            arrived.wait_recv()

    def value_step(o, carry):
        part = rows_of(o * 2 * tokens, 2 * tokens)
        dvh[part] = jnp.dot(prob[part], ga[...], preferred_element_type=f32).astype(bf16)
        return carry

    lax.fori_loop(0, n // 2, value_step, 0)
    for i in offsets:
        copy = out_send(2, i, dvh, dv)
        copy.start()
        sends.append(copy)
    dv[:, head_cols(me)] = dvh[rows(me)]

    def backward(i, carry):
        o = lax.rem(me + i, n)
        part = rows(o)
        ga_rows = ga[part]
        delta = (att[part].astype(f32) * ga_rows.astype(f32)).T.sum(0, keepdims=True)
        dprob = lax.dot_general(vh[...], ga_rows, nt, preferred_element_type=f32)
        ds = (prob[:, part].astype(f32) * ((dprob - delta) * (1.0 / HEAD))).astype(bf16)
        dsb[:, part] = ds
        dqh[part] = jnp.dot(kt[...], ds, preferred_element_type=f32).T.astype(bf16)

        @pl.when(i > 0)
        def _():
            out_send(3, i, dqh, dq).start()

        return carry

    lax.fori_loop(0, n, lambda i, c: backward(lax.rem(i + n // 2, n), c), 0)
    dq[:, head_cols(me)] = dqh[rows(me)]

    def key_step(o, carry):
        part = rows_of(o * 2 * tokens, 2 * tokens)
        dkh[part] = jnp.dot(dsb[part], qh[...], preferred_element_type=f32).astype(bf16)
        return carry

    lax.fori_loop(0, n // 2, key_step, 0)
    for i in offsets:
        copy = out_send(1, i, dkh, dk)
        copy.start()
        sends.append(copy)
    dk[:, head_cols(me)] = dkh[rows(me)]

    for i in range(2):
        for j in range(cols):
            if i == 0 and j == 0:
                continue
            other_y = lax.rem(why + 2 - i, 2)
            other_col = lax.rem(col + cols - j, cols)
            block = attp.at[rows_of((other_col * 2 + other_y) * tokens, tokens)]
            remote(
                block, block, attp_s.at[i * cols + j], attp_r.at[i * cols + j], {"cp": me}
            ).wait_recv()
    att_t = attp[...].astype(f32).T.astype(bf16)
    width = math.gcd(proj.shape[1], 512)
    for i in range(proj.shape[1] // width):
        part = slice(i * width, (i + 1) * width)
        dw[:, part] = jnp.dot(att_t, ups[:, part], preferred_element_type=f32).astype(bf16)

    def dw_copy(j):
        s = lax.rem(col + j, cols)
        return remote(
            dw.at[rows_of(s * slab, slab)], dwr.at[zed], dw_s.at[j], dw_r.at[zed],
            {"cp": work_head, "fsdp": s},
        )

    @pl.when(root)
    def _():
        dwr[zed] = dw[rows_of(col * slab, slab)]

    @pl.when(jnp.logical_not(root))
    def _():
        dw_copy(0).start()

    for j in range(1, cols):
        copy = dw_copy(j)
        copy.start()
        sends.append(copy)

    wide_gather.relay_diagonal(0)
    wide_gather.relay_diagonal(1)
    wide_gather.wait_mate()
    wide_gather.wait_mate_y()
    wide_gather.wait_mate_x()
    wide_gather.wait_mate_diagonal()

    def project(i, carry):
        part = rows_of(i * width, width)
        proj[:, part] = jnp.dot(
            attended[...], wall[:, part], preferred_element_type=f32
        ).astype(bf16)
        return carry

    lax.fori_loop(0, proj.shape[1] // width, project, 0)
    for j in range(planes):
        source = lax.rem(zed + j, planes)
        block = dwr.at[source]
        arrived = remote(block, block, dw_s.at[0], dw_r.at[source], {"cp": me})
        if j == 0:
            @pl.when(jnp.logical_not(root))
            def _():
                arrived.wait_recv()
        else:
            arrived.wait_recv()
    total = dwr[0].astype(f32)
    for j in range(1, planes):
        total = total + dwr[j].astype(f32)
    wg[...] = total
    out_wait(2, dv)
    out_wait(3, dq)
    out_wait(1, dk)
    for copy in sends:
        copy.wait_send()
    for i in offsets:
        out_send(3, i, dqh, dq).wait_send()

    @pl.when(jnp.logical_not(root))
    def _():
        slab_copy.wait_send()
        ga_copy(0, col).wait_send()
        dw_copy(0).wait_send()

    for p in range(pieces):
        @pl.when(rising)
        def _():
            chain_copy(p, 0).wait_send()

        @pl.when(falling)
        def _():
            chain_copy(p, 1).wait_send()


def by_heads(query_states, key_states, value_states, span_order, block_mask, output_weight, upstream):
    n = lax.axis_size("cp")
    m = lax.axis_size("fsdp")
    tokens, width = query_states.shape[1:]
    length = tokens * n
    model = upstream.shape[2]
    slab = output_weight.shape[0]
    bf16, f32 = jnp.bfloat16, jnp.float32
    shape = jax.ShapeDtypeStruct
    vmem = pl.BlockSpec(memory_space=pltpu.VMEM)
    dma = pltpu.SemaphoreType.DMA
    planes = n // 2
    pieces = 4
    head_array = pltpu.VMEM((length, HEAD), bf16)
    square = pltpu.VMEM((length, length), bf16)
    projected, dq, dk, dv, weight_gradient = pl.pallas_call(
        lambda *refs: layer_kernel(n, *refs),
        out_shape=(shape((tokens, model), bf16),)
        + (shape((tokens, width), bf16),) * 3
        + (shape((slab, model), f32),),
        in_specs=[vmem] * 7,
        out_specs=(vmem,) * 5,
        scratch_shapes=[
            head_array, head_array, head_array,
            pltpu.VMEM((length, model), bf16), pltpu.VMEM((width, model), bf16),
            pltpu.VMEM((length, length), f32), square, square,
            head_array, pltpu.VMEM((tokens, width), bf16), head_array, head_array, head_array,
            head_array, head_array, head_array,
            pltpu.VMEM((HEAD, model), bf16), pltpu.VMEM((planes, slab, model), bf16),
            pltpu.VMEM((HEAD, length), bf16), pltpu.VMEM((HEAD, length), bf16),
            dma((3, n)), dma((3, n)), dma((4, n)), dma((4, n)),
            dma((11,)), dma((11,)), dma((11,)), dma((11,)),
            dma((1,)), dma((m,)), dma((2, pieces)), dma((pieces,)),
            dma((m,)), dma((planes,)), dma((2 * m,)), dma((2 * m,)), dma((m,)), dma((planes,)),
        ],
        compiler_params=pltpu.CompilerParams(
            collective_id=0, has_side_effects=True, vmem_limit_bytes=48 << 20
        ),
        name="layer",
    )(
        query_states[0], key_states[0], value_states[0], upstream[0], output_weight,
        span_order, block_mask,
    )
    return (projected[None], dq[None], dk[None], dv[None], weight_gradient)


def solution(mesh):
    fits = mesh.shape["cp"] == HEADS and mesh.shape["fsdp"] == 4
    return jax.shard_map(
        by_heads if fits else local,
        mesh=mesh,
        in_specs=(
            P("fsdp", "cp", None),
            P("fsdp", "cp", None),
            P("fsdp", "cp", None),
            P(),
            P(),
            P(("cp", "fsdp"), None),
            P("fsdp", "cp", None),
        ),
        out_specs=(
            P("fsdp", "cp", None),
            P("fsdp", "cp", None),
            P("fsdp", "cp", None),
            P("fsdp", "cp", None),
            P(("cp", "fsdp"), None),
        ),
        check_vma=False,
    )
```

```python
import math

import jax
import jax.numpy as jnp
from jax import lax
from jax.experimental import pallas as pl
from jax.experimental.pallas import tpu as pltpu
from jax.sharding import PartitionSpec as P

HEADS = 8
HEAD = 128


lowest = -1e30


def split_heads(row_block):
    return row_block.reshape(row_block.shape[0], HEADS, HEAD)


def pair_scores(query_rows, key_rows):
    return jnp.einsum(
        "qhd,khd->hqk",
        split_heads(query_rows),
        split_heads(key_rows),
        preferred_element_type=jnp.float32,
    ) * (1.0 / HEAD)


def storage_mask(span_order, block_mask):
    span_count = span_order.shape[0]
    onehot = (span_order[:, None] == jnp.arange(span_count, dtype=jnp.int32)[None, :]).astype(
        jnp.float32
    )
    permuted = jnp.dot(jnp.dot(onehot, block_mask.astype(jnp.float32)), onehot.T)
    return permuted > 0.5


def allowed_block(span_ok, positions, query_begin, query_total, key_begin, key_total, span_rows):
    span_sub = lax.dynamic_slice(
        span_ok,
        (query_begin // span_rows, key_begin // span_rows),
        (query_total // span_rows, key_total // span_rows),
    )
    spread = jnp.broadcast_to(
        span_sub[:, None, :, None],
        (query_total // span_rows, span_rows, key_total // span_rows, span_rows),
    )
    spread = spread.reshape(query_total, key_total)
    query_pos = lax.dynamic_slice_in_dim(positions, query_begin, query_total)
    key_pos = lax.dynamic_slice_in_dim(positions, key_begin, key_total)
    return spread & (key_pos[None, :] <= query_pos[:, None])


def local_terms(query_rows, grad_rows, log_rows, delta_rows, key_rows, value_rows, allowed):
    scores = pair_scores(query_rows, key_rows)
    probability = jnp.where(allowed[None], jnp.exp(scores - log_rows[..., None]), 0.0)
    dprob = jnp.einsum(
        "qhd,khd->hqk",
        split_heads(grad_rows),
        split_heads(value_rows),
        preferred_element_type=jnp.float32,
    )
    dscores = (probability * (dprob - delta_rows[..., None]) * (1.0 / HEAD)).astype(jnp.bfloat16)
    return (probability, dscores)


def local(query_states, key_states, value_states, span_order, block_mask, output_weight, upstream):
    query_rows = query_states[0]
    key_local = key_states[0]
    value_local = value_states[0]
    upstream_rows = upstream[0]
    tokens = query_rows.shape[0]
    span_rows = tokens // 2
    positions = (
        span_order[:, None] * span_rows + jnp.arange(span_rows, dtype=jnp.int32)[None, :]
    ).reshape(-1)
    span_ok = storage_mask(span_order, block_mask)
    own_start = lax.axis_index("cp") * tokens
    key_all, value_all = (
        lax.all_gather(key_local, "cp", axis=0, tiled=True),
        lax.all_gather(value_local, "cp", axis=0, tiled=True),
    )
    weight = lax.all_gather(output_weight, ("cp", "fsdp"), axis=0, tiled=True)
    length = key_all.shape[0]
    key_block = math.gcd(length, 512)
    block_count = length // key_block
    block_steps = jnp.arange(block_count, dtype=jnp.int32)

    def stats_step(running, step_index):
        key_begin = step_index * key_block
        key_rows = lax.dynamic_slice_in_dim(key_all, key_begin, key_block)
        allowed = allowed_block(
            span_ok, positions, own_start, tokens, key_begin, key_block, span_rows
        )
        maxima, totals = running
        scores = pair_scores(query_rows, key_rows)
        masked = jnp.where(allowed[None], scores, lowest)
        new_max = jnp.maximum(maxima, masked.max(-1))
        exp_terms = jnp.where(allowed[None], jnp.exp(scores - new_max[..., None]), 0.0)
        return ((new_max, totals * jnp.exp(maxima - new_max) + exp_terms.sum(-1)), None)

    stat_start = (
        jnp.full((HEADS, tokens), lowest, jnp.float32),
        jnp.zeros((HEADS, tokens), jnp.float32),
    )
    (maxima, totals), _ = lax.scan(stats_step, stat_start, block_steps)
    log_total = maxima + jnp.log(totals)

    def output_step(attn_sum, step_index):
        key_begin = step_index * key_block
        key_rows = lax.dynamic_slice_in_dim(key_all, key_begin, key_block)
        value_rows = lax.dynamic_slice_in_dim(value_all, key_begin, key_block)
        allowed = allowed_block(
            span_ok, positions, own_start, tokens, key_begin, key_block, span_rows
        )
        scores = pair_scores(query_rows, key_rows)
        probability = jnp.where(allowed[None], jnp.exp(scores - log_total[..., None]), 0.0)
        return (
            attn_sum
            + jnp.einsum(
                "hqk,khd->qhd",
                probability.astype(jnp.bfloat16),
                split_heads(value_rows),
                preferred_element_type=jnp.float32,
            ),
            None,
        )

    zero_heads = jnp.zeros((tokens, HEADS, HEAD), jnp.float32)
    attn_sum, _ = lax.scan(output_step, zero_heads, block_steps)
    attended = lax.optimization_barrier(attn_sum.reshape(tokens, -1).astype(jnp.bfloat16))
    projected = jnp.dot(attended, weight, preferred_element_type=jnp.float32).astype(jnp.bfloat16)
    grad_attended = lax.dot_general(
        upstream_rows, weight, (((1,), (1,)), ((), ())), preferred_element_type=jnp.float32
    ).astype(jnp.bfloat16)
    grad_attended = lax.optimization_barrier(grad_attended)
    weight_term = lax.dot_general(
        attended, upstream_rows, (((0,), (0,)), ((), ())), preferred_element_type=jnp.float32
    )
    row_delta = (
        (grad_attended.astype(jnp.float32) * attended.astype(jnp.float32))
        .reshape(tokens, HEADS, HEAD)
        .sum(-1)
    )
    delta_heads = row_delta.T

    def query_step(grad_sum, step_index):
        key_begin = step_index * key_block
        key_rows = lax.dynamic_slice_in_dim(key_all, key_begin, key_block)
        value_rows = lax.dynamic_slice_in_dim(value_all, key_begin, key_block)
        allowed = allowed_block(
            span_ok, positions, own_start, tokens, key_begin, key_block, span_rows
        )
        probability, dscores = local_terms(
            query_rows, grad_attended, log_total, delta_heads, key_rows, value_rows, allowed
        )
        return (
            grad_sum
            + jnp.einsum(
                "hqk,khd->qhd", dscores, split_heads(key_rows), preferred_element_type=jnp.float32
            ),
            None,
        )

    query_sum, _ = lax.scan(query_step, zero_heads, block_steps)
    query_gradient = query_sum.reshape(tokens, -1).astype(jnp.bfloat16)
    log_all, delta_all = (
        lax.all_gather(log_total.T, "cp", axis=0, tiled=True),
        lax.all_gather(row_delta, "cp", axis=0, tiled=True),
    )
    sums_now = (zero_heads, zero_heads)
    query_piece = lax.all_gather(query_rows, "cp", axis=0, tiled=True)
    grad_piece = lax.all_gather(grad_attended, "cp", axis=0, tiled=True)
    row_count = query_piece.shape[0]
    sources = row_count // tokens
    group_size = math.gcd(sources, max(1, 512 // tokens))
    group_rows = group_size * tokens

    def group_step(running, step_index):
        offset = step_index * group_rows
        query_group = lax.dynamic_slice_in_dim(query_piece, offset, group_rows)
        grad_group = lax.dynamic_slice_in_dim(grad_piece, offset, group_rows)
        log_group = lax.dynamic_slice_in_dim(log_all, offset, group_rows).T
        delta_group = lax.dynamic_slice_in_dim(delta_all, offset, group_rows).T
        allowed = allowed_block(
            span_ok, positions, offset, group_rows, own_start, tokens, span_rows
        )
        key_sum, value_sum = running
        probability, dscores = local_terms(
            query_group, grad_group, log_group, delta_group, key_local, value_local, allowed
        )
        probability_low = probability.astype(jnp.bfloat16).reshape(
            HEADS, group_size, tokens, tokens
        )
        dscores_group = dscores.reshape(HEADS, group_size, tokens, tokens)
        qsplit = query_group.reshape(group_size, tokens, HEADS, HEAD)
        gsplit = grad_group.reshape(group_size, tokens, HEADS, HEAD)
        key_part = jnp.einsum(
            "hgqk,gqhd->gkhd", dscores_group, qsplit, preferred_element_type=jnp.float32
        ).astype(jnp.bfloat16)
        value_part = jnp.einsum(
            "hgqk,gqhd->gkhd", probability_low, gsplit, preferred_element_type=jnp.float32
        ).astype(jnp.bfloat16)
        key_part, value_part = lax.optimization_barrier((key_part, value_part))
        return (
            (
                key_sum + key_part.astype(jnp.float32).sum(0),
                value_sum + value_part.astype(jnp.float32).sum(0),
            ),
            None,
        )

    sums_now, _ = lax.scan(group_step, sums_now, jnp.arange(sources // group_size, dtype=jnp.int32))
    key_sum, value_sum = sums_now
    key_gradient = key_sum.reshape(tokens, -1).astype(jnp.bfloat16)
    value_gradient = value_sum.reshape(tokens, -1).astype(jnp.bfloat16)
    cycle_count = lax.axis_size("cp")
    batch_count = lax.axis_size("fsdp")
    slab_rows = weight_term.shape[0] // (cycle_count * batch_count)
    reordered = weight_term.reshape(cycle_count, batch_count, slab_rows, -1).transpose(1, 0, 2, 3)
    reordered = reordered.reshape(weight_term.shape[0], -1)
    partial_batch = lax.psum_scatter(
        reordered.astype(jnp.bfloat16), "fsdp", scatter_dimension=0, tiled=True
    )
    weight_gradient = lax.psum_scatter(partial_batch, "cp", scatter_dimension=0, tiled=True).astype(
        jnp.float32
    )
    return (
        projected[None],
        query_gradient[None],
        key_gradient[None],
        value_gradient[None],
        weight_gradient,
    )


MESH = pl.DeviceIdType.MESH


def remote(src, dst, send_sem, recv_sem, device):
    return pltpu.make_async_remote_copy(
        src_ref=src,
        dst_ref=dst,
        send_sem=send_sem,
        recv_sem=recv_sem,
        device_id=device,
        device_id_type=MESH,
    )


def rows_of(begin, count):
    return pl.ds(pl.multiple_of(begin, count), count)


def greet(devices):
    barrier = pltpu.get_barrier_semaphore()
    for device in devices:
        pl.semaphore_signal(barrier, inc=1, device_id=device, device_id_type=MESH)
    pl.semaphore_wait(barrier, len(devices))


def layer_kernel(
    n, q_in, k_in, v_in, up_in, w_in, order_in, mask_in, proj, dq, dk, dv, wg,
    q, k, v, up, w, order, mask, load,
    qh, kh, vh, ups, wall, bias, prob, dsb, att, attended, attp, ga_out, ga,
    dqh, dkh, dvh, dw, dwx, dwz, dwr, kt, vt,
    heads_s, heads_r, out_s, out_r, up_s, up_r, wide_s, wide_r,
    slab_s, slab_r, chain_s, chain_r, side_s, side_r, ga_s, ga_r, attp_s, attp_r,
    dwx_s, dwx_r, dw_s, dw_r,
):
    me = lax.axis_index("cp")
    col = lax.axis_index("fsdp")
    cols = lax.axis_size("fsdp")
    planes = n // 2
    zed, why = me // 2, lax.rem(me, 2)
    ex, core = col // 2, lax.rem(col, 2)
    mate = {"fsdp": 2 * ex + 1 - core}
    across = {"fsdp": 2 * (1 - ex) + core}
    beside = {"cp": 2 * zed + 1 - why}
    tokens = up.shape[0]
    slab = w.shape[0]
    length = tokens * n
    span_rows = tokens // 2
    bf16, f32 = jnp.bfloat16, jnp.float32
    nt = (((1,), (1,)), ((), ()))
    home = 2 * core + ex
    root = home == zed
    keeper = core == zed // 2
    pieces = chain_r.shape[0]
    piece_rows = HEAD // pieces

    def spot(y, plane):
        return y * planes + plane

    def cols_at(place):
        return rows_of(place * HEAD, HEAD)

    def head_cols(d):
        return rows_of(d * HEAD, HEAD)

    def rows(d):
        return rows_of(d * tokens, tokens)

    def two_rows(d):
        return rows_of(d * 2 * tokens, 2 * tokens)

    pairs = (
        (k_in, k), (up_in, up), (w_in, w), (q_in, q), (v_in, v), (order_in, order), (mask_in, mask)
    )
    loads = [pltpu.make_async_copy(a, b, load.at[t]) for t, (a, b) in enumerate(pairs)]
    for copy in loads:
        copy.start()
    barrier = pltpu.get_barrier_semaphore()
    for i in range(n):
        for j in range(cols):
            if i or j:
                pl.semaphore_signal(
                    barrier, inc=1,
                    device_id={"cp": lax.rem(me + i, n), "fsdp": lax.rem(col + j, cols)},
                    device_id_type=MESH,
                )
    for copy in loads:
        copy.wait()
    pl.semaphore_wait(barrier, n * cols - 1)

    sends = []
    offsets = [n // 2]
    for i in range(1, n // 2):
        offsets += [n // 2 - i, n // 2 + i]

    def launch(copy):
        copy.start()
        sends.append(copy)

    def heads_send(t, source, target):
        for i in offsets:
            d = lax.rem(me + i, n)
            launch(remote(
                source.at[:, head_cols(d)], target.at[rows(me)],
                heads_s.at[t, i], heads_r.at[t, i], {"cp": d},
            ))

    def heads_arrival(t, i, target):
        source = lax.rem(me + n - i, n)
        block = target.at[rows(source)]
        remote(block, block, heads_s.at[t, i], heads_r.at[t, i], {"cp": source}).wait_recv()

    def heads_wait(t, target):
        for i in offsets:
            heads_arrival(t, i, target)

    def out_copy(t, i, source, target, place):
        d = lax.rem(me + i, n)
        return remote(
            source.at[rows(d)], target.at[:, cols_at(place)],
            out_s.at[t, i], out_r.at[t, i], {"cp": d},
        )

    def out_send(t, source, target, place):
        for i in offsets:
            launch(out_copy(t, i, source, target, place))

    def out_wait(t, target, place_of):
        for i in offsets:
            source = lax.rem(me + n - i, n)
            block = target.at[:, cols_at(place_of(source))]
            remote(block, block, out_s.at[t, i], out_r.at[t, i], {"cp": source}).wait_recv()

    def spot_of(d):
        return spot(lax.rem(d, 2), d // 2)

    def w_head(y, plane):
        return wall.at[rows_of(spot(y, plane) * HEAD, HEAD)]

    def w_pair(y, c):
        return wall.at[rows_of(spot(y, 2 * c) * HEAD, 2 * HEAD)]

    own_slab = rows_of(spot(why, zed) * HEAD + col * slab, slab)
    slab_copy = remote(
        w, wall.at[own_slab], slab_s.at[0], slab_r.at[col],
        {"fsdp": 2 * lax.rem(zed, 2) + zed // 2},
    )

    @pl.when(jnp.logical_not(root))
    def _():
        slab_copy.start()

    heads_send(0, k, kh)
    mine_up = ups.at[rows(2 * core + why)]
    launch(remote(up, mine_up, up_s.at[0], up_r.at[0], mate))
    launch(remote(up, mine_up, up_s.at[1], up_r.at[1], beside))

    gateway = jnp.logical_and(jnp.logical_not(keeper), zed == 1 + zed // 2)
    to_pair = jnp.logical_or(root, gateway)
    pair = 2 * (zed + 1 - 2 * lax.rem(zed, 2)) + why

    def piece_of(plane, p):
        return wall.at[rows_of(spot(why, plane) * HEAD + p * piece_rows, piece_rows)]

    def chain_copy(p, way):
        block = piece_of(home, p)
        target = pair if way == 0 else 2 * (2 - core) + why
        return remote(block, block, chain_s.at[way, p], chain_r.at[p], {"cp": target})

    def chain_forward(p):
        @pl.when(root)
        def _():
            chain_copy(p, 1).start()

        @pl.when(to_pair)
        def _():
            chain_copy(p, 0).start()

        block = piece_of(home, p)
        remote(block, block, side_s.at[p], side_r.at[p], across).start()

    @pl.when(root)
    def _():
        wall[own_slab] = w[...]
        for j in range(1, cols):
            other = lax.rem(col + j, cols)
            block = wall.at[rows_of(spot(why, zed) * HEAD + other * slab, slab)]
            remote(block, block, slab_s.at[0], slab_r.at[other], {"fsdp": other}).wait_recv()
        for p in range(pieces):
            chain_forward(p)

    heads_send(1, q, qh)
    for source, target in ((k, kh), (q, qh), (v, vh)):
        target[rows(me)] = source[:, head_cols(me)]
    ups[rows(2 * core + why)] = up[...]

    spans = order.shape[0]
    order_row = jnp.broadcast_to(order[...].reshape(1, spans), (spans, spans))
    place = lax.broadcasted_iota(jnp.int32, (spans, spans), 0)
    at_place = (order_row == place).astype(f32).astype(bf16)
    row = lax.broadcasted_iota(jnp.int32, (spans, length), 1)
    line = lax.broadcasted_iota(jnp.int32, (spans, length), 0)
    begin = line * span_rows
    member = jnp.logical_and(row >= begin, row < begin + span_rows).astype(f32)
    placed = jnp.dot(at_place, member.astype(bf16), preferred_element_type=f32)
    within = (row - begin).astype(f32) * member
    query_pos = (placed * begin.astype(f32) + within).sum(0, keepdims=True)
    key_pos = jnp.broadcast_to(query_pos, (8, length)).T[:, :1]
    placed_low = placed.astype(bf16)
    key_side = jnp.dot(
        mask[...].astype(f32).astype(bf16), placed_low, preferred_element_type=f32
    ).T.astype(bf16)
    for o in range(n):
        part = slice(o * tokens, (o + 1) * tokens)
        seen = jnp.dot(key_side, placed_low[:, part], preferred_element_type=f32)
        allowed = jnp.logical_and(seen > 0.5, key_pos <= query_pos[:, part])
        bias[:, part] = jnp.where(allowed, 0.0, lowest)

    def chain_relay(p):
        @pl.when(jnp.logical_not(root))
        def _():
            block = piece_of(home, p)
            remote(block, block, chain_s.at[0, p], chain_r.at[p], {"cp": me}).wait_recv()
            chain_forward(p)

    heads_wait(0, kh)
    heads_send(2, v, vh)
    kt[...] = kh[...].astype(f32).T.astype(bf16)
    for p in range(pieces // 2):
        chain_relay(p)
    beside_up = ups.at[rows(2 * core + 1 - why)]
    remote(beside_up, beside_up, up_s.at[1], up_r.at[1], beside).wait_recv()
    launch(remote(beside_up, beside_up, up_s.at[2], up_r.at[2], mate))
    for p in range(pieces // 2, pieces):
        chain_relay(p)

    for p in range(pieces):
        block = piece_of(2 * core + 1 - ex, p)
        remote(block, block, side_s.at[p], side_r.at[p], across).wait_recv()

    def seq_copy(ss, rs, slot, source, target, j, c):
        return remote(
            source, target, ss.at[slot], rs.at[zed], {"cp": 2 * (2 * core + j) + why, "fsdp": 2 * ex + c}
        )

    def seq_send(copy, here, j, i):
        if i:
            launch(copy)
            return
        stays = 2 * core + j == zed

        @pl.when(stays)
        def _():
            here()

        @pl.when(jnp.logical_not(stays))
        def _():
            copy.start()

    def seq_settle(copy, j):
        @pl.when(2 * core + j != zed)
        def _():
            copy.wait_send()

    def seq_wait(ss, rs, block_of):
        for i in range(planes):
            source = lax.rem(zed + i, planes)
            block = block_of(source)
            arrived = remote(block, block, ss.at[0], rs.at[source], {"cp": me})
            if i == 0:
                @pl.when(jnp.logical_not(keeper))
                def _():
                    arrived.wait_recv()
            else:
                arrived.wait_recv()

    def ga_copy(i, j):
        c = core if i == 0 else 1 - core
        return seq_copy(
            ga_s, ga_r, 2 * i + j,
            ga_out.at[j, two_rows(c)], ga.at[two_rows(zed)], j, c,
        )

    def ga_group(i):
        c = core if i == 0 else 1 - core
        weight = wall[rows_of(spot(why, 2 * core) * HEAD, 2 * HEAD)]
        result = lax.dot_general(
            ups[two_rows(c)], weight, nt, preferred_element_type=f32
        ).astype(bf16)
        for j in range(2):
            ga_out[j, two_rows(c)] = result[:, j * HEAD:(j + 1) * HEAD]

            def here(j=j):
                ga[two_rows(zed)] = result[:, j * HEAD:(j + 1) * HEAD]

            seq_send(ga_copy(i, j), here, j, i)

    ga_group(0)
    for slot, y in ((0, why), (2, 1 - why)):
        block = ups.at[rows(2 * (1 - core) + y)]
        remote(block, block, up_s.at[slot], up_r.at[slot], mate).wait_recv()
    ga_group(1)
    launch(remote(w_pair(why, core), w_pair(why, core), wide_s.at[0], wide_r.at[0], mate))
    launch(remote(w_head(why, home), w_head(why, home), wide_s.at[1], wide_r.at[1], beside))

    def soft(i, carry):
        @pl.when(i > 0)
        def _():
            heads_arrival(1, i, qh)

        part = rows(lax.rem(me + n - i, n))
        scores = lax.dot_general(kh[...], qh[part], nt, preferred_element_type=f32) * (1.0 / HEAD)
        scores = scores + bias[:, part]
        terms = jnp.exp(scores - scores.max(0, keepdims=True))
        probability = terms * (1.0 / terms.sum(0, keepdims=True))
        prob[:, part] = probability.astype(bf16)
        return carry

    lax.fori_loop(0, n, soft, 0)

    heads_wait(2, vh)
    vt[...] = vh[...].astype(f32).T.astype(bf16)

    def attend(o, carry):
        part = two_rows(o)
        att_t = jnp.dot(vt[...], prob[:, part], preferred_element_type=f32)
        att[part] = att_t.T.astype(bf16)
        return carry

    lax.fori_loop(0, n // 2, attend, 0)
    out_send(0, att, attended, spot_of(me))
    attended[:, cols_at(spot_of(me))] = att[rows(me)]
    seq_wait(ga_s, ga_r, lambda source: ga.at[two_rows(source)])

    def value_step(o, carry):
        part = two_rows(o)
        dvh[part] = jnp.dot(prob[part], ga[...], preferred_element_type=f32).astype(bf16)
        return carry

    lax.fori_loop(0, n // 2, value_step, 0)
    out_send(2, dvh, dv, me)
    dv[:, head_cols(me)] = dvh[rows(me)]

    block = w_head(1 - why, home)
    remote(block, block, wide_s.at[1], wide_r.at[1], beside).wait_recv()
    launch(remote(block, block, wide_s.at[2], wide_r.at[2], across))
    launch(remote(block, block, wide_s.at[3], wide_r.at[3], mate))

    def backward(i, carry):
        i = lax.rem(i + n // 2, n)
        o = lax.rem(me + i, n)
        part = rows(o)
        ga_rows = ga[part]
        delta = (att[part].astype(f32) * ga_rows.astype(f32)).T.sum(0, keepdims=True)
        dprob = lax.dot_general(vh[...], ga_rows, nt, preferred_element_type=f32)
        ds = (prob[:, part].astype(f32) * ((dprob - delta) * (1.0 / HEAD))).astype(bf16)
        dsb[:, part] = ds
        dqh[part] = jnp.dot(kt[...], ds, preferred_element_type=f32).T.astype(bf16)

        @pl.when(i > 0)
        def _():
            out_copy(3, i, dqh, dq, me).start()

        return carry

    lax.fori_loop(0, n, backward, 0)
    dq[:, head_cols(me)] = dqh[rows(me)]

    out_wait(0, attended, spot_of)
    for i in range(2):
        for j in range(2):
            y = why if i == 0 else 1 - why
            c = core if j == 0 else 1 - core
            part = rows_of(spot(y, 2 * c) * HEAD, 2 * HEAD)
            if i == 0 and j == 0:
                attp[rows(2 * core + why)] = attended[:, part]
                continue
            launch(remote(
                attended.at[:, part], attp.at[rows(2 * core + why)],
                attp_s.at[2 * i + j], attp_r.at[2 * i + j],
                {"cp": 2 * zed + y, "fsdp": 2 * ex + c},
            ))

    def key_step(o, carry):
        part = two_rows(o)
        dkh[part] = jnp.dot(dsb[part], qh[...], preferred_element_type=f32).astype(bf16)
        return carry

    lax.fori_loop(0, n // 2, key_step, 0)
    out_send(1, dkh, dk, me)
    dk[:, head_cols(me)] = dkh[rows(me)]

    for i in range(2):
        for j in range(2):
            if i == 0 and j == 0:
                continue
            y = why if i == 0 else 1 - why
            c = core if j == 0 else 1 - core
            block = attp.at[rows(2 * c + y)]
            remote(
                block, block, attp_s.at[2 * i + j], attp_r.at[2 * i + j], {"cp": me}
            ).wait_recv()
    att_t = attp[...].astype(f32).T.astype(bf16)
    width = math.gcd(proj.shape[1], 512)

    def weigh(i, carry):
        part = rows_of(i * width, width)
        dw[:, part] = jnp.dot(att_t, ups[:, part], preferred_element_type=f32).astype(bf16)
        return carry

    lax.fori_loop(0, proj.shape[1] // width, weigh, 0)
    share = 2 * slab

    def dw_rows(j, x):
        return rows_of(j * HEAD + x * share, share)

    for j in range(2):
        launch(remote(
            dw.at[dw_rows(j, 1 - ex)], dwx.at[j], dwx_s.at[j], dwx_r.at[j], across
        ))

    def dw_copy(i, j):
        c = core if i == 0 else 1 - core
        return seq_copy(
            dw_s, dw_r, 2 * i + j, dwz.at[j, rows_of(c * slab, slab)], dwr.at[zed], j, c
        )

    for j in range(2):
        remote(dwx.at[j], dwx.at[j], dwx_s.at[j], dwx_r.at[j], across).wait_recv()
        dwz[j] = (dw[dw_rows(j, ex)].astype(f32) + dwx[j].astype(f32)).astype(bf16)
        for i in range(2):
            def here(j=j):
                dwr[zed] = dwz[j, rows_of(core * slab, slab)]

            seq_send(dw_copy(i, j), here, j, i)

    block = w_head(1 - why, 2 * core + 1 - ex)
    remote(block, block, wide_s.at[2], wide_r.at[2], across).wait_recv()
    launch(remote(block, block, wide_s.at[4], wide_r.at[4], mate))
    for slot, block in (
        (0, w_pair(why, 1 - core)),
        (3, w_head(1 - why, 2 * (1 - core) + ex)),
        (4, w_head(1 - why, 2 * (1 - core) + 1 - ex)),
    ):
        remote(block, block, wide_s.at[slot], wide_r.at[slot], mate).wait_recv()

    def project(i, carry):
        part = rows_of(i * width, width)
        proj[:, part] = jnp.dot(
            attended[...], wall[:, part], preferred_element_type=f32
        ).astype(bf16)
        return carry

    lax.fori_loop(0, proj.shape[1] // width, project, 0)
    seq_wait(dw_s, dw_r, lambda source: dwr.at[source])
    total = dwr[0].astype(f32)
    for j in range(1, planes):
        total = total + dwr[j].astype(f32)
    wg[...] = total
    out_wait(2, dv, lambda d: d)
    out_wait(3, dq, lambda d: d)
    out_wait(1, dk, lambda d: d)
    for copy in sends:
        copy.wait_send()
    for i in offsets:
        out_copy(3, i, dqh, dq, me).wait_send()

    @pl.when(jnp.logical_not(root))
    def _():
        slab_copy.wait_send()

    for j in range(2):
        seq_settle(ga_copy(0, j), j)
        seq_settle(dw_copy(0, j), j)

    for p in range(pieces):
        block = piece_of(home, p)
        remote(block, block, side_s.at[p], side_r.at[p], across).wait_send()

        @pl.when(to_pair)
        def _():
            chain_copy(p, 0).wait_send()

        @pl.when(root)
        def _():
            chain_copy(p, 1).wait_send()


def deliver_kernel(*refs):
    count = len(refs) // 2
    copies = [
        pltpu.make_async_copy(refs[t], refs[count + t], refs[-1].at[t]) for t in range(count)
    ]
    for copy in copies:
        copy.start()
    for copy in copies:
        copy.wait()


def by_heads(query_states, key_states, value_states, span_order, block_mask, output_weight, upstream):
    n = lax.axis_size("cp")
    m = lax.axis_size("fsdp")
    tokens, width = query_states.shape[1:]
    length = tokens * n
    model = upstream.shape[2]
    slab = output_weight.shape[0]
    bf16, f32 = jnp.bfloat16, jnp.float32
    shape = jax.ShapeDtypeStruct
    vmem = pl.BlockSpec(memory_space=pltpu.VMEM)
    dma = pltpu.SemaphoreType.DMA
    planes = n // 2
    pieces = 4
    head_array = pltpu.VMEM((length, HEAD), bf16)
    square = pltpu.VMEM((length, length), bf16)
    projected, dq, dk, dv, weight_gradient = pl.pallas_call(
        lambda *refs: layer_kernel(n, *refs),
        out_shape=(shape((tokens, model), bf16),)
        + (shape((tokens, width), bf16),) * 3
        + (shape((slab, model), f32),),
        in_specs=[pl.BlockSpec(memory_space=pltpu.HBM)] * 7,
        out_specs=(vmem,) * 5,
        scratch_shapes=[
            pltpu.VMEM((tokens, width), bf16), pltpu.VMEM((tokens, width), bf16),
            pltpu.VMEM((tokens, width), bf16), pltpu.VMEM((tokens, model), bf16),
            pltpu.VMEM((slab, model), bf16), pltpu.VMEM(span_order.shape, jnp.int32),
            pltpu.VMEM(block_mask.shape, jnp.int32), dma((7,)),
            head_array, head_array, head_array,
            pltpu.VMEM((4 * tokens, model), bf16), pltpu.VMEM((width, model), bf16),
            pltpu.VMEM((length, length), f32), square, square,
            head_array, pltpu.VMEM((tokens, width), bf16),
            pltpu.VMEM((4 * tokens, 2 * HEAD), bf16), pltpu.VMEM((2, 4 * tokens, HEAD), bf16),
            head_array, head_array, head_array, head_array,
            pltpu.VMEM((2 * HEAD, model), bf16), pltpu.VMEM((2, 2 * slab, model), bf16),
            pltpu.VMEM((2, 2 * slab, model), bf16), pltpu.VMEM((planes, slab, model), bf16),
            pltpu.VMEM((HEAD, length), bf16), pltpu.VMEM((HEAD, length), bf16),
            dma((3, n)), dma((3, n)), dma((4, n)), dma((4, n)),
            dma((3,)), dma((3,)), dma((5,)), dma((5,)),
            dma((1,)), dma((m,)), dma((2, pieces)), dma((pieces,)), dma((pieces,)), dma((pieces,)),
            dma((4,)), dma((planes,)), dma((4,)), dma((4,)),
            dma((2,)), dma((2,)), dma((4,)), dma((planes,)),
        ],
        compiler_params=pltpu.CompilerParams(
            collective_id=0, has_side_effects=True, vmem_limit_bytes=48 << 20
        ),
        name="layer",
    )(
        *(
            pltpu.with_memory_space_constraint(a, pltpu.HBM)
            for a in (
                query_states[0], key_states[0], value_states[0], upstream[0], output_weight,
                span_order, block_mask,
            )
        ),
    )
    results = (projected, dq, dk, dv, weight_gradient)
    projected, dq, dk, dv, weight_gradient = pl.pallas_call(
        deliver_kernel,
        out_shape=tuple(shape(r.shape, r.dtype) for r in results),
        in_specs=[pl.BlockSpec(memory_space=pl.ANY)] * 5,
        out_specs=(pl.BlockSpec(memory_space=pl.ANY),) * 5,
        scratch_shapes=[dma((5,))],
        compiler_params=pltpu.CompilerParams(vmem_limit_bytes=1 << 20),
        name="deliver",
    )(*results)
    return (projected[None], dq[None], dk[None], dv[None], weight_gradient)


def solution(mesh):
    fits = mesh.shape["cp"] == HEADS and mesh.shape["fsdp"] == 4
    return jax.shard_map(
        by_heads if fits else local,
        mesh=mesh,
        in_specs=(
            P("fsdp", "cp", None),
            P("fsdp", "cp", None),
            P("fsdp", "cp", None),
            P(),
            P(),
            P(("cp", "fsdp"), None),
            P("fsdp", "cp", None),
        ),
        out_specs=(
            P("fsdp", "cp", None),
            P("fsdp", "cp", None),
            P("fsdp", "cp", None),
            P("fsdp", "cp", None),
            P(("cp", "fsdp"), None),
        ),
        check_vma=False,
    )
```

```python
import math

import jax
import jax.numpy as jnp
from jax import lax
from jax.experimental import pallas as pl
from jax.experimental.pallas import tpu as pltpu
from jax.sharding import PartitionSpec as P

HEADS = 8
HEAD = 128


lowest = -1e30


def split_heads(row_block):
    return row_block.reshape(row_block.shape[0], HEADS, HEAD)


def pair_scores(query_rows, key_rows):
    return jnp.einsum(
        "qhd,khd->hqk",
        split_heads(query_rows),
        split_heads(key_rows),
        preferred_element_type=jnp.float32,
    ) * (1.0 / HEAD)


def storage_mask(span_order, block_mask):
    span_count = span_order.shape[0]
    onehot = (span_order[:, None] == jnp.arange(span_count, dtype=jnp.int32)[None, :]).astype(
        jnp.float32
    )
    permuted = jnp.dot(jnp.dot(onehot, block_mask.astype(jnp.float32)), onehot.T)
    return permuted > 0.5


def allowed_block(span_ok, positions, query_begin, query_total, key_begin, key_total, span_rows):
    span_sub = lax.dynamic_slice(
        span_ok,
        (query_begin // span_rows, key_begin // span_rows),
        (query_total // span_rows, key_total // span_rows),
    )
    spread = jnp.broadcast_to(
        span_sub[:, None, :, None],
        (query_total // span_rows, span_rows, key_total // span_rows, span_rows),
    )
    spread = spread.reshape(query_total, key_total)
    query_pos = lax.dynamic_slice_in_dim(positions, query_begin, query_total)
    key_pos = lax.dynamic_slice_in_dim(positions, key_begin, key_total)
    return spread & (key_pos[None, :] <= query_pos[:, None])


def local_terms(query_rows, grad_rows, log_rows, delta_rows, key_rows, value_rows, allowed):
    scores = pair_scores(query_rows, key_rows)
    probability = jnp.where(allowed[None], jnp.exp(scores - log_rows[..., None]), 0.0)
    dprob = jnp.einsum(
        "qhd,khd->hqk",
        split_heads(grad_rows),
        split_heads(value_rows),
        preferred_element_type=jnp.float32,
    )
    dscores = (probability * (dprob - delta_rows[..., None]) * (1.0 / HEAD)).astype(jnp.bfloat16)
    return (probability, dscores)


def local(query_states, key_states, value_states, span_order, block_mask, output_weight, upstream):
    query_rows = query_states[0]
    key_local = key_states[0]
    value_local = value_states[0]
    upstream_rows = upstream[0]
    tokens = query_rows.shape[0]
    span_rows = tokens // 2
    positions = (
        span_order[:, None] * span_rows + jnp.arange(span_rows, dtype=jnp.int32)[None, :]
    ).reshape(-1)
    span_ok = storage_mask(span_order, block_mask)
    own_start = lax.axis_index("cp") * tokens
    key_all, value_all = (
        lax.all_gather(key_local, "cp", axis=0, tiled=True),
        lax.all_gather(value_local, "cp", axis=0, tiled=True),
    )
    weight = lax.all_gather(output_weight, ("cp", "fsdp"), axis=0, tiled=True)
    length = key_all.shape[0]
    key_block = math.gcd(length, 512)
    block_count = length // key_block
    block_steps = jnp.arange(block_count, dtype=jnp.int32)

    def stats_step(running, step_index):
        key_begin = step_index * key_block
        key_rows = lax.dynamic_slice_in_dim(key_all, key_begin, key_block)
        allowed = allowed_block(
            span_ok, positions, own_start, tokens, key_begin, key_block, span_rows
        )
        maxima, totals = running
        scores = pair_scores(query_rows, key_rows)
        masked = jnp.where(allowed[None], scores, lowest)
        new_max = jnp.maximum(maxima, masked.max(-1))
        exp_terms = jnp.where(allowed[None], jnp.exp(scores - new_max[..., None]), 0.0)
        return ((new_max, totals * jnp.exp(maxima - new_max) + exp_terms.sum(-1)), None)

    stat_start = (
        jnp.full((HEADS, tokens), lowest, jnp.float32),
        jnp.zeros((HEADS, tokens), jnp.float32),
    )
    (maxima, totals), _ = lax.scan(stats_step, stat_start, block_steps)
    log_total = maxima + jnp.log(totals)

    def output_step(attn_sum, step_index):
        key_begin = step_index * key_block
        key_rows = lax.dynamic_slice_in_dim(key_all, key_begin, key_block)
        value_rows = lax.dynamic_slice_in_dim(value_all, key_begin, key_block)
        allowed = allowed_block(
            span_ok, positions, own_start, tokens, key_begin, key_block, span_rows
        )
        scores = pair_scores(query_rows, key_rows)
        probability = jnp.where(allowed[None], jnp.exp(scores - log_total[..., None]), 0.0)
        return (
            attn_sum
            + jnp.einsum(
                "hqk,khd->qhd",
                probability.astype(jnp.bfloat16),
                split_heads(value_rows),
                preferred_element_type=jnp.float32,
            ),
            None,
        )

    zero_heads = jnp.zeros((tokens, HEADS, HEAD), jnp.float32)
    attn_sum, _ = lax.scan(output_step, zero_heads, block_steps)
    attended = lax.optimization_barrier(attn_sum.reshape(tokens, -1).astype(jnp.bfloat16))
    projected = jnp.dot(attended, weight, preferred_element_type=jnp.float32).astype(jnp.bfloat16)
    grad_attended = lax.dot_general(
        upstream_rows, weight, (((1,), (1,)), ((), ())), preferred_element_type=jnp.float32
    ).astype(jnp.bfloat16)
    grad_attended = lax.optimization_barrier(grad_attended)
    weight_term = lax.dot_general(
        attended, upstream_rows, (((0,), (0,)), ((), ())), preferred_element_type=jnp.float32
    )
    row_delta = (
        (grad_attended.astype(jnp.float32) * attended.astype(jnp.float32))
        .reshape(tokens, HEADS, HEAD)
        .sum(-1)
    )
    delta_heads = row_delta.T

    def query_step(grad_sum, step_index):
        key_begin = step_index * key_block
        key_rows = lax.dynamic_slice_in_dim(key_all, key_begin, key_block)
        value_rows = lax.dynamic_slice_in_dim(value_all, key_begin, key_block)
        allowed = allowed_block(
            span_ok, positions, own_start, tokens, key_begin, key_block, span_rows
        )
        probability, dscores = local_terms(
            query_rows, grad_attended, log_total, delta_heads, key_rows, value_rows, allowed
        )
        return (
            grad_sum
            + jnp.einsum(
                "hqk,khd->qhd", dscores, split_heads(key_rows), preferred_element_type=jnp.float32
            ),
            None,
        )

    query_sum, _ = lax.scan(query_step, zero_heads, block_steps)
    query_gradient = query_sum.reshape(tokens, -1).astype(jnp.bfloat16)
    log_all, delta_all = (
        lax.all_gather(log_total.T, "cp", axis=0, tiled=True),
        lax.all_gather(row_delta, "cp", axis=0, tiled=True),
    )
    sums_now = (zero_heads, zero_heads)
    query_piece = lax.all_gather(query_rows, "cp", axis=0, tiled=True)
    grad_piece = lax.all_gather(grad_attended, "cp", axis=0, tiled=True)
    row_count = query_piece.shape[0]
    sources = row_count // tokens
    group_size = math.gcd(sources, max(1, 512 // tokens))
    group_rows = group_size * tokens

    def group_step(running, step_index):
        offset = step_index * group_rows
        query_group = lax.dynamic_slice_in_dim(query_piece, offset, group_rows)
        grad_group = lax.dynamic_slice_in_dim(grad_piece, offset, group_rows)
        log_group = lax.dynamic_slice_in_dim(log_all, offset, group_rows).T
        delta_group = lax.dynamic_slice_in_dim(delta_all, offset, group_rows).T
        allowed = allowed_block(
            span_ok, positions, offset, group_rows, own_start, tokens, span_rows
        )
        key_sum, value_sum = running
        probability, dscores = local_terms(
            query_group, grad_group, log_group, delta_group, key_local, value_local, allowed
        )
        probability_low = probability.astype(jnp.bfloat16).reshape(
            HEADS, group_size, tokens, tokens
        )
        dscores_group = dscores.reshape(HEADS, group_size, tokens, tokens)
        qsplit = query_group.reshape(group_size, tokens, HEADS, HEAD)
        gsplit = grad_group.reshape(group_size, tokens, HEADS, HEAD)
        key_part = jnp.einsum(
            "hgqk,gqhd->gkhd", dscores_group, qsplit, preferred_element_type=jnp.float32
        ).astype(jnp.bfloat16)
        value_part = jnp.einsum(
            "hgqk,gqhd->gkhd", probability_low, gsplit, preferred_element_type=jnp.float32
        ).astype(jnp.bfloat16)
        key_part, value_part = lax.optimization_barrier((key_part, value_part))
        return (
            (
                key_sum + key_part.astype(jnp.float32).sum(0),
                value_sum + value_part.astype(jnp.float32).sum(0),
            ),
            None,
        )

    sums_now, _ = lax.scan(group_step, sums_now, jnp.arange(sources // group_size, dtype=jnp.int32))
    key_sum, value_sum = sums_now
    key_gradient = key_sum.reshape(tokens, -1).astype(jnp.bfloat16)
    value_gradient = value_sum.reshape(tokens, -1).astype(jnp.bfloat16)
    cycle_count = lax.axis_size("cp")
    batch_count = lax.axis_size("fsdp")
    slab_rows = weight_term.shape[0] // (cycle_count * batch_count)
    reordered = weight_term.reshape(cycle_count, batch_count, slab_rows, -1).transpose(1, 0, 2, 3)
    reordered = reordered.reshape(weight_term.shape[0], -1)
    partial_batch = lax.psum_scatter(
        reordered.astype(jnp.bfloat16), "fsdp", scatter_dimension=0, tiled=True
    )
    weight_gradient = lax.psum_scatter(partial_batch, "cp", scatter_dimension=0, tiled=True).astype(
        jnp.float32
    )
    return (
        projected[None],
        query_gradient[None],
        key_gradient[None],
        value_gradient[None],
        weight_gradient,
    )


MESH = pl.DeviceIdType.MESH


def remote(src, dst, send_sem, recv_sem, device):
    return pltpu.make_async_remote_copy(
        src_ref=src,
        dst_ref=dst,
        send_sem=send_sem,
        recv_sem=recv_sem,
        device_id=device,
        device_id_type=MESH,
    )


def rows_of(begin, count):
    return pl.ds(pl.multiple_of(begin, count), count)


def greet(devices):
    barrier = pltpu.get_barrier_semaphore()
    for device in devices:
        pl.semaphore_signal(barrier, inc=1, device_id=device, device_id_type=MESH)
    pl.semaphore_wait(barrier, len(devices))


def layer_kernel(
    n, q_in, k_in, v_in, up_in, w_in, order_in, mask_in, proj, dq, dk, dv, wg,
    q, k, v, up, w, order, mask, load,
    qh, kh, vh, ups, wall, bias, prob, dsb, att, attp, ga_out, ga,
    dqh, dkh, dvh, dw, dwx, dwz, dwp, dwr, kt, vt, mix, mix_mate, mix_send, mix_beside,
    heads_s, heads_r, out_s, out_r, up_s, up_r,
    slab_s, slab_r, pass_s, side_s, side_r, ga_s, ga_r, att_s, att_r,
    dwx_s, dwx_r, lift_s, lift_r, dw_s, dw_r, mix_s, mix_r,
):
    me = lax.axis_index("cp")
    col = lax.axis_index("fsdp")
    cols = lax.axis_size("fsdp")
    planes = n // 2
    zed, why = me // 2, lax.rem(me, 2)
    ex, core = col // 2, lax.rem(col, 2)
    mate = {"fsdp": 2 * ex + 1 - core}
    across = {"fsdp": 2 * (1 - ex) + core}
    beside = {"cp": 2 * zed + 1 - why}
    tokens = up.shape[0]
    slab = w.shape[0]
    length = tokens * n
    span_rows = tokens // 2
    bf16, f32 = jnp.bfloat16, jnp.float32
    nt = (((1,), (1,)), ((), ()))
    home = 2 * core + ex
    root = home == zed
    keeper = core == zed // 2
    gateway = jnp.logical_and(jnp.logical_not(keeper), zed == 1 + zed // 2)
    pair = 2 * (zed + 1 - 2 * lax.rem(zed, 2)) + why

    def head_cols(d):
        return rows_of(d * HEAD, HEAD)

    def rows(d):
        return rows_of(d * tokens, tokens)

    def two_rows(d):
        return rows_of(d * 2 * tokens, 2 * tokens)

    pairs = (
        (k_in, k), (up_in, up), (w_in, w), (q_in, q), (v_in, v), (order_in, order), (mask_in, mask)
    )
    loads = [pltpu.make_async_copy(a, b, load.at[t]) for t, (a, b) in enumerate(pairs)]
    for copy in loads:
        copy.start()
    barrier = pltpu.get_barrier_semaphore()
    for i in range(n):
        for j in range(cols):
            if i or j:
                pl.semaphore_signal(
                    barrier, inc=1,
                    device_id={"cp": lax.rem(me + i, n), "fsdp": lax.rem(col + j, cols)},
                    device_id_type=MESH,
                )
    for copy in loads:
        copy.wait()
    pl.semaphore_wait(barrier, n * cols - 1)

    sends = []
    offsets = [n // 2]
    for i in range(1, n // 2):
        offsets += [n // 2 - i, n // 2 + i]

    def launch(copy):
        copy.start()
        sends.append(copy)

    def heads_send(t, source, target):
        for i in offsets:
            d = lax.rem(me + i, n)
            launch(remote(
                source.at[:, head_cols(d)], target.at[rows(me)],
                heads_s.at[t, i], heads_r.at[t, i], {"cp": d},
            ))

    def heads_arrival(t, i, target):
        source = lax.rem(me + n - i, n)
        block = target.at[rows(source)]
        remote(block, block, heads_s.at[t, i], heads_r.at[t, i], {"cp": source}).wait_recv()

    def heads_wait(t, target):
        for i in offsets:
            heads_arrival(t, i, target)

    def out_copy(t, i, source, target):
        d = lax.rem(me + i, n)
        return remote(
            source.at[rows(d)], target.at[:, head_cols(me)],
            out_s.at[t, i], out_r.at[t, i], {"cp": d},
        )

    def out_send(t, source, target):
        for i in offsets:
            launch(out_copy(t, i, source, target))

    def out_wait(t, target):
        for i in offsets:
            source = lax.rem(me + n - i, n)
            block = target.at[:, head_cols(source)]
            remote(block, block, out_s.at[t, i], out_r.at[t, i], {"cp": source}).wait_recv()

    own_slab = rows_of(lax.rem(zed, 2) * HEAD + col * slab, slab)
    slab_copies = [
        remote(
            w, wall.at[own_slab], slab_s.at[i], slab_r.at[col],
            {"cp": target, "fsdp": 2 * lax.rem(zed, 2) + zed // 2},
        )
        for i, target in enumerate((me, pair, 2 * (2 - zed // 2) + why))
    ]
    launch(slab_copies[2])

    @pl.when(jnp.logical_not(root))
    def _():
        slab_copies[0].start()

    launch(slab_copies[1])
    mine_up = ups.at[rows(2 * core + why)]
    launch(remote(up, mine_up, up_s.at[1], up_r.at[1], beside))
    heads_send(0, k, kh)
    launch(remote(up, mine_up, up_s.at[0], up_r.at[0], mate))
    heads_send(1, q, qh)

    @pl.when(root)
    def _():
        wall[own_slab] = w[...]

    def piece_of(plane, p):
        return wall.at[rows_of(lax.rem(plane, 2) * HEAD + p * slab, slab)]

    def pass_copy(p):
        block = piece_of(home, p)
        return remote(block, block, pass_s.at[p], slab_r.at[p], {"cp": pair})

    def side_copy(p):
        block = piece_of(home, p)
        return remote(block, block, side_s.at[p], side_r.at[p], across)

    def piece_poll(p):
        @pl.when(jnp.logical_not(jnp.logical_and(root, col == p)))
        def _():
            block = piece_of(home, p)
            remote(block, block, slab_s.at[0], slab_r.at[p], mate).wait_recv()

        @pl.when(gateway)
        def _():
            pass_copy(p).start()

        side_copy(p).start()

    for source, target in ((k, kh), (q, qh), (v, vh)):
        target[rows(me)] = source[:, head_cols(me)]
    ups[rows(2 * core + why)] = up[...]

    spans = order.shape[0]
    order_row = jnp.broadcast_to(order[...].reshape(1, spans), (spans, spans))
    place = lax.broadcasted_iota(jnp.int32, (spans, spans), 0)
    at_place = (order_row == place).astype(f32).astype(bf16)
    row = lax.broadcasted_iota(jnp.int32, (spans, length), 1)
    line = lax.broadcasted_iota(jnp.int32, (spans, length), 0)
    begin = line * span_rows
    member = jnp.logical_and(row >= begin, row < begin + span_rows).astype(f32)
    placed = jnp.dot(at_place, member.astype(bf16), preferred_element_type=f32)
    within = (row - begin).astype(f32) * member
    query_pos = (placed * begin.astype(f32) + within).sum(0, keepdims=True)
    key_pos = jnp.broadcast_to(query_pos, (8, length)).T[:, :1]
    placed_low = placed.astype(bf16)
    key_side = jnp.dot(
        mask[...].astype(f32).astype(bf16), placed_low, preferred_element_type=f32
    ).T.astype(bf16)
    for o in range(n):
        part = slice(o * tokens, (o + 1) * tokens)
        seen = jnp.dot(key_side, placed_low[:, part], preferred_element_type=f32)
        allowed = jnp.logical_and(seen > 0.5, key_pos <= query_pos[:, part])
        bias[:, part] = jnp.where(allowed, 0.0, lowest)

    far = jnp.logical_not(jnp.logical_or(keeper, gateway))

    @pl.when(jnp.logical_not(far))
    def _():
        for p in range(cols):
            piece_poll(p)

    heads_send(2, v, vh)
    heads_wait(0, kh)
    kt[...] = kh[...].astype(f32).T.astype(bf16)
    beside_up = ups.at[rows(2 * core + 1 - why)]
    remote(beside_up, beside_up, up_s.at[1], up_r.at[1], beside).wait_recv()
    launch(remote(beside_up, beside_up, up_s.at[2], up_r.at[2], mate))
    @pl.when(far)
    def _():
        for p in range(cols // 2):
            piece_poll(p)

    def soft(i, carry):
        @pl.when(i > 0)
        def _():
            heads_arrival(1, i, qh)

        part = rows(lax.rem(me + n - i, n))
        scores = lax.dot_general(kh[...], qh[part], nt, preferred_element_type=f32) * (1.0 / HEAD)
        scores = scores + bias[:, part]
        terms = jnp.exp(scores - scores.max(0, keepdims=True))
        probability = terms * (1.0 / terms.sum(0, keepdims=True))
        prob[:, part] = probability.astype(bf16)
        return carry

    lax.fori_loop(0, n, soft, 0)

    def seq_copy(ss, rs, slot, source, target, j, c):
        return remote(
            source, target, ss.at[slot], rs.at[zed], {"cp": 2 * (2 * core + j) + why, "fsdp": 2 * ex + c}
        )

    def seq_send(copy, here, j, i):
        if i:
            copy.start()
            return
        stays = 2 * core + j == zed

        @pl.when(stays)
        def _():
            here()

        @pl.when(jnp.logical_not(stays))
        def _():
            copy.start()

    def seq_settle(copy, j):
        @pl.when(2 * core + j != zed)
        def _():
            copy.wait_send()

    def seq_wait(ss, rs, block_of):
        for i in range(planes):
            source = lax.rem(zed + i, planes)
            block = block_of(source)
            arrived = remote(block, block, ss.at[0], rs.at[source], {"cp": me})
            if i == 0:
                @pl.when(jnp.logical_not(keeper))
                def _():
                    arrived.wait_recv()
            else:
                arrived.wait_recv()

    def ga_copy(i, j):
        c = core if i == 0 else 1 - core
        return seq_copy(
            ga_s, ga_r, 2 * i + j,
            ga_out.at[j, two_rows(c)], ga.at[two_rows(zed)], j, c,
        )

    def ga_group(i):
        c = core if i == 0 else 1 - core
        result = lax.dot_general(
            ups[two_rows(c)], wall[...], nt, preferred_element_type=f32
        ).astype(bf16)
        for j in range(2):
            ga_out[j, two_rows(c)] = result[:, j * HEAD:(j + 1) * HEAD]

            def here(j=j):
                ga[two_rows(zed)] = result[:, j * HEAD:(j + 1) * HEAD]

            seq_send(ga_copy(i, j), here, j, i)

    def work_gradient():
        for p in range(cols):
            block = piece_of(2 * core + 1 - ex, p)
            remote(block, block, side_s.at[p], side_r.at[p], across).wait_recv()

        ga_group(0)
        for slot, y in ((0, why), (2, 1 - why)):
            block = ups.at[rows(2 * (1 - core) + y)]
            remote(block, block, up_s.at[slot], up_r.at[slot], mate).wait_recv()
        ga_group(1)

    @pl.when(far)
    def _():
        for p in range(cols // 2, cols):
            piece_poll(p)

    @pl.when(jnp.logical_not(far))
    def _():
        work_gradient()

    heads_wait(2, vh)
    vt[...] = vh[...].astype(f32).T.astype(bf16)

    def attend(o, carry):
        part = two_rows(o)
        att_t = jnp.dot(vt[...], prob[:, part], preferred_element_type=f32)
        att[part] = att_t.T.astype(bf16)
        return carry

    lax.fori_loop(0, n // 2, attend, 0)

    def att_copy(i):
        plane = lax.rem(zed + i, planes)
        return remote(
            att.at[two_rows(plane)], attp.at[lax.rem(zed, 2), two_rows(core)],
            att_s.at[i], att_r.at[2 * lax.rem(zed, 2) + core],
            {"cp": 2 * plane + why, "fsdp": 2 * ex + zed // 2},
        )

    for i in (2, 1, 3):
        launch(att_copy(i))

    @pl.when(keeper)
    def _():
        attp[lax.rem(zed, 2), two_rows(core)] = att[two_rows(zed)]

    @pl.when(jnp.logical_not(keeper))
    def _():
        att_copy(0).start()

    @pl.when(far)
    def _():
        work_gradient()

    width = math.gcd(proj.shape[1], 512)

    for j in range(2):
        for c in range(2):
            block = attp.at[j, 2 * c * tokens:2 * (c + 1) * tokens]
            arrived = remote(block, block, att_s.at[0], att_r.at[2 * j + c], {"cp": me})

            @pl.when(jnp.logical_not(jnp.logical_and(2 * core + j == zed, core == c)))
            def _():
                arrived.wait_recv()

    att_t = jnp.concatenate(
        [attp[0].astype(f32).T.astype(bf16), attp[1].astype(f32).T.astype(bf16)], axis=0
    )
    att_both = jnp.concatenate([attp[0], attp[1]], axis=1)

    def weigh(i, carry):
        lanes = rows_of(i * width, width)
        dw[:, lanes] = jnp.dot(att_t, ups[:, lanes], preferred_element_type=f32).astype(bf16)
        return carry

    def project(i, carry):
        lanes = rows_of(i * width, width)
        mix[:, lanes] = jnp.dot(
            att_both, wall[:, lanes], preferred_element_type=f32
        ).astype(bf16)
        return carry

    lax.fori_loop(0, proj.shape[1] // width, weigh, 0)
    share = 2 * slab

    def dw_rows(j, x):
        return rows_of(j * HEAD + x * share, share)

    for j in range(2):
        launch(remote(
            dw.at[dw_rows(j, 1 - ex)], dwx.at[j], dwx_s.at[j], dwx_r.at[j], across
        ))

    lax.fori_loop(0, proj.shape[1] // width, project, 0)
    launch(remote(mix.at[two_rows(1 - core)], mix_mate, mix_s.at[0], mix_r.at[0], mate))

    seq_wait(ga_s, ga_r, lambda source: ga.at[two_rows(source)])

    def value_step(o, carry):
        part = two_rows(o)
        dvh[part] = jnp.dot(prob[part], ga[...], preferred_element_type=f32).astype(bf16)
        return carry

    lax.fori_loop(0, n // 2, value_step, 0)
    out_send(2, dvh, dv)
    dv[:, head_cols(me)] = dvh[rows(me)]

    remote(mix_mate, mix_mate, mix_s.at[0], mix_r.at[0], mate).wait_recv()
    theirs, ours = rows(1 - why), rows(why)
    mix_send[...] = (
        mix[rows(2 * core + 1 - why)].astype(f32) + mix_mate[theirs].astype(f32)
    ).astype(bf16)
    launch(remote(mix_send, mix_beside, mix_s.at[1], mix_r.at[1], beside))

    def backward(i, carry):
        i = lax.rem(i + n // 2, n)
        o = lax.rem(me + i, n)
        part = rows(o)
        ga_rows = ga[part]
        delta = (att[part].astype(f32) * ga_rows.astype(f32)).T.sum(0, keepdims=True)
        dprob = lax.dot_general(vh[...], ga_rows, nt, preferred_element_type=f32)
        ds = (prob[:, part].astype(f32) * ((dprob - delta) * (1.0 / HEAD))).astype(bf16)
        dsb[:, part] = ds
        dqh[part] = jnp.dot(kt[...], ds, preferred_element_type=f32).T.astype(bf16)

        @pl.when(i > 0)
        def _():
            out_copy(0, i, dqh, dq).start()

        return carry

    lax.fori_loop(0, n, backward, 0)
    dq[:, head_cols(me)] = dqh[rows(me)]

    outer = jnp.logical_not(jnp.logical_or(keeper, gateway))

    def dw_copy(i, j):
        c = core if i == 0 else 1 - core
        return remote(
            dwz.at[j, rows_of(c * slab, slab)],
            dwr.at[jnp.where(keeper, jnp.where(2 * core + j == zed, 0, 1), 2)],
            dw_s.at[2 * i + j],
            dw_r.at[jnp.where(keeper, jnp.where(2 * core + j == zed, 0, 1), 2)],
            {"cp": 2 * (2 * core + j) + why, "fsdp": 2 * ex + c},
        )

    def lift_copy(j):
        return remote(dwz.at[j], dwp.at[j], lift_s.at[j], lift_r.at[j], {"cp": pair})

    def dw_send(j):
        for i in range(2):
            def here(j=j):
                dwr[0] = dwz[j, rows_of(core * slab, slab)]

            seq_send(dw_copy(i, j), here, j, i)

    for j in range(2):
        remote(dwx.at[j], dwx.at[j], dwx_s.at[j], dwx_r.at[j], across).wait_recv()
        dwz[j] = (dw[dw_rows(j, ex)].astype(f32) + dwx[j].astype(f32)).astype(bf16)

        @pl.when(outer)
        def _():
            lift_copy(j).start()

        @pl.when(keeper)
        def _():
            dw_send(j)

    def key_step(o, carry):
        part = two_rows(o)
        dkh[part] = jnp.dot(dsb[part], qh[...], preferred_element_type=f32).astype(bf16)
        return carry

    lax.fori_loop(0, n // 2, key_step, 0)
    out_send(1, dkh, dk)
    dk[:, head_cols(me)] = dkh[rows(me)]

    @pl.when(gateway)
    def _():
        for j in range(2):
            lift_copy(j).wait_recv()
            dwz[j] = (dwz[j].astype(f32) + dwp[j].astype(f32)).astype(bf16)
            dw_send(j)

    remote(mix_beside, mix_beside, mix_s.at[1], mix_r.at[1], beside).wait_recv()
    proj[...] = (
        mix[rows(2 * core + why)].astype(f32) + mix_mate[ours].astype(f32)
        + mix_beside[...].astype(f32)
    ).astype(bf16)
    for t in range(3):
        arrived = remote(dwr.at[t], dwr.at[t], dw_s.at[0], dw_r.at[t], {"cp": me})
        if t == 0:
            @pl.when(jnp.logical_not(keeper))
            def _():
                arrived.wait_recv()
        else:
            arrived.wait_recv()
    total = dwr[0].astype(f32) + dwr[1].astype(f32) + dwr[2].astype(f32)
    wg[...] = total
    out_wait(2, dv)
    out_wait(0, dq)
    out_wait(1, dk)
    for copy in sends:
        copy.wait_send()
    for i in offsets:
        out_copy(0, i, dqh, dq).wait_send()

    @pl.when(jnp.logical_not(root))
    def _():
        slab_copies[0].wait_send()

    @pl.when(jnp.logical_not(keeper))
    def _():
        att_copy(0).wait_send()

    for j in range(2):
        seq_settle(ga_copy(0, j), j)
        ga_copy(1, j).wait_send()

    for p in range(cols):
        side_copy(p).wait_send()

    for j in range(2):
        @pl.when(outer)
        def _():
            lift_copy(j).wait_send()

        @pl.when(jnp.logical_not(outer))
        def _():
            seq_settle(dw_copy(0, j), j)
            dw_copy(1, j).wait_send()


    @pl.when(gateway)
    def _():
        for p in range(cols):
            pass_copy(p).wait_send()


def deliver_kernel(*refs):
    count = len(refs) // 2
    copies = [
        pltpu.make_async_copy(refs[t], refs[count + t], refs[-1].at[t]) for t in range(count)
    ]
    for copy in copies:
        copy.start()
    for copy in copies:
        copy.wait()


def by_heads(query_states, key_states, value_states, span_order, block_mask, output_weight, upstream):
    n = lax.axis_size("cp")
    m = lax.axis_size("fsdp")
    tokens, width = query_states.shape[1:]
    length = tokens * n
    model = upstream.shape[2]
    slab = output_weight.shape[0]
    bf16, f32 = jnp.bfloat16, jnp.float32
    shape = jax.ShapeDtypeStruct
    vmem = pl.BlockSpec(memory_space=pltpu.VMEM)
    dma = pltpu.SemaphoreType.DMA
    planes = n // 2
    head_array = pltpu.VMEM((length, HEAD), bf16)
    square = pltpu.VMEM((length, length), bf16)
    projected, dq, dk, dv, weight_gradient = pl.pallas_call(
        lambda *refs: layer_kernel(n, *refs),
        out_shape=(shape((tokens, model), bf16),)
        + (shape((tokens, width), bf16),) * 3
        + (shape((slab, model), f32),),
        in_specs=[pl.BlockSpec(memory_space=pltpu.HBM)] * 7,
        out_specs=(vmem,) * 5,
        scratch_shapes=[
            pltpu.VMEM((tokens, width), bf16), pltpu.VMEM((tokens, width), bf16),
            pltpu.VMEM((tokens, width), bf16), pltpu.VMEM((tokens, model), bf16),
            pltpu.VMEM((slab, model), bf16), pltpu.VMEM(span_order.shape, jnp.int32),
            pltpu.VMEM(block_mask.shape, jnp.int32), dma((7,)),
            head_array, head_array, head_array,
            pltpu.VMEM((4 * tokens, model), bf16), pltpu.VMEM((2 * HEAD, model), bf16),
            pltpu.VMEM((length, length), f32), square, square,
            head_array, pltpu.VMEM((2, 4 * tokens, HEAD), bf16),
            pltpu.VMEM((2, 4 * tokens, HEAD), bf16),
            head_array, head_array, head_array, head_array,
            pltpu.VMEM((2 * HEAD, model), bf16), pltpu.VMEM((2, 2 * slab, model), bf16),
            pltpu.VMEM((2, 2 * slab, model), bf16),
            pltpu.VMEM((2, 2 * slab, model), bf16), pltpu.VMEM((3, slab, model), bf16),
            pltpu.VMEM((HEAD, length), bf16), pltpu.VMEM((HEAD, length), bf16),
            pltpu.VMEM((4 * tokens, model), bf16), pltpu.VMEM((2 * tokens, model), bf16),
            pltpu.VMEM((tokens, model), bf16), pltpu.VMEM((tokens, model), bf16),
            dma((3, n)), dma((3, n)), dma((3, n)), dma((3, n)), dma((3,)), dma((3,)),
            dma((3,)), dma((m,)), dma((m,)), dma((m,)), dma((m,)),
            dma((4,)), dma((planes,)), dma((planes,)), dma((4,)),
            dma((2,)), dma((2,)), dma((2,)), dma((2,)), dma((4,)), dma((3,)), dma((2,)), dma((2,)),
        ],
        compiler_params=pltpu.CompilerParams(
            collective_id=0, has_side_effects=True, vmem_limit_bytes=48 << 20
        ),
        name="layer",
    )(
        *(
            pltpu.with_memory_space_constraint(a, pltpu.HBM)
            for a in (
                query_states[0], key_states[0], value_states[0], upstream[0], output_weight,
                span_order, block_mask,
            )
        ),
    )
    results = (projected, dq, dk, dv, weight_gradient)
    projected, dq, dk, dv, weight_gradient = pl.pallas_call(
        deliver_kernel,
        out_shape=tuple(shape(r.shape, r.dtype) for r in results),
        in_specs=[pl.BlockSpec(memory_space=pl.ANY)] * 5,
        out_specs=(pl.BlockSpec(memory_space=pl.ANY),) * 5,
        scratch_shapes=[dma((5,))],
        compiler_params=pltpu.CompilerParams(vmem_limit_bytes=1 << 20),
        name="deliver",
    )(*results)
    return (projected[None], dq[None], dk[None], dv[None], weight_gradient)


def solution(mesh):
    fits = mesh.shape["cp"] == HEADS and mesh.shape["fsdp"] == 4
    return jax.shard_map(
        by_heads if fits else local,
        mesh=mesh,
        in_specs=(
            P("fsdp", "cp", None),
            P("fsdp", "cp", None),
            P("fsdp", "cp", None),
            P(),
            P(),
            P(("cp", "fsdp"), None),
            P("fsdp", "cp", None),
        ),
        out_specs=(
            P("fsdp", "cp", None),
            P("fsdp", "cp", None),
            P("fsdp", "cp", None),
            P("fsdp", "cp", None),
            P(("cp", "fsdp"), None),
        ),
        check_vma=False,
    )
```

```python
import math

import jax
import jax.numpy as jnp
from jax import lax
from jax.experimental import pallas as pl
from jax.experimental.pallas import tpu as pltpu
from jax.sharding import PartitionSpec as P

HEADS = 8
HEAD = 128


lowest = -1e30


def split_heads(row_block):
    return row_block.reshape(row_block.shape[0], HEADS, HEAD)


def pair_scores(query_rows, key_rows):
    return jnp.einsum(
        "qhd,khd->hqk",
        split_heads(query_rows),
        split_heads(key_rows),
        preferred_element_type=jnp.float32,
    ) * (1.0 / HEAD)


def storage_mask(span_order, block_mask):
    span_count = span_order.shape[0]
    onehot = (span_order[:, None] == jnp.arange(span_count, dtype=jnp.int32)[None, :]).astype(
        jnp.float32
    )
    permuted = jnp.dot(jnp.dot(onehot, block_mask.astype(jnp.float32)), onehot.T)
    return permuted > 0.5


def allowed_block(span_ok, positions, query_begin, query_total, key_begin, key_total, span_rows):
    span_sub = lax.dynamic_slice(
        span_ok,
        (query_begin // span_rows, key_begin // span_rows),
        (query_total // span_rows, key_total // span_rows),
    )
    spread = jnp.broadcast_to(
        span_sub[:, None, :, None],
        (query_total // span_rows, span_rows, key_total // span_rows, span_rows),
    )
    spread = spread.reshape(query_total, key_total)
    query_pos = lax.dynamic_slice_in_dim(positions, query_begin, query_total)
    key_pos = lax.dynamic_slice_in_dim(positions, key_begin, key_total)
    return spread & (key_pos[None, :] <= query_pos[:, None])


def local_terms(query_rows, grad_rows, log_rows, delta_rows, key_rows, value_rows, allowed):
    scores = pair_scores(query_rows, key_rows)
    probability = jnp.where(allowed[None], jnp.exp(scores - log_rows[..., None]), 0.0)
    dprob = jnp.einsum(
        "qhd,khd->hqk",
        split_heads(grad_rows),
        split_heads(value_rows),
        preferred_element_type=jnp.float32,
    )
    dscores = (probability * (dprob - delta_rows[..., None]) * (1.0 / HEAD)).astype(jnp.bfloat16)
    return (probability, dscores)


def local(query_states, key_states, value_states, span_order, block_mask, output_weight, upstream):
    query_rows = query_states[0]
    key_local = key_states[0]
    value_local = value_states[0]
    upstream_rows = upstream[0]
    tokens = query_rows.shape[0]
    span_rows = tokens // 2
    positions = (
        span_order[:, None] * span_rows + jnp.arange(span_rows, dtype=jnp.int32)[None, :]
    ).reshape(-1)
    span_ok = storage_mask(span_order, block_mask)
    own_start = lax.axis_index("cp") * tokens
    key_all, value_all = (
        lax.all_gather(key_local, "cp", axis=0, tiled=True),
        lax.all_gather(value_local, "cp", axis=0, tiled=True),
    )
    weight = lax.all_gather(output_weight, ("cp", "fsdp"), axis=0, tiled=True)
    length = key_all.shape[0]
    key_block = math.gcd(length, 512)
    block_count = length // key_block
    block_steps = jnp.arange(block_count, dtype=jnp.int32)

    def stats_step(running, step_index):
        key_begin = step_index * key_block
        key_rows = lax.dynamic_slice_in_dim(key_all, key_begin, key_block)
        allowed = allowed_block(
            span_ok, positions, own_start, tokens, key_begin, key_block, span_rows
        )
        maxima, totals = running
        scores = pair_scores(query_rows, key_rows)
        masked = jnp.where(allowed[None], scores, lowest)
        new_max = jnp.maximum(maxima, masked.max(-1))
        exp_terms = jnp.where(allowed[None], jnp.exp(scores - new_max[..., None]), 0.0)
        return ((new_max, totals * jnp.exp(maxima - new_max) + exp_terms.sum(-1)), None)

    stat_start = (
        jnp.full((HEADS, tokens), lowest, jnp.float32),
        jnp.zeros((HEADS, tokens), jnp.float32),
    )
    (maxima, totals), _ = lax.scan(stats_step, stat_start, block_steps)
    log_total = maxima + jnp.log(totals)

    def output_step(attn_sum, step_index):
        key_begin = step_index * key_block
        key_rows = lax.dynamic_slice_in_dim(key_all, key_begin, key_block)
        value_rows = lax.dynamic_slice_in_dim(value_all, key_begin, key_block)
        allowed = allowed_block(
            span_ok, positions, own_start, tokens, key_begin, key_block, span_rows
        )
        scores = pair_scores(query_rows, key_rows)
        probability = jnp.where(allowed[None], jnp.exp(scores - log_total[..., None]), 0.0)
        return (
            attn_sum
            + jnp.einsum(
                "hqk,khd->qhd",
                probability.astype(jnp.bfloat16),
                split_heads(value_rows),
                preferred_element_type=jnp.float32,
            ),
            None,
        )

    zero_heads = jnp.zeros((tokens, HEADS, HEAD), jnp.float32)
    attn_sum, _ = lax.scan(output_step, zero_heads, block_steps)
    attended = lax.optimization_barrier(attn_sum.reshape(tokens, -1).astype(jnp.bfloat16))
    projected = jnp.dot(attended, weight, preferred_element_type=jnp.float32).astype(jnp.bfloat16)
    grad_attended = lax.dot_general(
        upstream_rows, weight, (((1,), (1,)), ((), ())), preferred_element_type=jnp.float32
    ).astype(jnp.bfloat16)
    grad_attended = lax.optimization_barrier(grad_attended)
    weight_term = lax.dot_general(
        attended, upstream_rows, (((0,), (0,)), ((), ())), preferred_element_type=jnp.float32
    )
    row_delta = (
        (grad_attended.astype(jnp.float32) * attended.astype(jnp.float32))
        .reshape(tokens, HEADS, HEAD)
        .sum(-1)
    )
    delta_heads = row_delta.T

    def query_step(grad_sum, step_index):
        key_begin = step_index * key_block
        key_rows = lax.dynamic_slice_in_dim(key_all, key_begin, key_block)
        value_rows = lax.dynamic_slice_in_dim(value_all, key_begin, key_block)
        allowed = allowed_block(
            span_ok, positions, own_start, tokens, key_begin, key_block, span_rows
        )
        probability, dscores = local_terms(
            query_rows, grad_attended, log_total, delta_heads, key_rows, value_rows, allowed
        )
        return (
            grad_sum
            + jnp.einsum(
                "hqk,khd->qhd", dscores, split_heads(key_rows), preferred_element_type=jnp.float32
            ),
            None,
        )

    query_sum, _ = lax.scan(query_step, zero_heads, block_steps)
    query_gradient = query_sum.reshape(tokens, -1).astype(jnp.bfloat16)
    log_all, delta_all = (
        lax.all_gather(log_total.T, "cp", axis=0, tiled=True),
        lax.all_gather(row_delta, "cp", axis=0, tiled=True),
    )
    sums_now = (zero_heads, zero_heads)
    query_piece = lax.all_gather(query_rows, "cp", axis=0, tiled=True)
    grad_piece = lax.all_gather(grad_attended, "cp", axis=0, tiled=True)
    row_count = query_piece.shape[0]
    sources = row_count // tokens
    group_size = math.gcd(sources, max(1, 512 // tokens))
    group_rows = group_size * tokens

    def group_step(running, step_index):
        offset = step_index * group_rows
        query_group = lax.dynamic_slice_in_dim(query_piece, offset, group_rows)
        grad_group = lax.dynamic_slice_in_dim(grad_piece, offset, group_rows)
        log_group = lax.dynamic_slice_in_dim(log_all, offset, group_rows).T
        delta_group = lax.dynamic_slice_in_dim(delta_all, offset, group_rows).T
        allowed = allowed_block(
            span_ok, positions, offset, group_rows, own_start, tokens, span_rows
        )
        key_sum, value_sum = running
        probability, dscores = local_terms(
            query_group, grad_group, log_group, delta_group, key_local, value_local, allowed
        )
        probability_low = probability.astype(jnp.bfloat16).reshape(
            HEADS, group_size, tokens, tokens
        )
        dscores_group = dscores.reshape(HEADS, group_size, tokens, tokens)
        qsplit = query_group.reshape(group_size, tokens, HEADS, HEAD)
        gsplit = grad_group.reshape(group_size, tokens, HEADS, HEAD)
        key_part = jnp.einsum(
            "hgqk,gqhd->gkhd", dscores_group, qsplit, preferred_element_type=jnp.float32
        ).astype(jnp.bfloat16)
        value_part = jnp.einsum(
            "hgqk,gqhd->gkhd", probability_low, gsplit, preferred_element_type=jnp.float32
        ).astype(jnp.bfloat16)
        key_part, value_part = lax.optimization_barrier((key_part, value_part))
        return (
            (
                key_sum + key_part.astype(jnp.float32).sum(0),
                value_sum + value_part.astype(jnp.float32).sum(0),
            ),
            None,
        )

    sums_now, _ = lax.scan(group_step, sums_now, jnp.arange(sources // group_size, dtype=jnp.int32))
    key_sum, value_sum = sums_now
    key_gradient = key_sum.reshape(tokens, -1).astype(jnp.bfloat16)
    value_gradient = value_sum.reshape(tokens, -1).astype(jnp.bfloat16)
    cycle_count = lax.axis_size("cp")
    batch_count = lax.axis_size("fsdp")
    slab_rows = weight_term.shape[0] // (cycle_count * batch_count)
    reordered = weight_term.reshape(cycle_count, batch_count, slab_rows, -1).transpose(1, 0, 2, 3)
    reordered = reordered.reshape(weight_term.shape[0], -1)
    partial_batch = lax.psum_scatter(
        reordered.astype(jnp.bfloat16), "fsdp", scatter_dimension=0, tiled=True
    )
    weight_gradient = lax.psum_scatter(partial_batch, "cp", scatter_dimension=0, tiled=True).astype(
        jnp.float32
    )
    return (
        projected[None],
        query_gradient[None],
        key_gradient[None],
        value_gradient[None],
        weight_gradient,
    )


MESH = pl.DeviceIdType.MESH


def remote(src, dst, send_sem, recv_sem, device):
    return pltpu.make_async_remote_copy(
        src_ref=src,
        dst_ref=dst,
        send_sem=send_sem,
        recv_sem=recv_sem,
        device_id=device,
        device_id_type=MESH,
    )


def rows_of(begin, count):
    return pl.ds(pl.multiple_of(begin, count), count)


def greet(devices):
    barrier = pltpu.get_barrier_semaphore()
    for device in devices:
        pl.semaphore_signal(barrier, inc=1, device_id=device, device_id_type=MESH)
    pl.semaphore_wait(barrier, len(devices))


def layer_kernel(
    n, q_in, k_in, v_in, up_in, w_in, order_in, mask_in, proj, dq, dk, dv, wg,
    q, k, v, up, w, order, mask, load,
    qh, kh, vh, ups, wall, bias, prob, dsb, att, attp, ga_out, ga,
    dqh, dkh, dvh, dw, dwx, dwz, dwp, dwr, kt, vt, mix, mix_mate, mix_send, mix_beside,
    heads_s, heads_r, out_s, out_r, up_s, up_r,
    slab_s, slab_r, pass_s, side_s, side_r, ga_s, ga_r, att_s, att_r,
    dwx_s, dwx_r, lift_s, lift_r, dw_s, dw_r, mix_s, mix_r,
):
    me = lax.axis_index("cp")
    col = lax.axis_index("fsdp")
    cols = lax.axis_size("fsdp")
    planes = n // 2
    zed, why = me // 2, lax.rem(me, 2)
    ex, core = col // 2, lax.rem(col, 2)
    mate = {"fsdp": 2 * ex + 1 - core}
    across = {"fsdp": 2 * (1 - ex) + core}
    beside = {"cp": 2 * zed + 1 - why}
    tokens = up.shape[0]
    slab = w.shape[0]
    length = tokens * n
    span_rows = tokens // 2
    bf16, f32 = jnp.bfloat16, jnp.float32
    nt = (((1,), (1,)), ((), ()))
    home = 2 * core + ex
    root = home == zed
    keeper = core == zed // 2
    gateway = jnp.logical_and(jnp.logical_not(keeper), zed == 1 + zed // 2)
    pair = 2 * (zed + 1 - 2 * lax.rem(zed, 2)) + why

    def head_cols(d):
        return rows_of(d * HEAD, HEAD)

    def rows(d):
        return rows_of(d * tokens, tokens)

    def two_rows(d):
        return rows_of(d * 2 * tokens, 2 * tokens)

    pairs = (
        (k_in, k), (up_in, up), (w_in, w), (q_in, q), (v_in, v), (order_in, order), (mask_in, mask)
    )
    loads = [pltpu.make_async_copy(a, b, load.at[t]) for t, (a, b) in enumerate(pairs)]
    for copy in loads:
        copy.start()
    barrier = pltpu.get_barrier_semaphore()
    for i in range(n):
        for j in range(cols):
            if i or j:
                pl.semaphore_signal(
                    barrier, inc=1,
                    device_id={"cp": lax.rem(me + i, n), "fsdp": lax.rem(col + j, cols)},
                    device_id_type=MESH,
                )
    for copy in loads:
        copy.wait()
    pl.semaphore_wait(barrier, n * cols - 1)

    sends = []
    offsets = [n // 2]
    for i in range(1, n // 2):
        offsets += [n // 2 - i, n // 2 + i]

    def launch(copy):
        copy.start()
        sends.append(copy)

    def heads_send(t, source, target):
        for i in offsets:
            d = lax.rem(me + i, n)
            launch(remote(
                source.at[:, head_cols(d)], target.at[rows(me)],
                heads_s.at[t, i], heads_r.at[t, i], {"cp": d},
            ))

    def heads_arrival(t, i, target):
        source = lax.rem(me + n - i, n)
        block = target.at[rows(source)]
        remote(block, block, heads_s.at[t, i], heads_r.at[t, i], {"cp": source}).wait_recv()

    def heads_wait(t, target):
        for i in offsets:
            heads_arrival(t, i, target)

    def out_copy(t, i, source, target):
        d = lax.rem(me + i, n)
        return remote(
            source.at[rows(d)], target.at[:, head_cols(me)],
            out_s.at[t, i], out_r.at[t, i], {"cp": d},
        )

    def out_send(t, source, target):
        for i in offsets:
            launch(out_copy(t, i, source, target))

    def out_wait(t, target):
        for i in offsets:
            source = lax.rem(me + n - i, n)
            block = target.at[:, head_cols(source)]
            remote(block, block, out_s.at[t, i], out_r.at[t, i], {"cp": source}).wait_recv()

    own_slab = rows_of(lax.rem(zed, 2) * HEAD + col * slab, slab)
    slab_copies = [
        remote(
            w, wall.at[own_slab], slab_s.at[i], slab_r.at[col],
            {"cp": target, "fsdp": 2 * lax.rem(zed, 2) + zed // 2},
        )
        for i, target in enumerate((me, pair, 2 * (2 - zed // 2) + why))
    ]
    launch(slab_copies[2])

    @pl.when(jnp.logical_not(root))
    def _():
        slab_copies[0].start()

    launch(slab_copies[1])
    mine_up = ups.at[rows(2 * core + why)]
    launch(remote(up, mine_up, up_s.at[1], up_r.at[1], beside))
    heads_send(0, k, kh)
    launch(remote(up, mine_up, up_s.at[0], up_r.at[0], mate))
    heads_send(1, q, qh)

    @pl.when(root)
    def _():
        wall[own_slab] = w[...]

    def piece_of(plane, p):
        return wall.at[rows_of(lax.rem(plane, 2) * HEAD + p * slab, slab)]

    def pass_copy(p):
        block = piece_of(home, p)
        return remote(block, block, pass_s.at[p], slab_r.at[p], {"cp": pair})

    def side_copy(p):
        block = piece_of(home, p)
        return remote(block, block, side_s.at[p], side_r.at[p], across)

    def piece_poll(p):
        @pl.when(jnp.logical_not(jnp.logical_and(root, col == p)))
        def _():
            block = piece_of(home, p)
            remote(block, block, slab_s.at[0], slab_r.at[p], mate).wait_recv()

        @pl.when(gateway)
        def _():
            pass_copy(p).start()

        side_copy(p).start()

    for source, target in ((k, kh), (q, qh), (v, vh)):
        target[rows(me)] = source[:, head_cols(me)]
    ups[rows(2 * core + why)] = up[...]

    spans = order.shape[0]
    order_row = jnp.broadcast_to(order[...].reshape(1, spans), (spans, spans))
    place = lax.broadcasted_iota(jnp.int32, (spans, spans), 0)
    at_place = (order_row == place).astype(f32).astype(bf16)
    row = lax.broadcasted_iota(jnp.int32, (spans, length), 1)
    line = lax.broadcasted_iota(jnp.int32, (spans, length), 0)
    begin = line * span_rows
    member = jnp.logical_and(row >= begin, row < begin + span_rows).astype(f32)
    placed = jnp.dot(at_place, member.astype(bf16), preferred_element_type=f32)
    within = (row - begin).astype(f32) * member
    query_pos = (placed * begin.astype(f32) + within).sum(0, keepdims=True)
    key_pos = jnp.broadcast_to(query_pos, (8, length)).T[:, :1]
    placed_low = placed.astype(bf16)
    key_side = jnp.dot(
        mask[...].astype(f32).astype(bf16), placed_low, preferred_element_type=f32
    ).T.astype(bf16)
    for o in range(n):
        part = slice(o * tokens, (o + 1) * tokens)
        seen = jnp.dot(key_side, placed_low[:, part], preferred_element_type=f32)
        allowed = jnp.logical_and(seen > 0.5, key_pos <= query_pos[:, part])
        bias[:, part] = jnp.where(allowed, 0.0, lowest)

    far = jnp.logical_not(jnp.logical_or(keeper, gateway))

    @pl.when(jnp.logical_not(far))
    def _():
        for p in range(cols):
            piece_poll(p)

    heads_wait(0, kh)
    heads_send(2, v, vh)
    kt[...] = kh[...].astype(f32).T.astype(bf16)
    beside_up = ups.at[rows(2 * core + 1 - why)]
    remote(beside_up, beside_up, up_s.at[1], up_r.at[1], beside).wait_recv()
    launch(remote(beside_up, beside_up, up_s.at[2], up_r.at[2], mate))
    @pl.when(far)
    def _():
        for p in range(cols // 2):
            piece_poll(p)

    def soft(i, carry):
        @pl.when(i > 0)
        def _():
            heads_arrival(1, i, qh)

        part = rows(lax.rem(me + n - i, n))
        scores = lax.dot_general(kh[...], qh[part], nt, preferred_element_type=f32) * (1.0 / HEAD)
        scores = scores + bias[:, part]
        terms = jnp.exp(scores - scores.max(0, keepdims=True))
        probability = terms * (1.0 / terms.sum(0, keepdims=True))
        prob[:, part] = probability.astype(bf16)
        return carry

    lax.fori_loop(0, n, soft, 0)

    def seq_copy(ss, rs, slot, source, target, j, c):
        return remote(
            source, target, ss.at[slot], rs.at[zed], {"cp": 2 * (2 * core + j) + why, "fsdp": 2 * ex + c}
        )

    def seq_send(copy, here, j, i):
        if i:
            copy.start()
            return
        stays = 2 * core + j == zed

        @pl.when(stays)
        def _():
            here()

        @pl.when(jnp.logical_not(stays))
        def _():
            copy.start()

    def seq_settle(copy, j):
        @pl.when(2 * core + j != zed)
        def _():
            copy.wait_send()

    def seq_wait(ss, rs, block_of):
        for i in range(planes):
            source = lax.rem(zed + i, planes)
            block = block_of(source)
            arrived = remote(block, block, ss.at[0], rs.at[source], {"cp": me})
            if i == 0:
                @pl.when(jnp.logical_not(keeper))
                def _():
                    arrived.wait_recv()
            else:
                arrived.wait_recv()

    def ga_copy(i, j):
        c = core if i == 0 else 1 - core
        return seq_copy(
            ga_s, ga_r, 2 * i + j,
            ga_out.at[j, two_rows(c)], ga.at[two_rows(zed)], j, c,
        )

    def ga_group(i):
        c = core if i == 0 else 1 - core
        result = lax.dot_general(
            ups[two_rows(c)], wall[...], nt, preferred_element_type=f32
        ).astype(bf16)
        for j in range(2):
            ga_out[j, two_rows(c)] = result[:, j * HEAD:(j + 1) * HEAD]

            def here(j=j):
                ga[two_rows(zed)] = result[:, j * HEAD:(j + 1) * HEAD]

            seq_send(ga_copy(i, j), here, j, i)

    def work_gradient():
        for p in range(cols):
            block = piece_of(2 * core + 1 - ex, p)
            remote(block, block, side_s.at[p], side_r.at[p], across).wait_recv()

        ga_group(0)
        for slot, y in ((0, why), (2, 1 - why)):
            block = ups.at[rows(2 * (1 - core) + y)]
            remote(block, block, up_s.at[slot], up_r.at[slot], mate).wait_recv()
        ga_group(1)

    @pl.when(far)
    def _():
        for p in range(cols // 2, cols):
            piece_poll(p)

    @pl.when(jnp.logical_not(far))
    def _():
        work_gradient()

    heads_wait(2, vh)
    vt[...] = vh[...].astype(f32).T.astype(bf16)

    def attend(o, carry):
        part = two_rows(o)
        att_t = jnp.dot(vt[...], prob[:, part], preferred_element_type=f32)
        att[part] = att_t.T.astype(bf16)
        return carry

    lax.fori_loop(0, n // 2, attend, 0)

    def att_copy(i):
        plane = lax.rem(zed + i, planes)
        return remote(
            att.at[two_rows(plane)], attp.at[lax.rem(zed, 2), two_rows(core)],
            att_s.at[i], att_r.at[2 * lax.rem(zed, 2) + core],
            {"cp": 2 * plane + why, "fsdp": 2 * ex + zed // 2},
        )

    for i in (2, 1, 3):
        launch(att_copy(i))

    @pl.when(keeper)
    def _():
        attp[lax.rem(zed, 2), two_rows(core)] = att[two_rows(zed)]

    @pl.when(jnp.logical_not(keeper))
    def _():
        att_copy(0).start()

    @pl.when(far)
    def _():
        work_gradient()

    width = math.gcd(proj.shape[1], 512)

    for j in range(2):
        for c in range(2):
            block = attp.at[j, 2 * c * tokens:2 * (c + 1) * tokens]
            arrived = remote(block, block, att_s.at[0], att_r.at[2 * j + c], {"cp": me})

            @pl.when(jnp.logical_not(jnp.logical_and(2 * core + j == zed, core == c)))
            def _():
                arrived.wait_recv()

    att_t = jnp.concatenate(
        [attp[0].astype(f32).T.astype(bf16), attp[1].astype(f32).T.astype(bf16)], axis=0
    )
    att_both = jnp.concatenate([attp[0], attp[1]], axis=1)

    def weigh(i, carry):
        lanes = rows_of(i * width, width)
        dw[:, lanes] = jnp.dot(att_t, ups[:, lanes], preferred_element_type=f32).astype(bf16)
        return carry

    def project(i, carry):
        lanes = rows_of(i * width, width)
        mix[:, lanes] = jnp.dot(
            att_both, wall[:, lanes], preferred_element_type=f32
        ).astype(bf16)
        return carry

    lax.fori_loop(0, proj.shape[1] // width, weigh, 0)
    share = 2 * slab

    def dw_rows(j, x):
        return rows_of(j * HEAD + x * share, share)

    for j in range(2):
        launch(remote(
            dw.at[dw_rows(j, 1 - ex)], dwx.at[j], dwx_s.at[j], dwx_r.at[j], across
        ))

    lax.fori_loop(0, proj.shape[1] // width, project, 0)
    launch(remote(mix.at[two_rows(1 - core)], mix_mate, mix_s.at[0], mix_r.at[0], mate))

    seq_wait(ga_s, ga_r, lambda source: ga.at[two_rows(source)])

    def value_step(o, carry):
        part = two_rows(o)
        dvh[part] = jnp.dot(prob[part], ga[...], preferred_element_type=f32).astype(bf16)
        return carry

    lax.fori_loop(0, n // 2, value_step, 0)
    out_send(2, dvh, dv)
    dv[:, head_cols(me)] = dvh[rows(me)]

    def backward(i, carry):
        i = lax.rem(i + n // 2, n)
        o = lax.rem(me + i, n)
        part = rows(o)
        ga_rows = ga[part]
        delta = (att[part].astype(f32) * ga_rows.astype(f32)).T.sum(0, keepdims=True)
        dprob = lax.dot_general(vh[...], ga_rows, nt, preferred_element_type=f32)
        ds = (prob[:, part].astype(f32) * ((dprob - delta) * (1.0 / HEAD))).astype(bf16)
        dsb[:, part] = ds
        dqh[part] = jnp.dot(kt[...], ds, preferred_element_type=f32).T.astype(bf16)

        @pl.when(i > 0)
        def _():
            out_copy(0, i, dqh, dq).start()

        return carry

    lax.fori_loop(0, n // 2, backward, 0)
    remote(mix_mate, mix_mate, mix_s.at[0], mix_r.at[0], mate).wait_recv()
    theirs, ours = rows(1 - why), rows(why)
    mix_send[...] = (
        mix[rows(2 * core + 1 - why)].astype(f32) + mix_mate[theirs].astype(f32)
    ).astype(bf16)
    launch(remote(mix_send, mix_beside, mix_s.at[1], mix_r.at[1], beside))

    lax.fori_loop(n // 2, n, backward, 0)
    dq[:, head_cols(me)] = dqh[rows(me)]

    outer = jnp.logical_not(jnp.logical_or(keeper, gateway))

    def dw_copy(i, j):
        c = core if i == 0 else 1 - core
        return remote(
            dwz.at[j, rows_of(c * slab, slab)],
            dwr.at[jnp.where(keeper, jnp.where(2 * core + j == zed, 0, 1), 2)],
            dw_s.at[2 * i + j],
            dw_r.at[jnp.where(keeper, jnp.where(2 * core + j == zed, 0, 1), 2)],
            {"cp": 2 * (2 * core + j) + why, "fsdp": 2 * ex + c},
        )

    def lift_copy(j):
        return remote(dwz.at[j], dwp.at[j], lift_s.at[j], lift_r.at[j], {"cp": pair})

    def dw_send(j):
        for i in range(2):
            def here(j=j):
                dwr[0] = dwz[j, rows_of(core * slab, slab)]

            seq_send(dw_copy(i, j), here, j, i)

    for j in range(2):
        remote(dwx.at[j], dwx.at[j], dwx_s.at[j], dwx_r.at[j], across).wait_recv()
        dwz[j] = (dw[dw_rows(j, ex)].astype(f32) + dwx[j].astype(f32)).astype(bf16)

        @pl.when(outer)
        def _():
            lift_copy(j).start()

        @pl.when(keeper)
        def _():
            dw_send(j)

    def key_step(o, carry):
        part = two_rows(o)
        dkh[part] = jnp.dot(dsb[part], qh[...], preferred_element_type=f32).astype(bf16)
        return carry

    lax.fori_loop(0, n // 2, key_step, 0)
    out_send(1, dkh, dk)
    dk[:, head_cols(me)] = dkh[rows(me)]

    @pl.when(gateway)
    def _():
        for j in range(2):
            lift_copy(j).wait_recv()
            dwz[j] = (dwz[j].astype(f32) + dwp[j].astype(f32)).astype(bf16)
            dw_send(j)

    remote(mix_beside, mix_beside, mix_s.at[1], mix_r.at[1], beside).wait_recv()
    proj[...] = (
        mix[rows(2 * core + why)].astype(f32) + mix_mate[ours].astype(f32)
        + mix_beside[...].astype(f32)
    ).astype(bf16)
    for t in range(3):
        arrived = remote(dwr.at[t], dwr.at[t], dw_s.at[0], dw_r.at[t], {"cp": me})
        if t == 0:
            @pl.when(jnp.logical_not(keeper))
            def _():
                arrived.wait_recv()
        else:
            arrived.wait_recv()
    total = dwr[0].astype(f32) + dwr[1].astype(f32) + dwr[2].astype(f32)
    wg[...] = total
    out_wait(2, dv)
    out_wait(0, dq)
    out_wait(1, dk)
    for copy in sends:
        copy.wait_send()
    for i in offsets:
        out_copy(0, i, dqh, dq).wait_send()

    @pl.when(jnp.logical_not(root))
    def _():
        slab_copies[0].wait_send()

    @pl.when(jnp.logical_not(keeper))
    def _():
        att_copy(0).wait_send()

    for j in range(2):
        seq_settle(ga_copy(0, j), j)
        ga_copy(1, j).wait_send()

    for p in range(cols):
        side_copy(p).wait_send()

    for j in range(2):
        @pl.when(outer)
        def _():
            lift_copy(j).wait_send()

        @pl.when(jnp.logical_not(outer))
        def _():
            seq_settle(dw_copy(0, j), j)
            dw_copy(1, j).wait_send()


    @pl.when(gateway)
    def _():
        for p in range(cols):
            pass_copy(p).wait_send()


def deliver_kernel(*refs):
    count = len(refs) // 2
    copies = [
        pltpu.make_async_copy(refs[t], refs[count + t], refs[-1].at[t]) for t in range(count)
    ]
    for copy in copies:
        copy.start()
    for copy in copies:
        copy.wait()


def by_heads(query_states, key_states, value_states, span_order, block_mask, output_weight, upstream):
    n = lax.axis_size("cp")
    m = lax.axis_size("fsdp")
    tokens, width = query_states.shape[1:]
    length = tokens * n
    model = upstream.shape[2]
    slab = output_weight.shape[0]
    bf16, f32 = jnp.bfloat16, jnp.float32
    shape = jax.ShapeDtypeStruct
    vmem = pl.BlockSpec(memory_space=pltpu.VMEM)
    dma = pltpu.SemaphoreType.DMA
    planes = n // 2
    head_array = pltpu.VMEM((length, HEAD), bf16)
    square = pltpu.VMEM((length, length), bf16)
    projected, dq, dk, dv, weight_gradient = pl.pallas_call(
        lambda *refs: layer_kernel(n, *refs),
        out_shape=(shape((tokens, model), bf16),)
        + (shape((tokens, width), bf16),) * 3
        + (shape((slab, model), f32),),
        in_specs=[pl.BlockSpec(memory_space=pltpu.HBM)] * 7,
        out_specs=(vmem,) * 5,
        scratch_shapes=[
            pltpu.VMEM((tokens, width), bf16), pltpu.VMEM((tokens, width), bf16),
            pltpu.VMEM((tokens, width), bf16), pltpu.VMEM((tokens, model), bf16),
            pltpu.VMEM((slab, model), bf16), pltpu.VMEM(span_order.shape, jnp.int32),
            pltpu.VMEM(block_mask.shape, jnp.int32), dma((7,)),
            head_array, head_array, head_array,
            pltpu.VMEM((4 * tokens, model), bf16), pltpu.VMEM((2 * HEAD, model), bf16),
            pltpu.VMEM((length, length), f32), square, square,
            head_array, pltpu.VMEM((2, 4 * tokens, HEAD), bf16),
            pltpu.VMEM((2, 4 * tokens, HEAD), bf16),
            head_array, head_array, head_array, head_array,
            pltpu.VMEM((2 * HEAD, model), bf16), pltpu.VMEM((2, 2 * slab, model), bf16),
            pltpu.VMEM((2, 2 * slab, model), bf16),
            pltpu.VMEM((2, 2 * slab, model), bf16), pltpu.VMEM((3, slab, model), bf16),
            pltpu.VMEM((HEAD, length), bf16), pltpu.VMEM((HEAD, length), bf16),
            pltpu.VMEM((4 * tokens, model), bf16), pltpu.VMEM((2 * tokens, model), bf16),
            pltpu.VMEM((tokens, model), bf16), pltpu.VMEM((tokens, model), bf16),
            dma((3, n)), dma((3, n)), dma((3, n)), dma((3, n)), dma((3,)), dma((3,)),
            dma((3,)), dma((m,)), dma((m,)), dma((m,)), dma((m,)),
            dma((4,)), dma((planes,)), dma((planes,)), dma((4,)),
            dma((2,)), dma((2,)), dma((2,)), dma((2,)), dma((4,)), dma((3,)), dma((2,)), dma((2,)),
        ],
        compiler_params=pltpu.CompilerParams(
            collective_id=0, has_side_effects=True, vmem_limit_bytes=48 << 20
        ),
        name="layer",
    )(
        *(
            pltpu.with_memory_space_constraint(a, pltpu.HBM)
            for a in (
                query_states[0], key_states[0], value_states[0], upstream[0], output_weight,
                span_order, block_mask,
            )
        ),
    )
    results = (projected, dq, dk, dv, weight_gradient)
    projected, dq, dk, dv, weight_gradient = pl.pallas_call(
        deliver_kernel,
        out_shape=tuple(shape(r.shape, r.dtype) for r in results),
        in_specs=[pl.BlockSpec(memory_space=pl.ANY)] * 5,
        out_specs=(pl.BlockSpec(memory_space=pl.ANY),) * 5,
        scratch_shapes=[dma((5,))],
        compiler_params=pltpu.CompilerParams(vmem_limit_bytes=1 << 20),
        name="deliver",
    )(*results)
    return (projected[None], dq[None], dk[None], dv[None], weight_gradient)


def solution(mesh):
    fits = mesh.shape["cp"] == HEADS and mesh.shape["fsdp"] == 4
    return jax.shard_map(
        by_heads if fits else local,
        mesh=mesh,
        in_specs=(
            P("fsdp", "cp", None),
            P("fsdp", "cp", None),
            P("fsdp", "cp", None),
            P(),
            P(),
            P(("cp", "fsdp"), None),
            P("fsdp", "cp", None),
        ),
        out_specs=(
            P("fsdp", "cp", None),
            P("fsdp", "cp", None),
            P("fsdp", "cp", None),
            P("fsdp", "cp", None),
            P(("cp", "fsdp"), None),
        ),
        check_vma=False,
    )
```

```python
import math

import jax
import jax.numpy as jnp
from jax import lax
from jax.experimental import pallas as pl
from jax.experimental.pallas import tpu as pltpu
from jax.sharding import PartitionSpec as P

HEADS = 8
HEAD = 128


lowest = -1e30


def split_heads(row_block):
    return row_block.reshape(row_block.shape[0], HEADS, HEAD)


def pair_scores(query_rows, key_rows):
    return jnp.einsum(
        "qhd,khd->hqk",
        split_heads(query_rows),
        split_heads(key_rows),
        preferred_element_type=jnp.float32,
    ) * (1.0 / HEAD)


def storage_mask(span_order, block_mask):
    span_count = span_order.shape[0]
    onehot = (span_order[:, None] == jnp.arange(span_count, dtype=jnp.int32)[None, :]).astype(
        jnp.float32
    )
    permuted = jnp.dot(jnp.dot(onehot, block_mask.astype(jnp.float32)), onehot.T)
    return permuted > 0.5


def allowed_block(span_ok, positions, query_begin, query_total, key_begin, key_total, span_rows):
    span_sub = lax.dynamic_slice(
        span_ok,
        (query_begin // span_rows, key_begin // span_rows),
        (query_total // span_rows, key_total // span_rows),
    )
    spread = jnp.broadcast_to(
        span_sub[:, None, :, None],
        (query_total // span_rows, span_rows, key_total // span_rows, span_rows),
    )
    spread = spread.reshape(query_total, key_total)
    query_pos = lax.dynamic_slice_in_dim(positions, query_begin, query_total)
    key_pos = lax.dynamic_slice_in_dim(positions, key_begin, key_total)
    return spread & (key_pos[None, :] <= query_pos[:, None])


def local_terms(query_rows, grad_rows, log_rows, delta_rows, key_rows, value_rows, allowed):
    scores = pair_scores(query_rows, key_rows)
    probability = jnp.where(allowed[None], jnp.exp(scores - log_rows[..., None]), 0.0)
    dprob = jnp.einsum(
        "qhd,khd->hqk",
        split_heads(grad_rows),
        split_heads(value_rows),
        preferred_element_type=jnp.float32,
    )
    dscores = (probability * (dprob - delta_rows[..., None]) * (1.0 / HEAD)).astype(jnp.bfloat16)
    return (probability, dscores)


def local(query_states, key_states, value_states, span_order, block_mask, output_weight, upstream):
    query_rows = query_states[0]
    key_local = key_states[0]
    value_local = value_states[0]
    upstream_rows = upstream[0]
    tokens = query_rows.shape[0]
    span_rows = tokens // 2
    positions = (
        span_order[:, None] * span_rows + jnp.arange(span_rows, dtype=jnp.int32)[None, :]
    ).reshape(-1)
    span_ok = storage_mask(span_order, block_mask)
    own_start = lax.axis_index("cp") * tokens
    key_all, value_all = (
        lax.all_gather(key_local, "cp", axis=0, tiled=True),
        lax.all_gather(value_local, "cp", axis=0, tiled=True),
    )
    weight = lax.all_gather(output_weight, ("cp", "fsdp"), axis=0, tiled=True)
    length = key_all.shape[0]
    key_block = math.gcd(length, 512)
    block_count = length // key_block
    block_steps = jnp.arange(block_count, dtype=jnp.int32)

    def stats_step(running, step_index):
        key_begin = step_index * key_block
        key_rows = lax.dynamic_slice_in_dim(key_all, key_begin, key_block)
        allowed = allowed_block(
            span_ok, positions, own_start, tokens, key_begin, key_block, span_rows
        )
        maxima, totals = running
        scores = pair_scores(query_rows, key_rows)
        masked = jnp.where(allowed[None], scores, lowest)
        new_max = jnp.maximum(maxima, masked.max(-1))
        exp_terms = jnp.where(allowed[None], jnp.exp(scores - new_max[..., None]), 0.0)
        return ((new_max, totals * jnp.exp(maxima - new_max) + exp_terms.sum(-1)), None)

    stat_start = (
        jnp.full((HEADS, tokens), lowest, jnp.float32),
        jnp.zeros((HEADS, tokens), jnp.float32),
    )
    (maxima, totals), _ = lax.scan(stats_step, stat_start, block_steps)
    log_total = maxima + jnp.log(totals)

    def output_step(attn_sum, step_index):
        key_begin = step_index * key_block
        key_rows = lax.dynamic_slice_in_dim(key_all, key_begin, key_block)
        value_rows = lax.dynamic_slice_in_dim(value_all, key_begin, key_block)
        allowed = allowed_block(
            span_ok, positions, own_start, tokens, key_begin, key_block, span_rows
        )
        scores = pair_scores(query_rows, key_rows)
        probability = jnp.where(allowed[None], jnp.exp(scores - log_total[..., None]), 0.0)
        return (
            attn_sum
            + jnp.einsum(
                "hqk,khd->qhd",
                probability.astype(jnp.bfloat16),
                split_heads(value_rows),
                preferred_element_type=jnp.float32,
            ),
            None,
        )

    zero_heads = jnp.zeros((tokens, HEADS, HEAD), jnp.float32)
    attn_sum, _ = lax.scan(output_step, zero_heads, block_steps)
    attended = lax.optimization_barrier(attn_sum.reshape(tokens, -1).astype(jnp.bfloat16))
    projected = jnp.dot(attended, weight, preferred_element_type=jnp.float32).astype(jnp.bfloat16)
    grad_attended = lax.dot_general(
        upstream_rows, weight, (((1,), (1,)), ((), ())), preferred_element_type=jnp.float32
    ).astype(jnp.bfloat16)
    grad_attended = lax.optimization_barrier(grad_attended)
    weight_term = lax.dot_general(
        attended, upstream_rows, (((0,), (0,)), ((), ())), preferred_element_type=jnp.float32
    )
    row_delta = (
        (grad_attended.astype(jnp.float32) * attended.astype(jnp.float32))
        .reshape(tokens, HEADS, HEAD)
        .sum(-1)
    )
    delta_heads = row_delta.T

    def query_step(grad_sum, step_index):
        key_begin = step_index * key_block
        key_rows = lax.dynamic_slice_in_dim(key_all, key_begin, key_block)
        value_rows = lax.dynamic_slice_in_dim(value_all, key_begin, key_block)
        allowed = allowed_block(
            span_ok, positions, own_start, tokens, key_begin, key_block, span_rows
        )
        probability, dscores = local_terms(
            query_rows, grad_attended, log_total, delta_heads, key_rows, value_rows, allowed
        )
        return (
            grad_sum
            + jnp.einsum(
                "hqk,khd->qhd", dscores, split_heads(key_rows), preferred_element_type=jnp.float32
            ),
            None,
        )

    query_sum, _ = lax.scan(query_step, zero_heads, block_steps)
    query_gradient = query_sum.reshape(tokens, -1).astype(jnp.bfloat16)
    log_all, delta_all = (
        lax.all_gather(log_total.T, "cp", axis=0, tiled=True),
        lax.all_gather(row_delta, "cp", axis=0, tiled=True),
    )
    sums_now = (zero_heads, zero_heads)
    query_piece = lax.all_gather(query_rows, "cp", axis=0, tiled=True)
    grad_piece = lax.all_gather(grad_attended, "cp", axis=0, tiled=True)
    row_count = query_piece.shape[0]
    sources = row_count // tokens
    group_size = math.gcd(sources, max(1, 512 // tokens))
    group_rows = group_size * tokens

    def group_step(running, step_index):
        offset = step_index * group_rows
        query_group = lax.dynamic_slice_in_dim(query_piece, offset, group_rows)
        grad_group = lax.dynamic_slice_in_dim(grad_piece, offset, group_rows)
        log_group = lax.dynamic_slice_in_dim(log_all, offset, group_rows).T
        delta_group = lax.dynamic_slice_in_dim(delta_all, offset, group_rows).T
        allowed = allowed_block(
            span_ok, positions, offset, group_rows, own_start, tokens, span_rows
        )
        key_sum, value_sum = running
        probability, dscores = local_terms(
            query_group, grad_group, log_group, delta_group, key_local, value_local, allowed
        )
        probability_low = probability.astype(jnp.bfloat16).reshape(
            HEADS, group_size, tokens, tokens
        )
        dscores_group = dscores.reshape(HEADS, group_size, tokens, tokens)
        qsplit = query_group.reshape(group_size, tokens, HEADS, HEAD)
        gsplit = grad_group.reshape(group_size, tokens, HEADS, HEAD)
        key_part = jnp.einsum(
            "hgqk,gqhd->gkhd", dscores_group, qsplit, preferred_element_type=jnp.float32
        ).astype(jnp.bfloat16)
        value_part = jnp.einsum(
            "hgqk,gqhd->gkhd", probability_low, gsplit, preferred_element_type=jnp.float32
        ).astype(jnp.bfloat16)
        key_part, value_part = lax.optimization_barrier((key_part, value_part))
        return (
            (
                key_sum + key_part.astype(jnp.float32).sum(0),
                value_sum + value_part.astype(jnp.float32).sum(0),
            ),
            None,
        )

    sums_now, _ = lax.scan(group_step, sums_now, jnp.arange(sources // group_size, dtype=jnp.int32))
    key_sum, value_sum = sums_now
    key_gradient = key_sum.reshape(tokens, -1).astype(jnp.bfloat16)
    value_gradient = value_sum.reshape(tokens, -1).astype(jnp.bfloat16)
    cycle_count = lax.axis_size("cp")
    batch_count = lax.axis_size("fsdp")
    slab_rows = weight_term.shape[0] // (cycle_count * batch_count)
    reordered = weight_term.reshape(cycle_count, batch_count, slab_rows, -1).transpose(1, 0, 2, 3)
    reordered = reordered.reshape(weight_term.shape[0], -1)
    partial_batch = lax.psum_scatter(
        reordered.astype(jnp.bfloat16), "fsdp", scatter_dimension=0, tiled=True
    )
    weight_gradient = lax.psum_scatter(partial_batch, "cp", scatter_dimension=0, tiled=True).astype(
        jnp.float32
    )
    return (
        projected[None],
        query_gradient[None],
        key_gradient[None],
        value_gradient[None],
        weight_gradient,
    )


MESH = pl.DeviceIdType.MESH


def remote(src, dst, send_sem, recv_sem, device):
    return pltpu.make_async_remote_copy(
        src_ref=src,
        dst_ref=dst,
        send_sem=send_sem,
        recv_sem=recv_sem,
        device_id=device,
        device_id_type=MESH,
    )


def rows_of(begin, count):
    return pl.ds(pl.multiple_of(begin, count), count)


def greet(devices):
    barrier = pltpu.get_barrier_semaphore()
    for device in devices:
        pl.semaphore_signal(barrier, inc=1, device_id=device, device_id_type=MESH)
    pl.semaphore_wait(barrier, len(devices))


def layer_kernel(
    n, q_in, k_in, v_in, up_in, w_in, order_in, mask_in, proj, dq, dk, dv, wg,
    q, k, v, up, w, order, mask, load,
    qh, kh, vh, ups, wall, bias, prob, dsb, att, attp, ga_out, ga,
    dqh, dkh, dvh, dw, dwx, dwz, dwp, dwr, kt, vt, mix, mix_mate, mix_send, mix_beside,
    heads_s, heads_r, out_s, out_r, up_s, up_r,
    slab_s, slab_r, pass_s, side_s, side_r, ga_s, ga_r, att_s, att_r,
    dwx_s, dwx_r, lift_s, lift_r, dw_s, dw_r, mix_s, mix_r,
):
    me = lax.axis_index("cp")
    col = lax.axis_index("fsdp")
    cols = lax.axis_size("fsdp")
    planes = n // 2
    zed, why = me // 2, lax.rem(me, 2)
    ex, core = col // 2, lax.rem(col, 2)
    mate = {"fsdp": 2 * ex + 1 - core}
    across = {"fsdp": 2 * (1 - ex) + core}
    beside = {"cp": 2 * zed + 1 - why}
    tokens = up.shape[0]
    slab = w.shape[0]
    length = tokens * n
    span_rows = tokens // 2
    bf16, f32 = jnp.bfloat16, jnp.float32
    nt = (((1,), (1,)), ((), ()))
    home = 2 * core + ex
    root = home == zed
    keeper = core == zed // 2
    gateway = jnp.logical_and(jnp.logical_not(keeper), zed == 1 + zed // 2)
    pair = 2 * (zed + 1 - 2 * lax.rem(zed, 2)) + why

    def head_cols(d):
        return rows_of(d * HEAD, HEAD)

    def rows(d):
        return rows_of(d * tokens, tokens)

    def two_rows(d):
        return rows_of(d * 2 * tokens, 2 * tokens)

    pairs = (
        (k_in, k), (up_in, up), (w_in, w), (q_in, q), (v_in, v), (order_in, order), (mask_in, mask)
    )
    loads = [pltpu.make_async_copy(a, b, load.at[t]) for t, (a, b) in enumerate(pairs)]
    for copy in loads:
        copy.start()
    barrier = pltpu.get_barrier_semaphore()
    for i in range(n):
        for j in range(cols):
            if i or j:
                pl.semaphore_signal(
                    barrier, inc=1,
                    device_id={"cp": lax.rem(me + i, n), "fsdp": lax.rem(col + j, cols)},
                    device_id_type=MESH,
                )
    for copy in loads:
        copy.wait()
    pl.semaphore_wait(barrier, n * cols - 1)

    sends = []
    offsets = [n // 2]
    for i in range(1, n // 2):
        offsets += [n // 2 - i, n // 2 + i]

    def launch(copy):
        copy.start()
        sends.append(copy)

    def heads_send(t, source, target):
        for i in offsets:
            d = lax.rem(me + i, n)
            launch(remote(
                source.at[:, head_cols(d)], target.at[rows(me)],
                heads_s.at[t, i], heads_r.at[t, i], {"cp": d},
            ))

    def heads_arrival(t, i, target):
        source = lax.rem(me + n - i, n)
        block = target.at[rows(source)]
        remote(block, block, heads_s.at[t, i], heads_r.at[t, i], {"cp": source}).wait_recv()

    def heads_wait(t, target):
        for i in offsets:
            heads_arrival(t, i, target)

    def out_copy(t, i, source, target):
        d = lax.rem(me + i, n)
        return remote(
            source.at[rows(d)], target.at[:, head_cols(me)],
            out_s.at[t, i], out_r.at[t, i], {"cp": d},
        )

    def out_send(t, source, target):
        for i in offsets:
            launch(out_copy(t, i, source, target))

    def out_wait(t, target):
        for i in offsets:
            source = lax.rem(me + n - i, n)
            block = target.at[:, head_cols(source)]
            remote(block, block, out_s.at[t, i], out_r.at[t, i], {"cp": source}).wait_recv()

    own_slab = rows_of(lax.rem(zed, 2) * HEAD + col * slab, slab)
    slab_copies = [
        remote(
            w, wall.at[own_slab], slab_s.at[i], slab_r.at[col],
            {"cp": target, "fsdp": 2 * lax.rem(zed, 2) + zed // 2},
        )
        for i, target in enumerate((me, pair, 2 * (2 - zed // 2) + why))
    ]
    launch(slab_copies[2])

    @pl.when(jnp.logical_not(root))
    def _():
        slab_copies[0].start()

    launch(slab_copies[1])
    mine_up = ups.at[rows(2 * core + why)]
    launch(remote(up, mine_up, up_s.at[1], up_r.at[1], beside))
    heads_send(0, k, kh)
    launch(remote(up, mine_up, up_s.at[0], up_r.at[0], mate))
    heads_send(1, q, qh)

    @pl.when(root)
    def _():
        wall[own_slab] = w[...]

    def piece_of(plane, p):
        return wall.at[rows_of(lax.rem(plane, 2) * HEAD + p * slab, slab)]

    def pass_copy(p):
        block = piece_of(home, p)
        return remote(block, block, pass_s.at[p], slab_r.at[p], {"cp": pair})

    def side_copy(p):
        block = piece_of(home, p)
        return remote(block, block, side_s.at[p], side_r.at[p], across)

    def piece_poll(p):
        @pl.when(jnp.logical_not(jnp.logical_and(root, col == p)))
        def _():
            block = piece_of(home, p)
            remote(block, block, slab_s.at[0], slab_r.at[p], mate).wait_recv()

        @pl.when(gateway)
        def _():
            pass_copy(p).start()

        side_copy(p).start()

    for source, target in ((k, kh), (q, qh), (v, vh)):
        target[rows(me)] = source[:, head_cols(me)]
    ups[rows(2 * core + why)] = up[...]

    spans = order.shape[0]
    order_row = jnp.broadcast_to(order[...].reshape(1, spans), (spans, spans))
    place = lax.broadcasted_iota(jnp.int32, (spans, spans), 0)
    at_place = (order_row == place).astype(f32).astype(bf16)
    row = lax.broadcasted_iota(jnp.int32, (spans, length), 1)
    line = lax.broadcasted_iota(jnp.int32, (spans, length), 0)
    begin = line * span_rows
    member = jnp.logical_and(row >= begin, row < begin + span_rows).astype(f32)
    placed = jnp.dot(at_place, member.astype(bf16), preferred_element_type=f32)
    within = (row - begin).astype(f32) * member
    query_pos = (placed * begin.astype(f32) + within).sum(0, keepdims=True)
    key_pos = jnp.broadcast_to(query_pos, (8, length)).T[:, :1]
    placed_low = placed.astype(bf16)
    key_side = jnp.dot(
        mask[...].astype(f32).astype(bf16), placed_low, preferred_element_type=f32
    ).T.astype(bf16)
    for o in range(n):
        part = slice(o * tokens, (o + 1) * tokens)
        seen = jnp.dot(key_side, placed_low[:, part], preferred_element_type=f32)
        allowed = jnp.logical_and(seen > 0.5, key_pos <= query_pos[:, part])
        bias[:, part] = jnp.where(allowed, 0.0, lowest)

    far = jnp.logical_not(jnp.logical_or(keeper, gateway))

    @pl.when(jnp.logical_not(far))
    def _():
        for p in range(cols):
            piece_poll(p)

    heads_wait(0, kh)
    heads_send(2, v, vh)
    kt[...] = kh[...].astype(f32).T.astype(bf16)
    beside_up = ups.at[rows(2 * core + 1 - why)]
    remote(beside_up, beside_up, up_s.at[1], up_r.at[1], beside).wait_recv()
    launch(remote(beside_up, beside_up, up_s.at[2], up_r.at[2], mate))
    @pl.when(far)
    def _():
        for p in range(cols // 2):
            piece_poll(p)

    def soft(i, carry):
        @pl.when(i > 0)
        def _():
            heads_arrival(1, i, qh)

        part = rows(lax.rem(me + n - i, n))
        scores = lax.dot_general(kh[...], qh[part], nt, preferred_element_type=f32) * (1.0 / HEAD)
        scores = scores + bias[:, part]
        terms = jnp.exp(scores - scores.max(0, keepdims=True))
        probability = terms * (1.0 / terms.sum(0, keepdims=True))
        prob[:, part] = probability.astype(bf16)
        return carry

    lax.fori_loop(0, n, soft, 0)

    def seq_copy(ss, rs, slot, source, target, j, c):
        return remote(
            source, target, ss.at[slot], rs.at[zed], {"cp": 2 * (2 * core + j) + why, "fsdp": 2 * ex + c}
        )

    def seq_send(copy, here, j, i):
        if i:
            copy.start()
            return
        stays = 2 * core + j == zed

        @pl.when(stays)
        def _():
            here()

        @pl.when(jnp.logical_not(stays))
        def _():
            copy.start()

    def seq_settle(copy, j):
        @pl.when(2 * core + j != zed)
        def _():
            copy.wait_send()

    def seq_wait(ss, rs, block_of):
        for i in range(planes):
            source = lax.rem(zed + i, planes)
            block = block_of(source)
            arrived = remote(block, block, ss.at[0], rs.at[source], {"cp": me})
            if i == 0:
                @pl.when(jnp.logical_not(keeper))
                def _():
                    arrived.wait_recv()
            else:
                arrived.wait_recv()

    def ga_copy(i, j):
        c = core if i == 0 else 1 - core
        return seq_copy(
            ga_s, ga_r, 2 * i + j,
            ga_out.at[j, two_rows(c)], ga.at[two_rows(zed)], j, c,
        )

    def ga_group(i):
        c = core if i == 0 else 1 - core
        result = lax.dot_general(
            ups[two_rows(c)], wall[...], nt, preferred_element_type=f32
        ).astype(bf16)
        for j in range(2):
            ga_out[j, two_rows(c)] = result[:, j * HEAD:(j + 1) * HEAD]

            def here(j=j):
                ga[two_rows(zed)] = result[:, j * HEAD:(j + 1) * HEAD]

            seq_send(ga_copy(i, j), here, j, i)

    def work_gradient():
        for p in range(cols):
            block = piece_of(2 * core + 1 - ex, p)
            remote(block, block, side_s.at[p], side_r.at[p], across).wait_recv()

        ga_group(0)
        for slot, y in ((0, why), (2, 1 - why)):
            block = ups.at[rows(2 * (1 - core) + y)]
            remote(block, block, up_s.at[slot], up_r.at[slot], mate).wait_recv()
        ga_group(1)

    @pl.when(far)
    def _():
        for p in range(cols // 2, cols):
            piece_poll(p)

    @pl.when(jnp.logical_not(far))
    def _():
        work_gradient()

    heads_wait(2, vh)
    vt[...] = vh[...].astype(f32).T.astype(bf16)

    def att_copy(i):
        plane = lax.rem(zed + i, planes)
        return remote(
            att.at[two_rows(plane)], attp.at[lax.rem(zed, 2), two_rows(core)],
            att_s.at[i], att_r.at[2 * lax.rem(zed, 2) + core],
            {"cp": 2 * plane + why, "fsdp": 2 * ex + zed // 2},
        )

    def attend(o, carry):
        part = two_rows(o)
        att_t = jnp.dot(vt[...], prob[:, part], preferred_element_type=f32)
        att[part] = att_t.T.astype(bf16)
        return carry

    for i in (2, 1, 3):
        attend(lax.rem(zed + i, planes), 0)
        launch(att_copy(i))
    attend(zed, 0)

    @pl.when(keeper)
    def _():
        attp[lax.rem(zed, 2), two_rows(core)] = att[two_rows(zed)]

    @pl.when(jnp.logical_not(keeper))
    def _():
        att_copy(0).start()

    @pl.when(far)
    def _():
        work_gradient()

    width = math.gcd(proj.shape[1], 512)

    for j in range(2):
        for c in range(2):
            block = attp.at[j, 2 * c * tokens:2 * (c + 1) * tokens]
            arrived = remote(block, block, att_s.at[0], att_r.at[2 * j + c], {"cp": me})

            @pl.when(jnp.logical_not(jnp.logical_and(2 * core + j == zed, core == c)))
            def _():
                arrived.wait_recv()

    att_t = jnp.concatenate(
        [attp[0].astype(f32).T.astype(bf16), attp[1].astype(f32).T.astype(bf16)], axis=0
    )
    att_both = jnp.concatenate([attp[0], attp[1]], axis=1)

    def weigh(i, carry):
        lanes = rows_of(i * width, width)
        dw[:, lanes] = jnp.dot(att_t, ups[:, lanes], preferred_element_type=f32).astype(bf16)
        return carry

    def project(i, carry):
        lanes = rows_of(i * width, width)
        mix[:, lanes] = jnp.dot(
            att_both, wall[:, lanes], preferred_element_type=f32
        ).astype(bf16)
        return carry

    lax.fori_loop(0, proj.shape[1] // width, weigh, 0)
    share = 2 * slab

    def dw_rows(j, x):
        return rows_of(j * HEAD + x * share, share)

    for j in range(2):
        launch(remote(
            dw.at[dw_rows(j, 1 - ex)], dwx.at[j], dwx_s.at[j], dwx_r.at[j], across
        ))

    lax.fori_loop(0, proj.shape[1] // width, project, 0)
    launch(remote(mix.at[two_rows(1 - core)], mix_mate, mix_s.at[0], mix_r.at[0], mate))

    seq_wait(ga_s, ga_r, lambda source: ga.at[two_rows(source)])

    def piece_send(t, source, target, plane):
        for h in range(2):
            i = lax.rem(2 * plane + h + n - me, n)

            @pl.when(i > 0)
            def _():
                out_copy(t, i, source, target).start()

    def value_step(b, carry):
        plane = lax.rem(zed + 2 + b, planes)
        part = two_rows(plane)
        dvh[part] = jnp.dot(prob[part], ga[...], preferred_element_type=f32).astype(bf16)
        piece_send(2, dvh, dv, plane)
        return carry

    lax.fori_loop(0, planes, value_step, 0)
    dv[:, head_cols(me)] = dvh[rows(me)]

    def backward(i, carry):
        i = lax.rem(i + n // 2, n)
        o = lax.rem(me + i, n)
        part = rows(o)
        ga_rows = ga[part]
        delta = (att[part].astype(f32) * ga_rows.astype(f32)).T.sum(0, keepdims=True)
        dprob = lax.dot_general(vh[...], ga_rows, nt, preferred_element_type=f32)
        ds = (prob[:, part].astype(f32) * ((dprob - delta) * (1.0 / HEAD))).astype(bf16)
        dsb[:, part] = ds
        dqh[part] = jnp.dot(kt[...], ds, preferred_element_type=f32).T.astype(bf16)

        @pl.when(i > 0)
        def _():
            out_copy(0, i, dqh, dq).start()

        return carry

    lax.fori_loop(0, n // 2, backward, 0)
    remote(mix_mate, mix_mate, mix_s.at[0], mix_r.at[0], mate).wait_recv()
    theirs, ours = rows(1 - why), rows(why)
    mix_send[...] = (
        mix[rows(2 * core + 1 - why)].astype(f32) + mix_mate[theirs].astype(f32)
    ).astype(bf16)
    launch(remote(mix_send, mix_beside, mix_s.at[1], mix_r.at[1], beside))

    lax.fori_loop(n // 2, n, backward, 0)
    dq[:, head_cols(me)] = dqh[rows(me)]

    outer = jnp.logical_not(jnp.logical_or(keeper, gateway))

    def dw_copy(i, j):
        c = core if i == 0 else 1 - core
        return remote(
            dwz.at[j, rows_of(c * slab, slab)],
            dwr.at[jnp.where(keeper, jnp.where(2 * core + j == zed, 0, 1), 2)],
            dw_s.at[2 * i + j],
            dw_r.at[jnp.where(keeper, jnp.where(2 * core + j == zed, 0, 1), 2)],
            {"cp": 2 * (2 * core + j) + why, "fsdp": 2 * ex + c},
        )

    def lift_copy(j):
        return remote(dwz.at[j], dwp.at[j], lift_s.at[j], lift_r.at[j], {"cp": pair})

    def dw_send(j):
        for i in range(2):
            def here(j=j):
                dwr[0] = dwz[j, rows_of(core * slab, slab)]

            seq_send(dw_copy(i, j), here, j, i)

    for j in range(2):
        remote(dwx.at[j], dwx.at[j], dwx_s.at[j], dwx_r.at[j], across).wait_recv()
        dwz[j] = (dw[dw_rows(j, ex)].astype(f32) + dwx[j].astype(f32)).astype(bf16)

        @pl.when(outer)
        def _():
            lift_copy(j).start()

        @pl.when(keeper)
        def _():
            dw_send(j)

    def key_step(b, carry):
        plane = lax.rem(zed + 2 + b, planes)
        part = two_rows(plane)
        dkh[part] = jnp.dot(dsb[part], qh[...], preferred_element_type=f32).astype(bf16)
        piece_send(1, dkh, dk, plane)
        return carry

    lax.fori_loop(0, planes, key_step, 0)
    dk[:, head_cols(me)] = dkh[rows(me)]

    @pl.when(gateway)
    def _():
        for j in range(2):
            lift_copy(j).wait_recv()
            dwz[j] = (dwz[j].astype(f32) + dwp[j].astype(f32)).astype(bf16)
            dw_send(j)

    remote(mix_beside, mix_beside, mix_s.at[1], mix_r.at[1], beside).wait_recv()
    proj[...] = (
        mix[rows(2 * core + why)].astype(f32) + mix_mate[ours].astype(f32)
        + mix_beside[...].astype(f32)
    ).astype(bf16)
    for t in range(3):
        arrived = remote(dwr.at[t], dwr.at[t], dw_s.at[0], dw_r.at[t], {"cp": me})
        if t == 0:
            @pl.when(jnp.logical_not(keeper))
            def _():
                arrived.wait_recv()
        else:
            arrived.wait_recv()
    total = dwr[0].astype(f32) + dwr[1].astype(f32) + dwr[2].astype(f32)
    wg[...] = total
    out_wait(2, dv)
    out_wait(0, dq)
    out_wait(1, dk)
    for copy in sends:
        copy.wait_send()
    for i in offsets:
        out_copy(0, i, dqh, dq).wait_send()
        out_copy(2, i, dvh, dv).wait_send()
        out_copy(1, i, dkh, dk).wait_send()

    @pl.when(jnp.logical_not(root))
    def _():
        slab_copies[0].wait_send()

    @pl.when(jnp.logical_not(keeper))
    def _():
        att_copy(0).wait_send()

    for j in range(2):
        seq_settle(ga_copy(0, j), j)
        ga_copy(1, j).wait_send()

    for p in range(cols):
        side_copy(p).wait_send()

    for j in range(2):
        @pl.when(outer)
        def _():
            lift_copy(j).wait_send()

        @pl.when(jnp.logical_not(outer))
        def _():
            seq_settle(dw_copy(0, j), j)
            dw_copy(1, j).wait_send()


    @pl.when(gateway)
    def _():
        for p in range(cols):
            pass_copy(p).wait_send()


def deliver_kernel(*refs):
    count = len(refs) // 2
    copies = [
        pltpu.make_async_copy(refs[t], refs[count + t], refs[-1].at[t]) for t in range(count)
    ]
    for copy in copies:
        copy.start()
    for copy in copies:
        copy.wait()


def by_heads(query_states, key_states, value_states, span_order, block_mask, output_weight, upstream):
    n = lax.axis_size("cp")
    m = lax.axis_size("fsdp")
    tokens, width = query_states.shape[1:]
    length = tokens * n
    model = upstream.shape[2]
    slab = output_weight.shape[0]
    bf16, f32 = jnp.bfloat16, jnp.float32
    shape = jax.ShapeDtypeStruct
    vmem = pl.BlockSpec(memory_space=pltpu.VMEM)
    dma = pltpu.SemaphoreType.DMA
    planes = n // 2
    head_array = pltpu.VMEM((length, HEAD), bf16)
    square = pltpu.VMEM((length, length), bf16)
    projected, dq, dk, dv, weight_gradient = pl.pallas_call(
        lambda *refs: layer_kernel(n, *refs),
        out_shape=(shape((tokens, model), bf16),)
        + (shape((tokens, width), bf16),) * 3
        + (shape((slab, model), f32),),
        in_specs=[pl.BlockSpec(memory_space=pltpu.HBM)] * 7,
        out_specs=(vmem,) * 5,
        scratch_shapes=[
            pltpu.VMEM((tokens, width), bf16), pltpu.VMEM((tokens, width), bf16),
            pltpu.VMEM((tokens, width), bf16), pltpu.VMEM((tokens, model), bf16),
            pltpu.VMEM((slab, model), bf16), pltpu.VMEM(span_order.shape, jnp.int32),
            pltpu.VMEM(block_mask.shape, jnp.int32), dma((7,)),
            head_array, head_array, head_array,
            pltpu.VMEM((4 * tokens, model), bf16), pltpu.VMEM((2 * HEAD, model), bf16),
            pltpu.VMEM((length, length), f32), square, square,
            head_array, pltpu.VMEM((2, 4 * tokens, HEAD), bf16),
            pltpu.VMEM((2, 4 * tokens, HEAD), bf16),
            head_array, head_array, head_array, head_array,
            pltpu.VMEM((2 * HEAD, model), bf16), pltpu.VMEM((2, 2 * slab, model), bf16),
            pltpu.VMEM((2, 2 * slab, model), bf16),
            pltpu.VMEM((2, 2 * slab, model), bf16), pltpu.VMEM((3, slab, model), bf16),
            pltpu.VMEM((HEAD, length), bf16), pltpu.VMEM((HEAD, length), bf16),
            pltpu.VMEM((4 * tokens, model), bf16), pltpu.VMEM((2 * tokens, model), bf16),
            pltpu.VMEM((tokens, model), bf16), pltpu.VMEM((tokens, model), bf16),
            dma((3, n)), dma((3, n)), dma((3, n)), dma((3, n)), dma((3,)), dma((3,)),
            dma((3,)), dma((m,)), dma((m,)), dma((m,)), dma((m,)),
            dma((4,)), dma((planes,)), dma((planes,)), dma((4,)),
            dma((2,)), dma((2,)), dma((2,)), dma((2,)), dma((4,)), dma((3,)), dma((2,)), dma((2,)),
        ],
        compiler_params=pltpu.CompilerParams(
            collective_id=0, has_side_effects=True, vmem_limit_bytes=48 << 20
        ),
        name="layer",
    )(
        *(
            pltpu.with_memory_space_constraint(a, pltpu.HBM)
            for a in (
                query_states[0], key_states[0], value_states[0], upstream[0], output_weight,
                span_order, block_mask,
            )
        ),
    )
    results = (projected, dq, dk, dv, weight_gradient)
    projected, dq, dk, dv, weight_gradient = pl.pallas_call(
        deliver_kernel,
        out_shape=tuple(shape(r.shape, r.dtype) for r in results),
        in_specs=[pl.BlockSpec(memory_space=pl.ANY)] * 5,
        out_specs=(pl.BlockSpec(memory_space=pl.ANY),) * 5,
        scratch_shapes=[dma((5,))],
        compiler_params=pltpu.CompilerParams(vmem_limit_bytes=1 << 20),
        name="deliver",
    )(*results)
    return (projected[None], dq[None], dk[None], dv[None], weight_gradient)


def solution(mesh):
    fits = mesh.shape["cp"] == HEADS and mesh.shape["fsdp"] == 4
    return jax.shard_map(
        by_heads if fits else local,
        mesh=mesh,
        in_specs=(
            P("fsdp", "cp", None),
            P("fsdp", "cp", None),
            P("fsdp", "cp", None),
            P(),
            P(),
            P(("cp", "fsdp"), None),
            P("fsdp", "cp", None),
        ),
        out_specs=(
            P("fsdp", "cp", None),
            P("fsdp", "cp", None),
            P("fsdp", "cp", None),
            P("fsdp", "cp", None),
            P(("cp", "fsdp"), None),
        ),
        check_vma=False,
    )
```

```python
import math

import jax
import jax.numpy as jnp
from jax import lax
from jax.experimental import pallas as pl
from jax.experimental.pallas import tpu as pltpu
from jax.sharding import PartitionSpec as P

HEADS = 8
HEAD = 128


lowest = -1e30


def split_heads(row_block):
    return row_block.reshape(row_block.shape[0], HEADS, HEAD)


def pair_scores(query_rows, key_rows):
    return jnp.einsum(
        "qhd,khd->hqk",
        split_heads(query_rows),
        split_heads(key_rows),
        preferred_element_type=jnp.float32,
    ) * (1.0 / HEAD)


def storage_mask(span_order, block_mask):
    span_count = span_order.shape[0]
    onehot = (span_order[:, None] == jnp.arange(span_count, dtype=jnp.int32)[None, :]).astype(
        jnp.float32
    )
    permuted = jnp.dot(jnp.dot(onehot, block_mask.astype(jnp.float32)), onehot.T)
    return permuted > 0.5


def allowed_block(span_ok, positions, query_begin, query_total, key_begin, key_total, span_rows):
    span_sub = lax.dynamic_slice(
        span_ok,
        (query_begin // span_rows, key_begin // span_rows),
        (query_total // span_rows, key_total // span_rows),
    )
    spread = jnp.broadcast_to(
        span_sub[:, None, :, None],
        (query_total // span_rows, span_rows, key_total // span_rows, span_rows),
    )
    spread = spread.reshape(query_total, key_total)
    query_pos = lax.dynamic_slice_in_dim(positions, query_begin, query_total)
    key_pos = lax.dynamic_slice_in_dim(positions, key_begin, key_total)
    return spread & (key_pos[None, :] <= query_pos[:, None])


def local_terms(query_rows, grad_rows, log_rows, delta_rows, key_rows, value_rows, allowed):
    scores = pair_scores(query_rows, key_rows)
    probability = jnp.where(allowed[None], jnp.exp(scores - log_rows[..., None]), 0.0)
    dprob = jnp.einsum(
        "qhd,khd->hqk",
        split_heads(grad_rows),
        split_heads(value_rows),
        preferred_element_type=jnp.float32,
    )
    dscores = (probability * (dprob - delta_rows[..., None]) * (1.0 / HEAD)).astype(jnp.bfloat16)
    return (probability, dscores)


def local(query_states, key_states, value_states, span_order, block_mask, output_weight, upstream):
    query_rows = query_states[0]
    key_local = key_states[0]
    value_local = value_states[0]
    upstream_rows = upstream[0]
    tokens = query_rows.shape[0]
    span_rows = tokens // 2
    positions = (
        span_order[:, None] * span_rows + jnp.arange(span_rows, dtype=jnp.int32)[None, :]
    ).reshape(-1)
    span_ok = storage_mask(span_order, block_mask)
    own_start = lax.axis_index("cp") * tokens
    key_all, value_all = (
        lax.all_gather(key_local, "cp", axis=0, tiled=True),
        lax.all_gather(value_local, "cp", axis=0, tiled=True),
    )
    weight = lax.all_gather(output_weight, ("cp", "fsdp"), axis=0, tiled=True)
    length = key_all.shape[0]
    key_block = math.gcd(length, 512)
    block_count = length // key_block
    block_steps = jnp.arange(block_count, dtype=jnp.int32)

    def stats_step(running, step_index):
        key_begin = step_index * key_block
        key_rows = lax.dynamic_slice_in_dim(key_all, key_begin, key_block)
        allowed = allowed_block(
            span_ok, positions, own_start, tokens, key_begin, key_block, span_rows
        )
        maxima, totals = running
        scores = pair_scores(query_rows, key_rows)
        masked = jnp.where(allowed[None], scores, lowest)
        new_max = jnp.maximum(maxima, masked.max(-1))
        exp_terms = jnp.where(allowed[None], jnp.exp(scores - new_max[..., None]), 0.0)
        return ((new_max, totals * jnp.exp(maxima - new_max) + exp_terms.sum(-1)), None)

    stat_start = (
        jnp.full((HEADS, tokens), lowest, jnp.float32),
        jnp.zeros((HEADS, tokens), jnp.float32),
    )
    (maxima, totals), _ = lax.scan(stats_step, stat_start, block_steps)
    log_total = maxima + jnp.log(totals)

    def output_step(attn_sum, step_index):
        key_begin = step_index * key_block
        key_rows = lax.dynamic_slice_in_dim(key_all, key_begin, key_block)
        value_rows = lax.dynamic_slice_in_dim(value_all, key_begin, key_block)
        allowed = allowed_block(
            span_ok, positions, own_start, tokens, key_begin, key_block, span_rows
        )
        scores = pair_scores(query_rows, key_rows)
        probability = jnp.where(allowed[None], jnp.exp(scores - log_total[..., None]), 0.0)
        return (
            attn_sum
            + jnp.einsum(
                "hqk,khd->qhd",
                probability.astype(jnp.bfloat16),
                split_heads(value_rows),
                preferred_element_type=jnp.float32,
            ),
            None,
        )

    zero_heads = jnp.zeros((tokens, HEADS, HEAD), jnp.float32)
    attn_sum, _ = lax.scan(output_step, zero_heads, block_steps)
    attended = lax.optimization_barrier(attn_sum.reshape(tokens, -1).astype(jnp.bfloat16))
    projected = jnp.dot(attended, weight, preferred_element_type=jnp.float32).astype(jnp.bfloat16)
    grad_attended = lax.dot_general(
        upstream_rows, weight, (((1,), (1,)), ((), ())), preferred_element_type=jnp.float32
    ).astype(jnp.bfloat16)
    grad_attended = lax.optimization_barrier(grad_attended)
    weight_term = lax.dot_general(
        attended, upstream_rows, (((0,), (0,)), ((), ())), preferred_element_type=jnp.float32
    )
    row_delta = (
        (grad_attended.astype(jnp.float32) * attended.astype(jnp.float32))
        .reshape(tokens, HEADS, HEAD)
        .sum(-1)
    )
    delta_heads = row_delta.T

    def query_step(grad_sum, step_index):
        key_begin = step_index * key_block
        key_rows = lax.dynamic_slice_in_dim(key_all, key_begin, key_block)
        value_rows = lax.dynamic_slice_in_dim(value_all, key_begin, key_block)
        allowed = allowed_block(
            span_ok, positions, own_start, tokens, key_begin, key_block, span_rows
        )
        probability, dscores = local_terms(
            query_rows, grad_attended, log_total, delta_heads, key_rows, value_rows, allowed
        )
        return (
            grad_sum
            + jnp.einsum(
                "hqk,khd->qhd", dscores, split_heads(key_rows), preferred_element_type=jnp.float32
            ),
            None,
        )

    query_sum, _ = lax.scan(query_step, zero_heads, block_steps)
    query_gradient = query_sum.reshape(tokens, -1).astype(jnp.bfloat16)
    log_all, delta_all = (
        lax.all_gather(log_total.T, "cp", axis=0, tiled=True),
        lax.all_gather(row_delta, "cp", axis=0, tiled=True),
    )
    sums_now = (zero_heads, zero_heads)
    query_piece = lax.all_gather(query_rows, "cp", axis=0, tiled=True)
    grad_piece = lax.all_gather(grad_attended, "cp", axis=0, tiled=True)
    row_count = query_piece.shape[0]
    sources = row_count // tokens
    group_size = math.gcd(sources, max(1, 512 // tokens))
    group_rows = group_size * tokens

    def group_step(running, step_index):
        offset = step_index * group_rows
        query_group = lax.dynamic_slice_in_dim(query_piece, offset, group_rows)
        grad_group = lax.dynamic_slice_in_dim(grad_piece, offset, group_rows)
        log_group = lax.dynamic_slice_in_dim(log_all, offset, group_rows).T
        delta_group = lax.dynamic_slice_in_dim(delta_all, offset, group_rows).T
        allowed = allowed_block(
            span_ok, positions, offset, group_rows, own_start, tokens, span_rows
        )
        key_sum, value_sum = running
        probability, dscores = local_terms(
            query_group, grad_group, log_group, delta_group, key_local, value_local, allowed
        )
        probability_low = probability.astype(jnp.bfloat16).reshape(
            HEADS, group_size, tokens, tokens
        )
        dscores_group = dscores.reshape(HEADS, group_size, tokens, tokens)
        qsplit = query_group.reshape(group_size, tokens, HEADS, HEAD)
        gsplit = grad_group.reshape(group_size, tokens, HEADS, HEAD)
        key_part = jnp.einsum(
            "hgqk,gqhd->gkhd", dscores_group, qsplit, preferred_element_type=jnp.float32
        ).astype(jnp.bfloat16)
        value_part = jnp.einsum(
            "hgqk,gqhd->gkhd", probability_low, gsplit, preferred_element_type=jnp.float32
        ).astype(jnp.bfloat16)
        key_part, value_part = lax.optimization_barrier((key_part, value_part))
        return (
            (
                key_sum + key_part.astype(jnp.float32).sum(0),
                value_sum + value_part.astype(jnp.float32).sum(0),
            ),
            None,
        )

    sums_now, _ = lax.scan(group_step, sums_now, jnp.arange(sources // group_size, dtype=jnp.int32))
    key_sum, value_sum = sums_now
    key_gradient = key_sum.reshape(tokens, -1).astype(jnp.bfloat16)
    value_gradient = value_sum.reshape(tokens, -1).astype(jnp.bfloat16)
    cycle_count = lax.axis_size("cp")
    batch_count = lax.axis_size("fsdp")
    slab_rows = weight_term.shape[0] // (cycle_count * batch_count)
    reordered = weight_term.reshape(cycle_count, batch_count, slab_rows, -1).transpose(1, 0, 2, 3)
    reordered = reordered.reshape(weight_term.shape[0], -1)
    partial_batch = lax.psum_scatter(
        reordered.astype(jnp.bfloat16), "fsdp", scatter_dimension=0, tiled=True
    )
    weight_gradient = lax.psum_scatter(partial_batch, "cp", scatter_dimension=0, tiled=True).astype(
        jnp.float32
    )
    return (
        projected[None],
        query_gradient[None],
        key_gradient[None],
        value_gradient[None],
        weight_gradient,
    )


MESH = pl.DeviceIdType.MESH


def remote(src, dst, send_sem, recv_sem, device):
    return pltpu.make_async_remote_copy(
        src_ref=src,
        dst_ref=dst,
        send_sem=send_sem,
        recv_sem=recv_sem,
        device_id=device,
        device_id_type=MESH,
    )


def rows_of(begin, count):
    return pl.ds(pl.multiple_of(begin, count), count)


def greet(devices):
    barrier = pltpu.get_barrier_semaphore()
    for device in devices:
        pl.semaphore_signal(barrier, inc=1, device_id=device, device_id_type=MESH)
    pl.semaphore_wait(barrier, len(devices))


def layer_kernel(
    n, q_in, k_in, v_in, up_in, w_in, order_in, mask_in, proj, dq, dk, dv, wg,
    q, k, v, up, w, order, mask, load,
    qh, kh, vh, ups, wall, bias, prob, dsb, att, attp, ga_out, ga,
    dqh, dkh, dvh, dw, dwx, dwz, dwp, dwr, kt, vt, mix, mix_mate, mix_send, mix_beside,
    heads_s, heads_r, out_s, out_r, up_s, up_r,
    slab_s, slab_r, pass_s, side_s, side_r, ga_s, ga_r, att_s, att_r,
    dwx_s, dwx_r, lift_s, lift_r, dw_s, dw_r, mix_s, mix_r,
):
    me = lax.axis_index("cp")
    col = lax.axis_index("fsdp")
    cols = lax.axis_size("fsdp")
    planes = n // 2
    zed, why = me // 2, lax.rem(me, 2)
    ex, core = col // 2, lax.rem(col, 2)
    mate = {"fsdp": 2 * ex + 1 - core}
    across = {"fsdp": 2 * (1 - ex) + core}
    beside = {"cp": 2 * zed + 1 - why}
    tokens = up.shape[0]
    slab = w.shape[0]
    length = tokens * n
    span_rows = tokens // 2
    bf16, f32 = jnp.bfloat16, jnp.float32
    nt = (((1,), (1,)), ((), ()))
    home = 2 * core + ex
    root = home == zed
    keeper = core == zed // 2
    gateway = jnp.logical_and(jnp.logical_not(keeper), zed == 1 + zed // 2)
    pair = 2 * (zed + 1 - 2 * lax.rem(zed, 2)) + why

    def head_cols(d):
        return rows_of(d * HEAD, HEAD)

    def rows(d):
        return rows_of(d * tokens, tokens)

    def two_rows(d):
        return rows_of(d * 2 * tokens, 2 * tokens)

    pairs = (
        (k_in, k), (up_in, up), (w_in, w), (q_in, q), (v_in, v), (order_in, order), (mask_in, mask)
    )
    loads = [pltpu.make_async_copy(a, b, load.at[t]) for t, (a, b) in enumerate(pairs)]
    for copy in loads:
        copy.start()
    barrier = pltpu.get_barrier_semaphore()
    for i in range(n):
        for j in range(cols):
            if i or j:
                pl.semaphore_signal(
                    barrier, inc=1,
                    device_id={"cp": lax.rem(me + i, n), "fsdp": lax.rem(col + j, cols)},
                    device_id_type=MESH,
                )
    for copy in loads[:3]:
        copy.wait()
    pl.semaphore_wait(barrier, n * cols - 1)

    sends = []
    offsets = [n // 2]
    for i in range(1, n // 2):
        offsets += [n // 2 - i, n // 2 + i]

    def launch(copy):
        copy.start()
        sends.append(copy)

    def heads_send(t, source, target):
        for i in offsets:
            d = lax.rem(me + i, n)
            launch(remote(
                source.at[:, head_cols(d)], target.at[rows(me)],
                heads_s.at[t, i], heads_r.at[t, i], {"cp": d},
            ))

    def heads_arrival(t, i, target):
        source = lax.rem(me + n - i, n)
        block = target.at[rows(source)]
        remote(block, block, heads_s.at[t, i], heads_r.at[t, i], {"cp": source}).wait_recv()

    def heads_wait(t, target):
        for i in offsets:
            heads_arrival(t, i, target)

    def out_copy(t, i, source, target):
        d = lax.rem(me + i, n)
        return remote(
            source.at[rows(d)], target.at[:, head_cols(me)],
            out_s.at[t, i], out_r.at[t, i], {"cp": d},
        )

    def out_send(t, source, target):
        for i in offsets:
            launch(out_copy(t, i, source, target))

    def out_wait(t, target):
        for i in offsets:
            source = lax.rem(me + n - i, n)
            block = target.at[:, head_cols(source)]
            remote(block, block, out_s.at[t, i], out_r.at[t, i], {"cp": source}).wait_recv()

    own_slab = rows_of(lax.rem(zed, 2) * HEAD + col * slab, slab)
    slab_copies = [
        remote(
            w, wall.at[own_slab], slab_s.at[i], slab_r.at[col],
            {"cp": target, "fsdp": 2 * lax.rem(zed, 2) + zed // 2},
        )
        for i, target in enumerate((me, pair, 2 * (2 - zed // 2) + why))
    ]
    launch(slab_copies[2])

    @pl.when(jnp.logical_not(root))
    def _():
        slab_copies[0].start()

    launch(slab_copies[1])
    mine_up = ups.at[rows(2 * core + why)]
    launch(remote(up, mine_up, up_s.at[1], up_r.at[1], beside))
    heads_send(0, k, kh)
    launch(remote(up, mine_up, up_s.at[0], up_r.at[0], mate))
    for copy in loads[3:]:
        copy.wait()
    heads_send(1, q, qh)

    @pl.when(root)
    def _():
        wall[own_slab] = w[...]

    def piece_of(plane, p):
        return wall.at[rows_of(lax.rem(plane, 2) * HEAD + p * slab, slab)]

    def pass_copy(p):
        block = piece_of(home, p)
        return remote(block, block, pass_s.at[p], slab_r.at[p], {"cp": pair})

    def side_copy(p):
        block = piece_of(home, p)
        return remote(block, block, side_s.at[p], side_r.at[p], across)

    def piece_poll(p):
        @pl.when(jnp.logical_not(jnp.logical_and(root, col == p)))
        def _():
            block = piece_of(home, p)
            remote(block, block, slab_s.at[0], slab_r.at[p], mate).wait_recv()

        @pl.when(gateway)
        def _():
            pass_copy(p).start()

        side_copy(p).start()

    for source, target in ((k, kh), (q, qh), (v, vh)):
        target[rows(me)] = source[:, head_cols(me)]
    ups[rows(2 * core + why)] = up[...]

    spans = order.shape[0]
    order_row = jnp.broadcast_to(order[...].reshape(1, spans), (spans, spans))
    place = lax.broadcasted_iota(jnp.int32, (spans, spans), 0)
    at_place = (order_row == place).astype(f32).astype(bf16)
    row = lax.broadcasted_iota(jnp.int32, (spans, length), 1)
    line = lax.broadcasted_iota(jnp.int32, (spans, length), 0)
    begin = line * span_rows
    member = jnp.logical_and(row >= begin, row < begin + span_rows).astype(f32)
    placed = jnp.dot(at_place, member.astype(bf16), preferred_element_type=f32)
    within = (row - begin).astype(f32) * member
    query_pos = (placed * begin.astype(f32) + within).sum(0, keepdims=True)
    key_pos = jnp.broadcast_to(query_pos, (8, length)).T[:, :1]
    placed_low = placed.astype(bf16)
    key_side = jnp.dot(
        mask[...].astype(f32).astype(bf16), placed_low, preferred_element_type=f32
    ).T.astype(bf16)
    for o in range(n):
        part = slice(o * tokens, (o + 1) * tokens)
        seen = jnp.dot(key_side, placed_low[:, part], preferred_element_type=f32)
        allowed = jnp.logical_and(seen > 0.5, key_pos <= query_pos[:, part])
        bias[:, part] = jnp.where(allowed, 0.0, lowest)

    far = jnp.logical_not(jnp.logical_or(keeper, gateway))

    @pl.when(jnp.logical_not(far))
    def _():
        for p in range(cols):
            piece_poll(p)

    heads_wait(0, kh)
    kt[...] = kh[...].astype(f32).T.astype(bf16)
    beside_up = ups.at[rows(2 * core + 1 - why)]
    remote(beside_up, beside_up, up_s.at[1], up_r.at[1], beside).wait_recv()
    launch(remote(beside_up, beside_up, up_s.at[2], up_r.at[2], mate))
    heads_send(2, v, vh)
    @pl.when(far)
    def _():
        for p in range(cols // 2):
            piece_poll(p)

    def soft(i, carry):
        @pl.when(i > 0)
        def _():
            heads_arrival(1, i, qh)

        part = rows(lax.rem(me + n - i, n))
        scores = lax.dot_general(kh[...], qh[part], nt, preferred_element_type=f32) * (1.0 / HEAD)
        scores = scores + bias[:, part]
        terms = jnp.exp(scores - scores.max(0, keepdims=True))
        probability = terms * (1.0 / terms.sum(0, keepdims=True))
        prob[:, part] = probability.astype(bf16)
        return carry

    lax.fori_loop(0, n, soft, 0)

    def seq_copy(ss, rs, slot, source, target, j, c):
        return remote(
            source, target, ss.at[slot], rs.at[zed], {"cp": 2 * (2 * core + j) + why, "fsdp": 2 * ex + c}
        )

    def seq_send(copy, here, j, i):
        if i:
            copy.start()
            return
        stays = 2 * core + j == zed

        @pl.when(stays)
        def _():
            here()

        @pl.when(jnp.logical_not(stays))
        def _():
            copy.start()

    def seq_settle(copy, j):
        @pl.when(2 * core + j != zed)
        def _():
            copy.wait_send()

    def seq_wait(ss, rs, block_of):
        for i in range(planes):
            source = lax.rem(zed + i, planes)
            block = block_of(source)
            arrived = remote(block, block, ss.at[0], rs.at[source], {"cp": me})
            if i == 0:
                @pl.when(jnp.logical_not(keeper))
                def _():
                    arrived.wait_recv()
            else:
                arrived.wait_recv()

    def ga_copy(i, j):
        c = core if i == 0 else 1 - core
        return seq_copy(
            ga_s, ga_r, 2 * i + j,
            ga_out.at[j, two_rows(c)], ga.at[two_rows(zed)], j, c,
        )

    def ga_group(i):
        c = core if i == 0 else 1 - core
        result = lax.dot_general(
            ups[two_rows(c)], wall[...], nt, preferred_element_type=f32
        ).astype(bf16)
        for j in range(2):
            ga_out[j, two_rows(c)] = result[:, j * HEAD:(j + 1) * HEAD]

            def here(j=j):
                ga[two_rows(zed)] = result[:, j * HEAD:(j + 1) * HEAD]

            seq_send(ga_copy(i, j), here, j, i)

    def work_gradient():
        for p in range(cols):
            block = piece_of(2 * core + 1 - ex, p)
            remote(block, block, side_s.at[p], side_r.at[p], across).wait_recv()

        ga_group(0)
        for slot, y in ((0, why), (2, 1 - why)):
            block = ups.at[rows(2 * (1 - core) + y)]
            remote(block, block, up_s.at[slot], up_r.at[slot], mate).wait_recv()
        ga_group(1)

    @pl.when(far)
    def _():
        for p in range(cols // 2, cols):
            piece_poll(p)

    @pl.when(jnp.logical_not(far))
    def _():
        work_gradient()

    heads_wait(2, vh)
    vt[...] = vh[...].astype(f32).T.astype(bf16)

    def att_copy(i):
        plane = lax.rem(zed + i, planes)
        return remote(
            att.at[two_rows(plane)], attp.at[lax.rem(zed, 2), two_rows(core)],
            att_s.at[i], att_r.at[2 * lax.rem(zed, 2) + core],
            {"cp": 2 * plane + why, "fsdp": 2 * ex + zed // 2},
        )

    def attend(o, carry):
        part = two_rows(o)
        att_t = jnp.dot(vt[...], prob[:, part], preferred_element_type=f32)
        att[part] = att_t.T.astype(bf16)
        return carry

    for i in (2, 1, 3):
        attend(lax.rem(zed + i, planes), 0)
        launch(att_copy(i))
    attend(zed, 0)

    @pl.when(keeper)
    def _():
        attp[lax.rem(zed, 2), two_rows(core)] = att[two_rows(zed)]

    @pl.when(jnp.logical_not(keeper))
    def _():
        att_copy(0).start()

    @pl.when(far)
    def _():
        work_gradient()

    width = math.gcd(proj.shape[1], 512)

    for j in range(2):
        for c in range(2):
            block = attp.at[j, 2 * c * tokens:2 * (c + 1) * tokens]
            arrived = remote(block, block, att_s.at[0], att_r.at[2 * j + c], {"cp": me})

            @pl.when(jnp.logical_not(jnp.logical_and(2 * core + j == zed, core == c)))
            def _():
                arrived.wait_recv()

    att_t = jnp.concatenate(
        [attp[0].astype(f32).T.astype(bf16), attp[1].astype(f32).T.astype(bf16)], axis=0
    )
    att_both = jnp.concatenate([attp[0], attp[1]], axis=1)

    def weigh(i, carry):
        lanes = rows_of(i * width, width)
        dw[:, lanes] = jnp.dot(att_t, ups[:, lanes], preferred_element_type=f32).astype(bf16)
        return carry

    def project(i, carry):
        lanes = rows_of(i * width, width)
        mix[:, lanes] = jnp.dot(
            att_both, wall[:, lanes], preferred_element_type=f32
        ).astype(bf16)
        return carry

    lax.fori_loop(0, proj.shape[1] // width, weigh, 0)
    share = 2 * slab

    def dw_rows(j, x):
        return rows_of(j * HEAD + x * share, share)

    for j in range(2):
        launch(remote(
            dw.at[dw_rows(j, 1 - ex)], dwx.at[j], dwx_s.at[j], dwx_r.at[j], across
        ))

    lax.fori_loop(0, proj.shape[1] // width, project, 0)
    launch(remote(mix.at[two_rows(1 - core)], mix_mate, mix_s.at[0], mix_r.at[0], mate))

    seq_wait(ga_s, ga_r, lambda source: ga.at[two_rows(source)])

    def piece_send(t, source, target, plane):
        for h in range(2):
            i = lax.rem(2 * plane + h + n - me, n)

            @pl.when(i > 0)
            def _():
                out_copy(t, i, source, target).start()

    def value_step(b, carry):
        plane = lax.rem(zed + 2 + b, planes)
        part = two_rows(plane)
        dvh[part] = jnp.dot(prob[part], ga[...], preferred_element_type=f32).astype(bf16)
        piece_send(2, dvh, dv, plane)
        return carry

    lax.fori_loop(0, planes, value_step, 0)
    dv[:, head_cols(me)] = dvh[rows(me)]

    def backward(i, carry):
        i = lax.rem(i + n // 2, n)
        o = lax.rem(me + i, n)
        part = rows(o)
        ga_rows = ga[part]
        delta = (att[part].astype(f32) * ga_rows.astype(f32)).T.sum(0, keepdims=True)
        dprob = lax.dot_general(vh[...], ga_rows, nt, preferred_element_type=f32)
        ds = (prob[:, part].astype(f32) * ((dprob - delta) * (1.0 / HEAD))).astype(bf16)
        dsb[:, part] = ds
        dqh[part] = jnp.dot(kt[...], ds, preferred_element_type=f32).T.astype(bf16)

        @pl.when(i > 0)
        def _():
            out_copy(0, i, dqh, dq).start()

        return carry

    lax.fori_loop(0, n // 2, backward, 0)
    remote(mix_mate, mix_mate, mix_s.at[0], mix_r.at[0], mate).wait_recv()
    theirs, ours = rows(1 - why), rows(why)
    mix_send[...] = (
        mix[rows(2 * core + 1 - why)].astype(f32) + mix_mate[theirs].astype(f32)
    ).astype(bf16)
    launch(remote(mix_send, mix_beside, mix_s.at[1], mix_r.at[1], beside))

    lax.fori_loop(n // 2, n, backward, 0)
    dq[:, head_cols(me)] = dqh[rows(me)]

    outer = jnp.logical_not(jnp.logical_or(keeper, gateway))

    def dw_copy(i, j):
        c = core if i == 0 else 1 - core
        return remote(
            dwz.at[j, rows_of(c * slab, slab)],
            dwr.at[jnp.where(keeper, jnp.where(2 * core + j == zed, 0, 1), 2)],
            dw_s.at[2 * i + j],
            dw_r.at[jnp.where(keeper, jnp.where(2 * core + j == zed, 0, 1), 2)],
            {"cp": 2 * (2 * core + j) + why, "fsdp": 2 * ex + c},
        )

    def lift_copy(j):
        return remote(dwz.at[j], dwp.at[j], lift_s.at[j], lift_r.at[j], {"cp": pair})

    def dw_send(j):
        for i in range(2):
            def here(j=j):
                dwr[0] = dwz[j, rows_of(core * slab, slab)]

            seq_send(dw_copy(i, j), here, j, i)

    for j in range(2):
        remote(dwx.at[j], dwx.at[j], dwx_s.at[j], dwx_r.at[j], across).wait_recv()
        dwz[j] = (dw[dw_rows(j, ex)].astype(f32) + dwx[j].astype(f32)).astype(bf16)

        @pl.when(outer)
        def _():
            lift_copy(j).start()

        @pl.when(keeper)
        def _():
            dw_send(j)

    def key_step(b, carry):
        plane = lax.rem(zed + 2 + b, planes)
        part = two_rows(plane)
        dkh[part] = jnp.dot(dsb[part], qh[...], preferred_element_type=f32).astype(bf16)
        piece_send(1, dkh, dk, plane)
        return carry

    lax.fori_loop(0, planes, key_step, 0)
    dk[:, head_cols(me)] = dkh[rows(me)]

    @pl.when(gateway)
    def _():
        for j in range(2):
            lift_copy(j).wait_recv()
            dwz[j] = (dwz[j].astype(f32) + dwp[j].astype(f32)).astype(bf16)
            dw_send(j)

    remote(mix_beside, mix_beside, mix_s.at[1], mix_r.at[1], beside).wait_recv()
    proj[...] = (
        mix[rows(2 * core + why)].astype(f32) + mix_mate[ours].astype(f32)
        + mix_beside[...].astype(f32)
    ).astype(bf16)
    for t in range(3):
        arrived = remote(dwr.at[t], dwr.at[t], dw_s.at[0], dw_r.at[t], {"cp": me})
        if t == 0:
            @pl.when(jnp.logical_not(keeper))
            def _():
                arrived.wait_recv()
        else:
            arrived.wait_recv()
    total = dwr[0].astype(f32) + dwr[1].astype(f32) + dwr[2].astype(f32)
    wg[...] = total
    out_wait(2, dv)
    out_wait(0, dq)
    out_wait(1, dk)
    for copy in sends:
        copy.wait_send()
    for i in offsets:
        out_copy(0, i, dqh, dq).wait_send()
        out_copy(2, i, dvh, dv).wait_send()
        out_copy(1, i, dkh, dk).wait_send()

    @pl.when(jnp.logical_not(root))
    def _():
        slab_copies[0].wait_send()

    @pl.when(jnp.logical_not(keeper))
    def _():
        att_copy(0).wait_send()

    for j in range(2):
        seq_settle(ga_copy(0, j), j)
        ga_copy(1, j).wait_send()

    for p in range(cols):
        side_copy(p).wait_send()

    for j in range(2):
        @pl.when(outer)
        def _():
            lift_copy(j).wait_send()

        @pl.when(jnp.logical_not(outer))
        def _():
            seq_settle(dw_copy(0, j), j)
            dw_copy(1, j).wait_send()


    @pl.when(gateway)
    def _():
        for p in range(cols):
            pass_copy(p).wait_send()


def deliver_kernel(*refs):
    count = len(refs) // 2
    copies = [
        pltpu.make_async_copy(refs[t], refs[count + t], refs[-1].at[t]) for t in range(count)
    ]
    for copy in copies:
        copy.start()
    for copy in copies:
        copy.wait()


def by_heads(query_states, key_states, value_states, span_order, block_mask, output_weight, upstream):
    n = lax.axis_size("cp")
    m = lax.axis_size("fsdp")
    tokens, width = query_states.shape[1:]
    length = tokens * n
    model = upstream.shape[2]
    slab = output_weight.shape[0]
    bf16, f32 = jnp.bfloat16, jnp.float32
    shape = jax.ShapeDtypeStruct
    vmem = pl.BlockSpec(memory_space=pltpu.VMEM)
    dma = pltpu.SemaphoreType.DMA
    planes = n // 2
    head_array = pltpu.VMEM((length, HEAD), bf16)
    square = pltpu.VMEM((length, length), bf16)
    projected, dq, dk, dv, weight_gradient = pl.pallas_call(
        lambda *refs: layer_kernel(n, *refs),
        out_shape=(shape((tokens, model), bf16),)
        + (shape((tokens, width), bf16),) * 3
        + (shape((slab, model), f32),),
        in_specs=[pl.BlockSpec(memory_space=pltpu.HBM)] * 7,
        out_specs=(vmem,) * 5,
        scratch_shapes=[
            pltpu.VMEM((tokens, width), bf16), pltpu.VMEM((tokens, width), bf16),
            pltpu.VMEM((tokens, width), bf16), pltpu.VMEM((tokens, model), bf16),
            pltpu.VMEM((slab, model), bf16), pltpu.VMEM(span_order.shape, jnp.int32),
            pltpu.VMEM(block_mask.shape, jnp.int32), dma((7,)),
            head_array, head_array, head_array,
            pltpu.VMEM((4 * tokens, model), bf16), pltpu.VMEM((2 * HEAD, model), bf16),
            pltpu.VMEM((length, length), f32), square, square,
            head_array, pltpu.VMEM((2, 4 * tokens, HEAD), bf16),
            pltpu.VMEM((2, 4 * tokens, HEAD), bf16),
            head_array, head_array, head_array, head_array,
            pltpu.VMEM((2 * HEAD, model), bf16), pltpu.VMEM((2, 2 * slab, model), bf16),
            pltpu.VMEM((2, 2 * slab, model), bf16),
            pltpu.VMEM((2, 2 * slab, model), bf16), pltpu.VMEM((3, slab, model), bf16),
            pltpu.VMEM((HEAD, length), bf16), pltpu.VMEM((HEAD, length), bf16),
            pltpu.VMEM((4 * tokens, model), bf16), pltpu.VMEM((2 * tokens, model), bf16),
            pltpu.VMEM((tokens, model), bf16), pltpu.VMEM((tokens, model), bf16),
            dma((3, n)), dma((3, n)), dma((3, n)), dma((3, n)), dma((3,)), dma((3,)),
            dma((3,)), dma((m,)), dma((m,)), dma((m,)), dma((m,)),
            dma((4,)), dma((planes,)), dma((planes,)), dma((4,)),
            dma((2,)), dma((2,)), dma((2,)), dma((2,)), dma((4,)), dma((3,)), dma((2,)), dma((2,)),
        ],
        compiler_params=pltpu.CompilerParams(
            collective_id=0, has_side_effects=True, vmem_limit_bytes=48 << 20
        ),
        name="layer",
    )(
        *(
            pltpu.with_memory_space_constraint(a, pltpu.HBM)
            for a in (
                query_states[0], key_states[0], value_states[0], upstream[0], output_weight,
                span_order, block_mask,
            )
        ),
    )
    results = (projected, dq, dk, dv, weight_gradient)
    projected, dq, dk, dv, weight_gradient = pl.pallas_call(
        deliver_kernel,
        out_shape=tuple(shape(r.shape, r.dtype) for r in results),
        in_specs=[pl.BlockSpec(memory_space=pl.ANY)] * 5,
        out_specs=(pl.BlockSpec(memory_space=pl.ANY),) * 5,
        scratch_shapes=[dma((5,))],
        compiler_params=pltpu.CompilerParams(vmem_limit_bytes=1 << 20),
        name="deliver",
    )(*results)
    return (projected[None], dq[None], dk[None], dv[None], weight_gradient)


def solution(mesh):
    fits = mesh.shape["cp"] == HEADS and mesh.shape["fsdp"] == 4
    return jax.shard_map(
        by_heads if fits else local,
        mesh=mesh,
        in_specs=(
            P("fsdp", "cp", None),
            P("fsdp", "cp", None),
            P("fsdp", "cp", None),
            P(),
            P(),
            P(("cp", "fsdp"), None),
            P("fsdp", "cp", None),
        ),
        out_specs=(
            P("fsdp", "cp", None),
            P("fsdp", "cp", None),
            P("fsdp", "cp", None),
            P("fsdp", "cp", None),
            P(("cp", "fsdp"), None),
        ),
        check_vma=False,
    )
```
